512 devices in a mesh: row: 16 (over x, y), col: 32 (over z, core).
Axes of the slice: x: 4, y: 4, z: 16, core: 2. Of those that a mesh axis runs over, the one named last changes fastest.
Arguments:
- start_vector: bfloat16 [4, 2048, 2048], P(None, 'row', 'col'), may hold values from -150 to 150
- left_env: bfloat16 [5, 2048, 2048], P(None, 'row', 'col'), may hold values from -5 to 6
- right_env: bfloat16 [5, 2048, 2048], P(None, 'col', 'row'), may hold values from -5 to 6
- left_tensor: float32 [5, 5, 2, 2], replicated, may hold values from -1.5 to 2.5
- right_tensor: float32 [5, 5, 2, 2], replicated, may hold values from -1.5 to 2.5
Outputs:
- next_vector: bfloat16 [4, 2048, 2048], P(None, 'row', 'col')
- coefficients: float32 [2], replicated
The draws below stay inside these ranges and needn't reach their ends.
All inputs are finite; a program needn't handle non-finite values.
Results may differ from the reference program's by a relative error of at most 0.023.
Values may be sent and summed in bfloat16 or wider, within the bound.
No kernel may reach another device: no remote copies, remote signals or barrier semaphores. Data moves between devices by JAX's collectives and lax.ppermute only.
A program may use at most 64 MiB of HBM per device.

```python
import jax
import jax.numpy as jnp
from jax import lax

D = 2048
CHANNELS = 5
STATES = 4
N_COL = 32


def environment(key, rising):
    random_part = jax.random.truncated_normal(key, -4.0, 4.0, (CHANNELS, D, D), jnp.float32)
    symmetric = (random_part + jnp.swapaxes(random_part, 1, 2)) * 0.5 ** 0.5 * D ** (-0.5)
    first_channel = (jnp.arange(CHANNELS) == 0).astype(jnp.float32)
    positions = jnp.arange(D, dtype=jnp.float32) / D
    diagonal_values = rising * (0.5 + 2.5 * positions) + (1.0 - rising) * jnp.ones((D,), jnp.float32)
    identity = jnp.eye(D, dtype=jnp.float32) * diagonal_values[:, None]
    return (symmetric + first_channel[:, None, None] * identity[None, :, :]).astype(jnp.bfloat16)


def site_tensor(key):
    raw_values = jax.random.truncated_normal(key, -4.0, 4.0, (CHANNELS, CHANNELS, 2, 2), jnp.float32)
    symmetric = (raw_values + jnp.swapaxes(raw_values, 2, 3)) * 0.5 * 0.3
    indices = jnp.arange(CHANNELS)
    corner = (indices == 0) | (indices == CHANNELS - 1)
    marks = ((indices[:, None] == indices[None, :]) & corner[:, None]).astype(jnp.float32)
    return symmetric + marks[:, :, None, None] * jnp.eye(2, dtype=jnp.float32)[None, None, :, :]


def draw_start_vector(key, part):
    positions = jnp.arange(D, dtype=jnp.float32) / D
    row_scale = jnp.exp(jax.random.uniform(jax.random.fold_in(key, 11), (D,), jnp.float32, -0.7, 0.7))
    col_scale = jnp.exp(jax.random.uniform(jax.random.fold_in(key, 12), (D,), jnp.float32, -0.7, 0.7))
    base_values = jax.random.truncated_normal(jax.random.fold_in(key, 13), -4.0, 4.0, (STATES, D, D), jnp.float32)
    row_scale = row_scale * (1.0 + 2.0 * positions)
    col_scale = col_scale * (1.0 + 2.0 * positions)
    return (base_values * row_scale[None, :, None] * col_scale[None, None, :]).astype(jnp.bfloat16)


def draw_left_env(key, part):
    return environment(jax.random.fold_in(key, 1), 1.0)


def draw_right_env(key, part):
    return environment(jax.random.fold_in(key, 2), 0.0)


def draw_left_tensor(key, part):
    return site_tensor(jax.random.fold_in(key, 3))


def draw_right_tensor(key, part):
    return site_tensor(jax.random.fold_in(key, 4))


def setup_inputs(seed: int = 0) -> dict:
    key_list = jax.random.split(jax.random.key(seed), 6)
    start_vector = draw_start_vector(jax.random.fold_in(key_list[5], 71), 0)
    left_env = draw_left_env(jax.random.fold_in(key_list[5], 71), 0)
    right_env = draw_right_env(jax.random.fold_in(key_list[5], 71), 0)
    left_tensor = draw_left_tensor(jax.random.fold_in(key_list[5], 71), 0)
    right_tensor = draw_right_tensor(jax.random.fold_in(key_list[5], 71), 0)
    return dict(start_vector=start_vector, left_env=left_env, right_env=right_env, left_tensor=left_tensor, right_tensor=right_tensor)


def coupling(left_tensor, right_tensor):
    channels = left_tensor.shape[0]
    joined = jnp.einsum('wuac,uvbd->vabwcd', left_tensor.astype(jnp.float32), right_tensor.astype(jnp.float32), precision=lax.Precision.HIGHEST)
    return joined.reshape(channels, 4, channels, 4)

def apply_hamiltonian(vector, coupling_table, left_env, right_env):
    cross = jnp.einsum('wax,txb->wtab', left_env.astype(jnp.float32), vector.astype(jnp.float32), precision=lax.Precision.HIGHEST)
    mixed_bond = jnp.einsum('vswt,wtab->vsab', coupling_table, cross, precision=lax.Precision.HIGHEST).astype(jnp.bfloat16)
    block_width = D // N_COL

    def accumulate(running, block_index):
        offset = block_index * block_width
        mixed_part = lax.dynamic_slice_in_dim(mixed_bond, offset, block_width, 3)
        right_part = lax.dynamic_slice_in_dim(right_env, offset, block_width, 1)
        partial_value = jnp.einsum('vsab,vbc->sac', mixed_part.astype(jnp.float32), right_part.astype(jnp.float32), precision=lax.Precision.HIGHEST)
        partial_value = lax.optimization_barrier(partial_value.astype(jnp.bfloat16)).astype(jnp.float32)
        return (running + partial_value, None)
    initial = jnp.zeros((vector.shape[0], D, D), jnp.float32)
    result, unused = lax.scan(accumulate, initial, jnp.arange(N_COL, dtype=jnp.int32))
    return result

def reference(start_vector, left_env, right_env, left_tensor, right_tensor):
    epsilon = 1e-06
    coupling_table = coupling(left_tensor, right_tensor)
    base_vector = start_vector.astype(jnp.float32)
    image = apply_hamiltonian(start_vector, coupling_table, left_env, right_env)
    base_square = jnp.mean(base_vector * base_vector)
    alpha = jnp.mean(base_vector * image) / (base_square + epsilon)
    residual = image - alpha * base_vector
    rho = jnp.sqrt(jnp.mean(residual * residual) + epsilon)
    next_vector = (residual / rho).astype(jnp.bfloat16)
    coefficients = jnp.stack([alpha, rho]).astype(jnp.float32)
    return (next_vector, coefficients)
```

```python
import jax
import jax.numpy as jnp
from jax import lax
from jax.experimental import pallas as pl
from jax.experimental.pallas import tpu as pltpu
from jax.sharding import Mesh
from jax.sharding import PartitionSpec as P

X, Y, Z, C = "row_0", "row_1", "col_0", "col_1"
ROW = (X, Y)
COL = (Z, C)
STATES = 4
CHANNELS = 5

epsilon = 1e-06
SCALE = 8192.0


def coupling(left_tensor, right_tensor):
    channels = left_tensor.shape[0]
    joined = jnp.einsum(
        "wuac,uvbd->vabwcd", left_tensor, right_tensor, precision=lax.Precision.HIGHEST
    )
    return joined.reshape(channels * STATES, channels * STATES)


def swap_of_cores(x):
    n, rows, cols = x.shape
    halves = jnp.moveaxis(x.reshape(n, 2, rows // 2, cols), 1, 0)
    halves = lax.all_to_all(halves, C, 0, 0, tiled=True)
    return jnp.moveaxis(halves, 0, 2).reshape(n, rows // 2, 2 * cols)


def other_core(x):
    return lax.ppermute(x, C, [(0, 1), (1, 0)])


def kernel(core_ref, table_ref, left_ref, own_ref, other_ref, out_ref, left_s, vec_s, right_s, cross_s, mixed_s):
    blocks, rows, width = out_ref.shape
    half = rows // STATES
    core = core_ref[0]
    own_at = pl.multiple_of(core * half, half)
    other_at = pl.multiple_of((1 - core) * half, half)
    for r in range(blocks):
        left_s[:, r * width : (r + 1) * width] = left_ref[r]
        for source, at in ((own_ref, own_at), (other_ref, other_at)):
            for t in range(STATES):
                vec_s[pl.ds(r * width + at, half), t * width : (t + 1) * width] = source[r, t * half : (t + 1) * half, :]
            for v in range(CHANNELS):
                k = (STATES + v) * half
                right_s[pl.ds(v * width + at, half), r * width : (r + 1) * width] = source[r, k : k + half, :]
    cross_s[...] = jnp.dot(left_s[...], vec_s[...], preferred_element_type=jnp.float32)
    for v in range(CHANNELS):
        for s in range(STATES):
            total = None
            for w in range(CHANNELS):
                for t in range(STATES):
                    part = (
                        table_ref[v * STATES + s, w * STATES + t]
                        * cross_s[w * half : (w + 1) * half, t * width : (t + 1) * width]
                    )
                    total = part if total is None else total + part
            mixed_s[s * half : (s + 1) * half, v * width : (v + 1) * width] = total.astype(jnp.bfloat16)
    for j in range(blocks // 2):
        image = jnp.dot(
            mixed_s[...], right_s[:, 2 * j * width : 2 * (j + 1) * width], preferred_element_type=jnp.float32
        ).astype(jnp.bfloat16)
        out_ref[2 * j] = image[:, :width]
        out_ref[2 * j + 1] = image[:, width:]


def terms(core, table, left, own, other):
    blocks, left_rows, width = left.shape
    half = left_rows // CHANNELS
    rows = STATES * half
    vmem = pl.BlockSpec(memory_space=pltpu.VMEM)
    smem = pl.BlockSpec(memory_space=pltpu.SMEM)
    return pl.pallas_call(
        kernel,
        out_shape=jax.ShapeDtypeStruct((blocks, rows, width), jnp.bfloat16),
        in_specs=[smem, smem, vmem, vmem, vmem],
        out_specs=vmem,
        scratch_shapes=[
            pltpu.VMEM((left_rows, blocks * width), jnp.bfloat16),
            pltpu.VMEM((blocks * width, STATES * width), jnp.bfloat16),
            pltpu.VMEM((CHANNELS * width, blocks * width), jnp.bfloat16),
            pltpu.VMEM((left_rows, STATES * width), jnp.float32),
            pltpu.VMEM((rows, CHANNELS * width), jnp.bfloat16),
        ],
        compiler_params=pltpu.CompilerParams(vmem_limit_bytes=40 * 1024 * 1024),
    )(core, table, left, own, other)


def summed(x, axes):
    size = lax.axis_size(axes)
    pieces = lax.all_to_all(jnp.broadcast_to(x[None], (size, *x.shape)), axes, 0, 0, tiled=True)
    return jnp.sum(pieces, 0)


def body(start_vector, left_env, right_env, left_tensor, right_tensor):
    n_row = lax.axis_size(ROW)
    n_z = lax.axis_size(Z)
    _, rows, cols = start_vector.shape
    half = rows // 2
    entries = float(STATES * rows * cols * n_row * n_z * lax.axis_size(C))
    core = lax.axis_index(C).astype(jnp.int32)
    table = coupling(left_tensor, right_tensor)

    both = swap_of_cores(jnp.concatenate([start_vector, left_env], 0))
    vector = both[:STATES]
    left = (both[STATES:].astype(jnp.float32) * SCALE).astype(jnp.float16)

    mine = jnp.concatenate([vector, right_env], 0).reshape(1, (STATES + CHANNELS) * half, 2 * cols)
    own = lax.all_to_all(jnp.broadcast_to(mine, (n_row, *mine.shape[1:])), ROW, 0, 0, tiled=True)
    left = lax.all_gather(left.reshape(CHANNELS * half, 2 * cols), Z, axis=0)
    own, left = lax.optimization_barrier((own, left))
    left = (left.astype(jnp.float32) * (1.0 / SCALE)).astype(jnp.bfloat16)
    other = other_core(own)

    sent = terms(core.reshape(1), table, left, own, other)
    pieces = lax.all_to_all(sent, Z, 0, 0, tiled=True)
    image = jnp.sum(pieces.astype(jnp.float32), 0).reshape(STATES, half, 2, cols)

    base = vector.astype(jnp.float32).reshape(STATES, half, 2, cols)
    sums = jnp.stack([jnp.sum(base * base), jnp.sum(base * image), jnp.sum(image * image)]) / entries
    sums = jnp.broadcast_to(sums[:, None, None], (3, 1, 128))
    sums = summed(summed(sums, (X, Y, C)), Z)[:, 0, 0]
    base_square, correlation, image_square = sums[0], sums[1], sums[2]

    kept = jnp.where(core == 0, image[:, :, 0], image[:, :, 1])
    received = other_core(jnp.where(core == 0, image[:, :, 1], image[:, :, 0]))
    image = jnp.where(
        core == 0, jnp.concatenate([kept, received], 1), jnp.concatenate([received, kept], 1)
    )
    alpha = correlation / (base_square + epsilon)
    residual = image - alpha * start_vector.astype(jnp.float32)
    rho = jnp.sqrt(image_square - 2.0 * alpha * correlation + alpha * alpha * base_square + epsilon)
    return (residual / rho).astype(jnp.bfloat16), jnp.stack([alpha, rho])


def solution(mesh):
    finer = Mesh(mesh.devices.reshape(4, 4, 16, 2), (X, Y, Z, C))
    in_specs = (P(None, ROW, COL), P(None, ROW, COL), P(None, COL, ROW), P(), P())
    out_specs = (P(None, ROW, COL), P())
    return jax.shard_map(body, mesh=finer, in_specs=in_specs, out_specs=out_specs, check_vma=False)
```

```python
import jax
import jax.numpy as jnp
from jax import lax
from jax.experimental import pallas as pl
from jax.experimental.pallas import tpu as pltpu
from jax.sharding import Mesh
from jax.sharding import PartitionSpec as P

X, Y, Z, C = "row_0", "row_1", "col_0", "col_1"
ROW = (X, Y)
COL = (Z, C)
STATES = 4
CHANNELS = 5
PAIRS = STATES * CHANNELS

epsilon = 1e-06
SCALE = 8192.0

VMEM = pl.BlockSpec(memory_space=pltpu.VMEM)
SMEM = pl.BlockSpec(memory_space=pltpu.SMEM)
PARAMS = pltpu.CompilerParams(vmem_limit_bytes=48 * 1024 * 1024)


def coupling(left_tensor, right_tensor):
    joined = jnp.einsum(
        "wuac,uvbd->vabwcd", left_tensor, right_tensor, precision=lax.Precision.HIGHEST
    )
    return joined.reshape(PAIRS, PAIRS)


def pack_kernel(vector_ref, right_ref, out_ref):
    states, half, width = vector_ref.shape
    for r in range(out_ref.shape[0]):
        for t in range(states):
            out_ref[r, t * half : (t + 1) * half, :] = vector_ref[t]
    for v in range(right_ref.shape[0]):
        turned = right_ref[v].astype(jnp.float32).T
        turned = jnp.concatenate([turned[:half], turned[half:]], 1).astype(jnp.bfloat16)
        at = (states + v) * half
        for r in range(out_ref.shape[0]):
            out_ref[r, at : at + half, :] = turned


def pack(vector, right, size):
    states, half, width = vector.shape
    rows = (states + right.shape[0]) * half
    return pl.pallas_call(
        pack_kernel,
        out_shape=jax.ShapeDtypeStruct((size, rows, width), jnp.bfloat16),
        in_specs=[VMEM, VMEM],
        out_specs=VMEM,
        compiler_params=PARAMS,
    )(vector, right)


def terms_kernel(core_ref, table_ref, left_own, left_other, own_ref, other_ref, out_ref, vec_s, left_s, right_s, cross_s, mixed_s):
    blocks, half, _ = out_ref.shape
    width = 2 * half
    core = core_ref[0]
    own_at = pl.multiple_of(core * half, half)
    other_at = pl.multiple_of((1 - core) * half, half)
    for r in range(blocks):
        for source, left, at in ((own_ref, left_own, own_at), (other_ref, left_other, other_at)):
            for t in range(STATES):
                vec_s[pl.ds(t * width + at, half), r * width : (r + 1) * width] = source[r, t * half : (t + 1) * half, :]
            for w in range(CHANNELS):
                left_s[pl.ds(r * width + at, half), w * width : (w + 1) * width] = left[r, w * half : (w + 1) * half, :]
    cross_s[...] = jnp.dot(vec_s[...], left_s[...], preferred_element_type=jnp.float32)
    for v in range(CHANNELS):
        for s in range(STATES):
            total = None
            for w in range(CHANNELS):
                for t in range(STATES):
                    part = (
                        table_ref[v * STATES + s, w * STATES + t]
                        * cross_s[t * width : (t + 1) * width, w * width : (w + 1) * width]
                    )
                    total = part if total is None else total + part
            mixed_s[v * width : (v + 1) * width, s * width : (s + 1) * width] = total.astype(jnp.bfloat16)
    mine = lax.broadcasted_iota(jnp.int32, (half, width), 1) // half == core
    for r in range(blocks):
        for v in range(CHANNELS):
            at = (STATES + v) * half
            own = own_ref[r, at : at + half, :].astype(jnp.float32)
            other = other_ref[r, at : at + half, :].astype(jnp.float32)
            other = jnp.concatenate([other[:, half:], other[:, :half]], 1)
            right_s[r * half : (r + 1) * half, v * width : (v + 1) * width] = jnp.where(mine, own, other).astype(jnp.bfloat16)
    image = jnp.dot(right_s[...], mixed_s[...], preferred_element_type=jnp.float32)
    for r in range(blocks):
        out_ref[r] = image[r * half : (r + 1) * half].astype(jnp.bfloat16)


def terms(core, table, left_own, left_other, own, other):
    blocks, left_rows, width = left_own.shape
    half = left_rows // CHANNELS
    return pl.pallas_call(
        terms_kernel,
        out_shape=jax.ShapeDtypeStruct((blocks, half, STATES * width), jnp.bfloat16),
        in_specs=[SMEM, SMEM, VMEM, VMEM, VMEM, VMEM],
        out_specs=VMEM,
        scratch_shapes=[
            pltpu.VMEM((STATES * width, blocks * width), jnp.bfloat16),
            pltpu.VMEM((blocks * width, CHANNELS * width), jnp.bfloat16),
            pltpu.VMEM((blocks * half, CHANNELS * width), jnp.bfloat16),
            pltpu.VMEM((STATES * width, CHANNELS * width), jnp.float32),
            pltpu.VMEM((CHANNELS * width, STATES * width), jnp.bfloat16),
        ],
        compiler_params=PARAMS,
    )(core, table, left_own, left_other, own, other)


def lanes_of(total):
    rows, cols = total.shape
    total = sum(total[:, k : k + 128] for k in range(0, cols, 128))
    return sum(total[k : k + 8] for k in range(0, rows, 8))


def sums_kernel(pieces_ref, vector_ref, image_ref, sums_ref):
    image = pieces_ref[0].astype(jnp.float32)
    for k in range(1, pieces_ref.shape[0]):
        image = image + pieces_ref[k].astype(jnp.float32)
    image_ref[...] = image
    base = jnp.concatenate([vector_ref[t].astype(jnp.float32) for t in range(STATES)], 1)
    found = [lanes_of(base * base), lanes_of(base * image), lanes_of(image * image)]
    found = [jnp.broadcast_to(jnp.sum(f, keepdims=True), (1, 128)) for f in found]
    found = jnp.concatenate([*found, jnp.zeros((5, 128), jnp.float32)], 0)
    for r in range(sums_ref.shape[0]):
        sums_ref[r] = found


def sums_of(pieces, vector, size):
    return pl.pallas_call(
        sums_kernel,
        out_shape=(
            jax.ShapeDtypeStruct(pieces.shape[1:], jnp.float32),
            jax.ShapeDtypeStruct((size, 8, 128), jnp.float32),
        ),
        in_specs=[VMEM, VMEM],
        out_specs=(VMEM, VMEM),
        compiler_params=PARAMS,
    )(pieces, vector)


def again_kernel(pieces_ref, out_ref):
    total = pieces_ref[0]
    for k in range(1, pieces_ref.shape[0]):
        total = total + pieces_ref[k]
    for r in range(out_ref.shape[0]):
        out_ref[r] = total


def again(pieces, size):
    return pl.pallas_call(
        again_kernel,
        out_shape=jax.ShapeDtypeStruct((size, *pieces.shape[1:]), jnp.float32),
        in_specs=[VMEM],
        out_specs=VMEM,
        compiler_params=PARAMS,
    )(pieces)


def last_kernel(entries, pieces_ref, image_ref, vector_ref, next_ref, coefficients_ref):
    total = pieces_ref[0]
    for k in range(1, pieces_ref.shape[0]):
        total = total + pieces_ref[k]
    total = total / entries
    base_square, correlation, image_square = total[0:1], total[1:2], total[2:3]
    alpha = correlation / (base_square + epsilon)
    rho = jnp.sqrt(image_square - 2.0 * alpha * correlation + alpha * alpha * base_square + epsilon)
    width = next_ref.shape[2]
    for t in range(STATES):
        residual = image_ref[:, t * width : (t + 1) * width] - alpha * vector_ref[t].astype(jnp.float32)
        next_ref[t] = (residual / rho).astype(jnp.bfloat16)
    coefficients_ref[0] = alpha[0, 0]
    coefficients_ref[1] = rho[0, 0]


def last(entries, pieces, image, vector):
    def step(*refs):
        last_kernel(entries, *refs)

    return pl.pallas_call(
        step,
        out_shape=(
            jax.ShapeDtypeStruct(vector.shape, jnp.bfloat16),
            jax.ShapeDtypeStruct((2,), jnp.float32),
        ),
        in_specs=[VMEM, VMEM, VMEM],
        out_specs=(VMEM, SMEM),
        compiler_params=PARAMS,
    )(pieces, image, vector)


def all_to_all(x, axes):
    return lax.all_to_all(x, axes, 0, 0, tiled=True)


def other_core(x):
    return lax.ppermute(x, C, [(0, 1), (1, 0)])


def body(start_vector, left_env, right_env, left_tensor, right_tensor):
    n_row = lax.axis_size(ROW)
    n_z = lax.axis_size(Z)
    _, rows, half = start_vector.shape
    entries = float(STATES * rows * half * n_row * n_z * lax.axis_size(C))
    core = lax.axis_index(C).astype(jnp.int32).reshape(1)
    table = coupling(left_tensor, right_tensor)
    vector = jnp.swapaxes(start_vector, 1, 2)
    left = jnp.swapaxes(left_env, 1, 2).reshape(CHANNELS * half, rows)
    left = (left.astype(jnp.float32) * SCALE).astype(jnp.float16)

    own = all_to_all(pack(vector, right_env, n_row), ROW)
    left = lax.all_gather(left, Z, axis=0)
    own, left = lax.optimization_barrier((own, left))
    left = (left.astype(jnp.float32) * (1.0 / SCALE)).astype(jnp.bfloat16)
    sent = terms(core, table, left, other_core(left), own, other_core(own))

    pieces = all_to_all(sent, Z)
    image, sums = sums_of(pieces, vector, lax.axis_size((X, Y, C)))
    sums = again(all_to_all(sums, (X, Y, C)), n_z)
    next_vector, coefficients = last(entries, all_to_all(sums, Z), image, vector)
    return jnp.swapaxes(next_vector, 1, 2), coefficients


def solution(mesh):
    finer = Mesh(mesh.devices.reshape(4, 4, 16, 2), (X, Y, Z, C))
    in_specs = (P(None, ROW, COL), P(None, ROW, COL), P(None, COL, ROW), P(), P())
    out_specs = (P(None, ROW, COL), P())
    return jax.shard_map(body, mesh=finer, in_specs=in_specs, out_specs=out_specs, check_vma=False)
```

```python
import jax
import jax.numpy as jnp
from jax import lax
from jax.experimental import pallas as pl
from jax.experimental.pallas import tpu as pltpu
from jax.sharding import Mesh
from jax.sharding import PartitionSpec as P

X, Y, Z, C = "row_0", "row_1", "col_0", "col_1"
ROW = (X, Y)
COL = (Z, C)
STATES = 4
CHANNELS = 5
PAIRS = STATES * CHANNELS

epsilon = 1e-06
SCALE = 8192.0

VMEM = pl.BlockSpec(memory_space=pltpu.VMEM)
SMEM = pl.BlockSpec(memory_space=pltpu.SMEM)
SMALL = pltpu.CompilerParams(vmem_limit_bytes=4 * 1024 * 1024)
LARGE = pltpu.CompilerParams(vmem_limit_bytes=24 * 1024 * 1024)


def coupling(left_tensor, right_tensor):
    joined = jnp.einsum("wuac,uvbd->vabwcd", left_tensor, right_tensor, precision=lax.Precision.HIGHEST)
    return joined.reshape(PAIRS, PAIRS)


def pack_kernel(vector_hbm, right_hbm, out_hbm, vector_s, right_s, piece_s, in_sems, out_sems):
    states, half, width = vector_s.shape
    rights = right_s.shape[0]
    loads = [
        pltpu.make_async_copy(vector_hbm, vector_s, in_sems.at[0]),
        pltpu.make_async_copy(right_hbm, right_s, in_sems.at[1]),
    ]
    for load in loads:
        load.start()
    loads[0].wait()
    for t in range(states):
        piece_s[t * half : (t + 1) * half, :] = vector_s[t]
    loads[1].wait()
    for v in range(rights):
        turned = right_s[v].astype(jnp.float32).T
        turned = jnp.concatenate([turned[:half], turned[half:]], 1).astype(jnp.bfloat16)
        piece_s[(states + v) * half : (states + v + 1) * half, :] = turned
    stores = [pltpu.make_async_copy(piece_s, out_hbm.at[r], out_sems.at[r]) for r in range(out_hbm.shape[0])]
    for store in stores:
        store.start()
    for store in stores:
        store.wait()


def pack(vector, right, size):
    states, half, width = vector.shape
    rows = (states + right.shape[0]) * half
    hbm = pl.BlockSpec(memory_space=pltpu.HBM)
    return pl.pallas_call(
        pack_kernel,
        out_shape=pltpu.HBM((size, rows, width), jnp.bfloat16),
        in_specs=[hbm, hbm],
        out_specs=hbm,
        scratch_shapes=[
            pltpu.VMEM(vector.shape, jnp.bfloat16),
            pltpu.VMEM(right.shape, jnp.bfloat16),
            pltpu.VMEM((rows, width), jnp.bfloat16),
            pltpu.SemaphoreType.DMA((2,)),
            pltpu.SemaphoreType.DMA((size,)),
        ],
        compiler_params=SMALL,
    )(pltpu.with_memory_space_constraint(vector, pltpu.HBM), pltpu.with_memory_space_constraint(right, pltpu.HBM))


def terms_kernel(core_ref, table_ref, left_ref, own_ref, other_ref, out_ref, vec_s, left_s, right_s, cross_s, mixed_s):
    blocks, half, _ = out_ref.shape
    width = 2 * half
    core = core_ref[0]
    own_at = pl.multiple_of(core * half, half)
    other_at = pl.multiple_of((1 - core) * half, half)
    for r in range(blocks):
        for source, at in ((own_ref, own_at), (other_ref, other_at)):
            for t in range(STATES):
                vec_s[pl.ds(t * width + at, half), r * width : (r + 1) * width] = source[r, t * half : (t + 1) * half, :]
    for r in range(left_ref.shape[0]):
        for w in range(CHANNELS):
            left_s[r * half : (r + 1) * half, w * width : (w + 1) * width] = left_ref[r, w * half : (w + 1) * half, :]
    cross_s[...] = jnp.dot(vec_s[...], left_s[...], preferred_element_type=jnp.float32)
    for v in range(CHANNELS):
        for s in range(STATES):
            total = None
            for w in range(CHANNELS):
                for t in range(STATES):
                    part = (
                        table_ref[v * STATES + s, w * STATES + t]
                        * cross_s[t * width : (t + 1) * width, w * width : (w + 1) * width]
                    )
                    total = part if total is None else total + part
            mixed_s[v * width : (v + 1) * width, s * width : (s + 1) * width] = total.astype(jnp.bfloat16)
    mine = lax.broadcasted_iota(jnp.int32, (half, width), 1) // half == core
    for r in range(blocks):
        for v in range(CHANNELS):
            at = (STATES + v) * half
            own = own_ref[r, at : at + half, :].astype(jnp.float32)
            other = other_ref[r, at : at + half, :].astype(jnp.float32)
            other = jnp.concatenate([other[:, half:], other[:, :half]], 1)
            right_s[r * half : (r + 1) * half, v * width : (v + 1) * width] = jnp.where(mine, own, other).astype(jnp.bfloat16)
    image = jnp.dot(right_s[...], mixed_s[...], preferred_element_type=jnp.float32)
    for r in range(blocks):
        out_ref[r] = image[r * half : (r + 1) * half].astype(jnp.bfloat16)


def terms(core, table, left, own, other):
    blocks, rows, width = own.shape
    half = rows // (STATES + CHANNELS)
    return pl.pallas_call(
        terms_kernel,
        out_shape=jax.ShapeDtypeStruct((blocks, half, STATES * width), jnp.bfloat16),
        in_specs=[SMEM, SMEM, VMEM, VMEM, VMEM],
        out_specs=VMEM,
        scratch_shapes=[
            pltpu.VMEM((STATES * width, blocks * width), jnp.bfloat16),
            pltpu.VMEM((blocks * width, CHANNELS * width), jnp.bfloat16),
            pltpu.VMEM((blocks * half, CHANNELS * width), jnp.bfloat16),
            pltpu.VMEM((STATES * width, CHANNELS * width), jnp.float32),
            pltpu.VMEM((CHANNELS * width, STATES * width), jnp.bfloat16),
        ],
        compiler_params=LARGE,
    )(core, table, left, own, other)


def lanes_of(total):
    rows, cols = total.shape
    total = sum(total[:, k : k + 128] for k in range(0, cols, 128))
    return sum(total[k : k + 8] for k in range(0, rows, 8))


def sums_kernel(pieces_ref, vector_ref, image_ref, sums_ref):
    image = pieces_ref[0].astype(jnp.float32)
    for k in range(1, pieces_ref.shape[0]):
        image = image + pieces_ref[k].astype(jnp.float32)
    image_ref[...] = image
    base = jnp.concatenate([vector_ref[t].astype(jnp.float32) for t in range(STATES)], 1)
    found = [lanes_of(base * base), lanes_of(base * image), lanes_of(image * image)]
    found = [jnp.broadcast_to(jnp.sum(f, keepdims=True), (1, 128)) for f in found]
    found = jnp.concatenate([*found, jnp.zeros((5, 128), jnp.float32)], 0)
    for r in range(sums_ref.shape[0]):
        sums_ref[r] = found


def sums_of(pieces, vector, size):
    return pl.pallas_call(
        sums_kernel,
        out_shape=(
            jax.ShapeDtypeStruct(pieces.shape[1:], jnp.float32),
            jax.ShapeDtypeStruct((size, 8, 128), jnp.float32),
        ),
        in_specs=[VMEM, VMEM],
        out_specs=(VMEM, VMEM),
        compiler_params=SMALL,
    )(pieces, vector)


def again_kernel(pieces_ref, out_ref):
    total = pieces_ref[0]
    for k in range(1, pieces_ref.shape[0]):
        total = total + pieces_ref[k]
    for r in range(out_ref.shape[0]):
        out_ref[r] = total


def again(pieces, size):
    return pl.pallas_call(
        again_kernel,
        out_shape=jax.ShapeDtypeStruct((size, *pieces.shape[1:]), jnp.float32),
        in_specs=[VMEM],
        out_specs=VMEM,
        compiler_params=SMALL,
    )(pieces)


def last_kernel(entries, pieces_ref, image_ref, vector_ref, next_ref, coefficients_ref):
    total = pieces_ref[0]
    for k in range(1, pieces_ref.shape[0]):
        total = total + pieces_ref[k]
    total = total / entries
    base_square, correlation, image_square = total[0:1], total[1:2], total[2:3]
    alpha = correlation / (base_square + epsilon)
    rho = jnp.sqrt(image_square - 2.0 * alpha * correlation + alpha * alpha * base_square + epsilon)
    width = next_ref.shape[2]
    for t in range(STATES):
        residual = image_ref[:, t * width : (t + 1) * width] - alpha * vector_ref[t].astype(jnp.float32)
        next_ref[t] = (residual / rho).astype(jnp.bfloat16)
    coefficients_ref[0] = alpha[0, 0]
    coefficients_ref[1] = rho[0, 0]


def last(entries, pieces, image, vector):
    def step(*refs):
        last_kernel(entries, *refs)

    return pl.pallas_call(
        step,
        out_shape=(
            jax.ShapeDtypeStruct(vector.shape, jnp.bfloat16),
            jax.ShapeDtypeStruct((2,), jnp.float32),
        ),
        in_specs=[VMEM, VMEM, VMEM],
        out_specs=(VMEM, SMEM),
        compiler_params=SMALL,
    )(pieces, image, vector)


def all_to_all(x, axes):
    return lax.all_to_all(x, axes, 0, 0, tiled=True)


def other_core(x):
    return lax.ppermute(x, C, [(0, 1), (1, 0)])


def body(start_vector, left_env, right_env, left_tensor, right_tensor):
    n_row = lax.axis_size(ROW)
    n_z = lax.axis_size(Z)
    _, rows, half = start_vector.shape
    entries = float(STATES * rows * half * n_row * n_z * lax.axis_size(C))
    core = lax.axis_index(C).astype(jnp.int32).reshape(1)
    table = coupling(left_tensor, right_tensor)
    vector = jnp.swapaxes(start_vector, 1, 2)
    left = jnp.swapaxes(left_env, 1, 2).reshape(CHANNELS * half, rows)
    left = (left.astype(jnp.float32) * SCALE).astype(jnp.float16)

    own = all_to_all(pack(vector, right_env, n_row), ROW)
    left = lax.all_gather(left, COL, axis=0)
    own, left = lax.optimization_barrier((own, left))
    left = (left.astype(jnp.float32) * (1.0 / SCALE)).astype(jnp.bfloat16)
    sent = terms(core, table, left, own, other_core(own))

    pieces = all_to_all(sent, Z)
    image, sums = sums_of(pieces, vector, lax.axis_size((X, Y, C)))
    sums = again(all_to_all(sums, (X, Y, C)), n_z)
    next_vector, coefficients = last(entries, all_to_all(sums, Z), image, vector)
    return jnp.swapaxes(next_vector, 1, 2), coefficients


def solution(mesh):
    finer = Mesh(mesh.devices.reshape(4, 4, 16, 2), (X, Y, Z, C))
    in_specs = (P(None, ROW, COL), P(None, ROW, COL), P(None, COL, ROW), P(), P())
    out_specs = (P(None, ROW, COL), P())
    return jax.shard_map(body, mesh=finer, in_specs=in_specs, out_specs=out_specs, check_vma=False)
```

```python
import jax
import jax.numpy as jnp
from jax import lax
from jax.experimental import pallas as pl
from jax.experimental.pallas import tpu as pltpu
from jax.sharding import Mesh
from jax.sharding import PartitionSpec as P

X, Y, FAR, NEAR, C = "row_0", "row_1", "far", "near", "core"
ROW = (X, Y)
Z = (FAR, NEAR)
COL = (FAR, NEAR, C)
STATES = 4
CHANNELS = 5
PAIRS = STATES * CHANNELS

epsilon = 1e-06
SCALE = 8192.0

VMEM = pl.BlockSpec(memory_space=pltpu.VMEM)
SMEM = pl.BlockSpec(memory_space=pltpu.SMEM)
SMALL = pltpu.CompilerParams(vmem_limit_bytes=4 * 1024 * 1024)
LARGE = pltpu.CompilerParams(vmem_limit_bytes=24 * 1024 * 1024)


def coupling(left_tensor, right_tensor):
    joined = jnp.einsum("wuac,uvbd->vabwcd", left_tensor, right_tensor, precision=lax.Precision.HIGHEST)
    return joined.reshape(PAIRS, PAIRS)


def pack_kernel(vector_hbm, right_hbm, out_hbm, vector_s, right_s, piece_s, in_sems, out_sems):
    states, half, width = vector_s.shape
    rights = right_s.shape[0]
    loads = [
        pltpu.make_async_copy(vector_hbm, vector_s, in_sems.at[0]),
        pltpu.make_async_copy(right_hbm, right_s, in_sems.at[1]),
    ]
    for load in loads:
        load.start()
    loads[0].wait()
    for t in range(states):
        piece_s[t * half : (t + 1) * half, :] = vector_s[t]
    loads[1].wait()
    for v in range(rights):
        turned = right_s[v].astype(jnp.float32).T
        turned = jnp.concatenate([turned[:half], turned[half:]], 1).astype(jnp.bfloat16)
        piece_s[(states + v) * half : (states + v + 1) * half, :] = turned
    stores = [pltpu.make_async_copy(piece_s, out_hbm.at[r], out_sems.at[r]) for r in range(out_hbm.shape[0])]
    for store in stores:
        store.start()
    for store in stores:
        store.wait()


def pack(vector, right, size):
    states, half, width = vector.shape
    rows = (states + right.shape[0]) * half
    hbm = pl.BlockSpec(memory_space=pltpu.HBM)
    return pl.pallas_call(
        pack_kernel,
        out_shape=pltpu.HBM((size, rows, width), jnp.bfloat16),
        in_specs=[hbm, hbm],
        out_specs=hbm,
        scratch_shapes=[
            pltpu.VMEM(vector.shape, jnp.bfloat16),
            pltpu.VMEM(right.shape, jnp.bfloat16),
            pltpu.VMEM((rows, width), jnp.bfloat16),
            pltpu.SemaphoreType.DMA((2,)),
            pltpu.SemaphoreType.DMA((size,)),
        ],
        compiler_params=SMALL,
    )(pltpu.with_memory_space_constraint(vector, pltpu.HBM), pltpu.with_memory_space_constraint(right, pltpu.HBM))


def terms_kernel(order, core_ref, table_ref, left_ref, own_ref, other_ref, out_ref, vec_s, left_s, right_s, cross_s, mixed_s):
    blocks, half, _ = out_ref.shape
    width = 2 * half
    core = core_ref[0]
    own_at = pl.multiple_of(core * half, half)
    other_at = pl.multiple_of((1 - core) * half, half)
    for r in range(blocks):
        for source, at in ((own_ref, own_at), (other_ref, other_at)):
            for t in range(STATES):
                vec_s[pl.ds(t * width + at, half), r * width : (r + 1) * width] = source[r, t * half : (t + 1) * half, :]
    for r in range(left_ref.shape[0]):
        for w in range(CHANNELS):
            left_s[r * half : (r + 1) * half, w * width : (w + 1) * width] = left_ref[r, w * half : (w + 1) * half, :]
    cross_s[...] = jnp.dot(vec_s[...], left_s[...], preferred_element_type=jnp.float32)
    for v in range(CHANNELS):
        for s in range(STATES):
            total = None
            for w in range(CHANNELS):
                for t in range(STATES):
                    part = (
                        table_ref[v * STATES + s, w * STATES + t]
                        * cross_s[t * width : (t + 1) * width, w * width : (w + 1) * width]
                    )
                    total = part if total is None else total + part
            mixed_s[v * width : (v + 1) * width, s * width : (s + 1) * width] = total.astype(jnp.bfloat16)
    mine = lax.broadcasted_iota(jnp.int32, (half, width), 1) // half == core
    for r in range(blocks):
        for v in range(CHANNELS):
            at = (STATES + v) * half
            own = own_ref[r, at : at + half, :].astype(jnp.float32)
            other = other_ref[r, at : at + half, :].astype(jnp.float32)
            other = jnp.concatenate([other[:, half:], other[:, :half]], 1)
            right_s[r * half : (r + 1) * half, v * width : (v + 1) * width] = jnp.where(mine, own, other).astype(jnp.bfloat16)
    image = jnp.dot(right_s[...], mixed_s[...], preferred_element_type=jnp.float32)
    for r in range(blocks):
        out_ref[order[r]] = image[r * half : (r + 1) * half].astype(jnp.bfloat16)


def terms(order, core, table, left, own, other):
    def step(*refs):
        terms_kernel(order, *refs)

    blocks, rows, width = own.shape
    half = rows // (STATES + CHANNELS)
    return pl.pallas_call(
        step,
        out_shape=jax.ShapeDtypeStruct((blocks, half, STATES * width), jnp.bfloat16),
        in_specs=[SMEM, SMEM, VMEM, VMEM, VMEM],
        out_specs=VMEM,
        scratch_shapes=[
            pltpu.VMEM((STATES * width, blocks * width), jnp.bfloat16),
            pltpu.VMEM((blocks * width, CHANNELS * width), jnp.bfloat16),
            pltpu.VMEM((blocks * half, CHANNELS * width), jnp.bfloat16),
            pltpu.VMEM((STATES * width, CHANNELS * width), jnp.float32),
            pltpu.VMEM((CHANNELS * width, STATES * width), jnp.bfloat16),
        ],
        compiler_params=LARGE,
    )(core, table, left, own, other)


def near_kernel(pieces_ref, out_ref):
    for j in range(out_ref.shape[0]):
        total = pieces_ref[0, j].astype(jnp.float32)
        for k in range(1, pieces_ref.shape[0]):
            total = total + pieces_ref[k, j].astype(jnp.float32)
        out_ref[j] = total.astype(jnp.bfloat16)


def near_sum(pieces):
    return pl.pallas_call(
        near_kernel,
        out_shape=jax.ShapeDtypeStruct(pieces.shape[1:], jnp.bfloat16),
        in_specs=[VMEM],
        out_specs=VMEM,
        compiler_params=SMALL,
    )(pieces)


def neighbours(n_far, n_near):
    n_z = n_far * n_near
    groups = []
    for core in range(2):
        for j in range(n_far):
            first = j * n_near + core * (n_near // 2)
            chips = sorted(((first + i) % n_z for i in range(n_near)), key=lambda z: z % n_near)
            groups.append([2 * z + core for z in chips])
    return groups


def lanes_of(total):
    rows, cols = total.shape
    total = sum(total[:, k : k + 128] for k in range(0, cols, 128))
    return sum(total[k : k + 8] for k in range(0, rows, 8))


def sums_kernel(pieces_ref, vector_ref, image_ref, sums_ref):
    image = pieces_ref[0].astype(jnp.float32)
    for k in range(1, pieces_ref.shape[0]):
        image = image + pieces_ref[k].astype(jnp.float32)
    image_ref[...] = image
    base = jnp.concatenate([vector_ref[t].astype(jnp.float32) for t in range(STATES)], 1)
    found = [lanes_of(base * base), lanes_of(base * image), lanes_of(image * image)]
    found = [jnp.broadcast_to(jnp.sum(f, keepdims=True), (1, 128)) for f in found]
    found = jnp.concatenate([*found, jnp.zeros((5, 128), jnp.float32)], 0)
    for r in range(sums_ref.shape[0]):
        sums_ref[r] = found


def sums_of(pieces, vector, size):
    return pl.pallas_call(
        sums_kernel,
        out_shape=(
            jax.ShapeDtypeStruct(pieces.shape[1:], jnp.float32),
            jax.ShapeDtypeStruct((size, 8, 128), jnp.float32),
        ),
        in_specs=[VMEM, VMEM],
        out_specs=(VMEM, VMEM),
        compiler_params=SMALL,
    )(pieces, vector)


def again_kernel(pieces_ref, out_ref):
    total = pieces_ref[0]
    for k in range(1, pieces_ref.shape[0]):
        total = total + pieces_ref[k]
    for r in range(out_ref.shape[0]):
        out_ref[r] = total


def again(pieces, size):
    return pl.pallas_call(
        again_kernel,
        out_shape=jax.ShapeDtypeStruct((size, *pieces.shape[1:]), jnp.float32),
        in_specs=[VMEM],
        out_specs=VMEM,
        compiler_params=SMALL,
    )(pieces)


def last_kernel(entries, pieces_ref, image_ref, vector_ref, next_ref, coefficients_ref):
    total = pieces_ref[0]
    for k in range(1, pieces_ref.shape[0]):
        total = total + pieces_ref[k]
    total = total / entries
    base_square, correlation, image_square = total[0:1], total[1:2], total[2:3]
    alpha = correlation / (base_square + epsilon)
    rho = jnp.sqrt(image_square - 2.0 * alpha * correlation + alpha * alpha * base_square + epsilon)
    width = next_ref.shape[2]
    for t in range(STATES):
        residual = image_ref[:, t * width : (t + 1) * width] - alpha * vector_ref[t].astype(jnp.float32)
        next_ref[t] = (residual / rho).astype(jnp.bfloat16)
    coefficients_ref[0] = alpha[0, 0]
    coefficients_ref[1] = rho[0, 0]


def last(entries, pieces, image, vector):
    def step(*refs):
        last_kernel(entries, *refs)

    return pl.pallas_call(
        step,
        out_shape=(
            jax.ShapeDtypeStruct(vector.shape, jnp.bfloat16),
            jax.ShapeDtypeStruct((2,), jnp.float32),
        ),
        in_specs=[VMEM, VMEM, VMEM],
        out_specs=(VMEM, SMEM),
        compiler_params=SMALL,
    )(pieces, image, vector)


def all_to_all(x, axes):
    return lax.all_to_all(x, axes, 0, 0, tiled=True)


def other_core(x):
    return lax.ppermute(x, C, [(0, 1), (1, 0)])


def body(start_vector, left_env, right_env, left_tensor, right_tensor):
    n_row = lax.axis_size(ROW)
    n_far, n_near = lax.axis_size(FAR), lax.axis_size(NEAR)
    n_z = n_far * n_near
    _, rows, half = start_vector.shape
    entries = float(STATES * rows * half * n_row * n_z * lax.axis_size(C))
    core = lax.axis_index(C).astype(jnp.int32).reshape(1)
    table = coupling(left_tensor, right_tensor)
    vector = jnp.swapaxes(start_vector, 1, 2)
    left = jnp.swapaxes(left_env, 1, 2).reshape(CHANNELS * half, rows)
    left = (left.astype(jnp.float32) * SCALE).astype(jnp.float16)

    own = all_to_all(pack(vector, right_env, n_row), ROW)
    left = lax.all_gather(left, COL, axis=0)
    own, left = lax.optimization_barrier((own, left))
    left = (left.astype(jnp.float32) * (1.0 / SCALE)).astype(jnp.bfloat16)
    order = [n_far * (z % n_near) + z // n_near for z in range(n_z)]
    sent = terms(order, core, table, left, own, other_core(own))

    pieces = lax.all_to_all(sent, COL, 0, 0, axis_index_groups=neighbours(n_far, n_near), tiled=True)
    pieces = all_to_all(near_sum(pieces.reshape(n_near, n_far, *pieces.shape[1:])), FAR)
    image, sums = sums_of(pieces, vector, lax.axis_size((X, Y, C)))
    sums = again(all_to_all(sums, (X, Y, C)), n_z)
    next_vector, coefficients = last(entries, all_to_all(sums, Z), image, vector)
    return jnp.swapaxes(next_vector, 1, 2), coefficients


def solution(mesh):
    finer = Mesh(mesh.devices.reshape(4, 4, 4, 4, 2), (X, Y, FAR, NEAR, C))
    in_specs = (P(None, ROW, COL), P(None, ROW, COL), P(None, COL, ROW), P(), P())
    out_specs = (P(None, ROW, COL), P())
    return jax.shard_map(body, mesh=finer, in_specs=in_specs, out_specs=out_specs, check_vma=False)
```

```python
import jax
import jax.numpy as jnp
from jax import lax
from jax.experimental import pallas as pl
from jax.experimental.pallas import tpu as pltpu
from jax.sharding import Mesh
from jax.sharding import PartitionSpec as P

X, Y, FAR, NEAR, C = "row_0", "row_1", "far", "near", "core"
ROW = (X, Y)
Z = (FAR, NEAR)
COL = (FAR, NEAR, C)
STATES = 4
CHANNELS = 5
PAIRS = STATES * CHANNELS

epsilon = 1e-06
SCALE = 8192.0

VMEM = pl.BlockSpec(memory_space=pltpu.VMEM)
SMEM = pl.BlockSpec(memory_space=pltpu.SMEM)
HBM = pl.BlockSpec(memory_space=pltpu.HBM)
SMALL = pltpu.CompilerParams(vmem_limit_bytes=4 * 1024 * 1024)
LARGE = pltpu.CompilerParams(vmem_limit_bytes=32 * 1024 * 1024)


def in_hbm(x):
    return pltpu.with_memory_space_constraint(x, pltpu.HBM)


def coupling(left_tensor, right_tensor):
    joined = jnp.einsum("wuac,uvbd->vabwcd", left_tensor, right_tensor, precision=lax.Precision.HIGHEST)
    return joined.reshape(PAIRS, PAIRS)


def pack_kernel(vector_hbm, right_hbm, out_hbm, vector_s, right_s, piece_s, in_sems, out_sems):
    states, half, width = vector_s.shape
    rights = right_s.shape[0]
    loads = [
        pltpu.make_async_copy(vector_hbm, vector_s, in_sems.at[0]),
        pltpu.make_async_copy(right_hbm, right_s, in_sems.at[1]),
    ]
    for load in loads:
        load.start()
    loads[0].wait()
    for t in range(states):
        piece_s[t * half : (t + 1) * half, :] = vector_s[t]
    loads[1].wait()
    for v in range(rights):
        turned = right_s[v].astype(jnp.float32).T
        turned = jnp.concatenate([turned[:half], turned[half:]], 1).astype(jnp.bfloat16)
        piece_s[(states + v) * half : (states + v + 1) * half, :] = turned
    stores = [pltpu.make_async_copy(piece_s, out_hbm.at[r], out_sems.at[r]) for r in range(out_hbm.shape[0])]
    for store in stores:
        store.start()
    for store in stores:
        store.wait()


def pack(vector, right, size):
    states, half, width = vector.shape
    rows = (states + right.shape[0]) * half
    return pl.pallas_call(
        pack_kernel,
        out_shape=pltpu.HBM((size, rows, width), jnp.bfloat16),
        in_specs=[HBM, HBM],
        out_specs=HBM,
        scratch_shapes=[
            pltpu.VMEM(vector.shape, jnp.bfloat16),
            pltpu.VMEM(right.shape, jnp.bfloat16),
            pltpu.VMEM((rows, width), jnp.bfloat16),
            pltpu.SemaphoreType.DMA((2,)),
            pltpu.SemaphoreType.DMA((size,)),
        ],
        compiler_params=SMALL,
    )(in_hbm(vector), in_hbm(right))


def terms_kernel(order, core_ref, table_ref, left_ref, own_hbm, other_hbm, out_ref, vec_s, left_s, right_s, cross_s, mixed_s, own_ref, other_ref, sems):
    blocks, half, _ = out_ref.shape
    width = 2 * half
    core = core_ref[0]
    own_at = pl.multiple_of(core * half, half)
    other_at = pl.multiple_of((1 - core) * half, half)
    parts = (pl.ds(0, STATES * half), pl.ds(STATES * half, CHANNELS * half))
    copies = [
        [pltpu.make_async_copy(src.at[:, part], dst.at[:, part], sems.at[i, j]) for j, (src, dst) in enumerate(((own_hbm, own_ref), (other_hbm, other_ref)))]
        for i, part in enumerate(parts)
    ]
    for pair in copies:
        for copy in pair:
            copy.start()
    for r in range(left_ref.shape[0]):
        for w in range(CHANNELS):
            left_s[r * half : (r + 1) * half, w * width : (w + 1) * width] = left_ref[r, w * half : (w + 1) * half, :]
    for copy in copies[0]:
        copy.wait()
    for r in range(blocks):
        for source, at in ((own_ref, own_at), (other_ref, other_at)):
            for t in range(STATES):
                vec_s[pl.ds(t * width + at, half), r * width : (r + 1) * width] = source[r, t * half : (t + 1) * half, :]
    cross_s[...] = jnp.dot(vec_s[...], left_s[...], preferred_element_type=jnp.float32)
    for v in range(CHANNELS):
        for s in range(STATES):
            total = None
            for w in range(CHANNELS):
                for t in range(STATES):
                    part = (
                        table_ref[v * STATES + s, w * STATES + t]
                        * cross_s[t * width : (t + 1) * width, w * width : (w + 1) * width]
                    )
                    total = part if total is None else total + part
            mixed_s[v * width : (v + 1) * width, s * width : (s + 1) * width] = total.astype(jnp.bfloat16)
    for copy in copies[1]:
        copy.wait()
    mine = lax.broadcasted_iota(jnp.int32, (half, width), 1) // half == core
    for r in range(blocks):
        for v in range(CHANNELS):
            at = (STATES + v) * half
            own = own_ref[r, at : at + half, :].astype(jnp.float32)
            other = other_ref[r, at : at + half, :].astype(jnp.float32)
            other = jnp.concatenate([other[:, half:], other[:, :half]], 1)
            right_s[r * half : (r + 1) * half, v * width : (v + 1) * width] = jnp.where(mine, own, other).astype(jnp.bfloat16)
    image = jnp.dot(right_s[...], mixed_s[...], preferred_element_type=jnp.float32)
    for r in range(blocks):
        out_ref[order[r]] = image[r * half : (r + 1) * half].astype(jnp.bfloat16)


def terms(order, core, table, left, own, other):
    def step(*refs):
        terms_kernel(order, *refs)

    blocks, rows, width = own.shape
    half = rows // (STATES + CHANNELS)
    return pl.pallas_call(
        step,
        out_shape=jax.ShapeDtypeStruct((blocks, half, STATES * width), jnp.bfloat16),
        in_specs=[SMEM, SMEM, VMEM, HBM, HBM],
        out_specs=VMEM,
        scratch_shapes=[
            pltpu.VMEM((STATES * width, blocks * width), jnp.bfloat16),
            pltpu.VMEM((blocks * width, CHANNELS * width), jnp.bfloat16),
            pltpu.VMEM((blocks * half, CHANNELS * width), jnp.bfloat16),
            pltpu.VMEM((STATES * width, CHANNELS * width), jnp.float32),
            pltpu.VMEM((CHANNELS * width, STATES * width), jnp.bfloat16),
            pltpu.VMEM(own.shape, jnp.bfloat16),
            pltpu.VMEM(other.shape, jnp.bfloat16),
            pltpu.SemaphoreType.DMA((2, 2)),
        ],
        compiler_params=LARGE,
    )(core, table, left, in_hbm(own), in_hbm(other))


def near_kernel(pieces_ref, out_ref):
    for j in range(out_ref.shape[0]):
        total = pieces_ref[0, j].astype(jnp.float32)
        for k in range(1, pieces_ref.shape[0]):
            total = total + pieces_ref[k, j].astype(jnp.float32)
        out_ref[j] = total.astype(jnp.bfloat16)


def near_sum(pieces):
    return pl.pallas_call(
        near_kernel,
        out_shape=jax.ShapeDtypeStruct(pieces.shape[1:], jnp.bfloat16),
        in_specs=[VMEM],
        out_specs=VMEM,
        compiler_params=SMALL,
    )(pieces)


def neighbours(n_far, n_near):
    n_z = n_far * n_near
    groups = []
    for core in range(2):
        for j in range(n_far):
            first = j * n_near + core * (n_near // 2)
            chips = sorted(((first + i) % n_z for i in range(n_near)), key=lambda z: z % n_near)
            groups.append([2 * z + core for z in chips])
    return groups


def lanes_of(total):
    rows, cols = total.shape
    total = sum(total[:, k : k + 128] for k in range(0, cols, 128))
    return sum(total[k : k + 8] for k in range(0, rows, 8))


def sums_kernel(pieces_ref, vector_ref, image_ref, sums_ref):
    image = pieces_ref[0].astype(jnp.float32)
    for k in range(1, pieces_ref.shape[0]):
        image = image + pieces_ref[k].astype(jnp.float32)
    image_ref[...] = image
    base = jnp.concatenate([vector_ref[t].astype(jnp.float32) for t in range(STATES)], 1)
    found = [lanes_of(base * base), lanes_of(base * image), lanes_of(image * image)]
    lane = lax.broadcasted_iota(jnp.int32, (1, 128), 1)
    row = jnp.zeros((1, 128), jnp.float32)
    for k in range(3):
        row = jnp.where(lane == k, jnp.sum(found[k], keepdims=True), row)
    for r in range(sums_ref.shape[0]):
        sums_ref[r] = row


def sums_of(pieces, vector, size):
    return pl.pallas_call(
        sums_kernel,
        out_shape=(
            jax.ShapeDtypeStruct(pieces.shape[1:], jnp.float32),
            jax.ShapeDtypeStruct((size, 1, 128), jnp.float32),
        ),
        in_specs=[VMEM, VMEM],
        out_specs=(VMEM, VMEM),
        compiler_params=SMALL,
    )(pieces, vector)


def again_kernel(pieces_ref, out_ref):
    total = pieces_ref[0]
    for k in range(1, pieces_ref.shape[0]):
        total = total + pieces_ref[k]
    for r in range(out_ref.shape[0]):
        out_ref[r] = total


def again(pieces, size):
    return pl.pallas_call(
        again_kernel,
        out_shape=jax.ShapeDtypeStruct((size, *pieces.shape[1:]), jnp.float32),
        in_specs=[VMEM],
        out_specs=VMEM,
        compiler_params=SMALL,
    )(pieces)


def last_kernel(entries, pieces_ref, image_ref, vector_ref, next_ref, coefficients_ref):
    total = pieces_ref[0]
    for k in range(1, pieces_ref.shape[0]):
        total = total + pieces_ref[k]
    total = total / entries
    lane = lax.broadcasted_iota(jnp.int32, total.shape, 1)
    base_square, correlation, image_square = (
        jnp.sum(jnp.where(lane == k, total, 0.0), 1, keepdims=True) for k in range(3)
    )
    alpha = correlation / (base_square + epsilon)
    rho = jnp.sqrt(image_square - 2.0 * alpha * correlation + alpha * alpha * base_square + epsilon)
    width = next_ref.shape[2]
    for t in range(STATES):
        residual = image_ref[:, t * width : (t + 1) * width] - alpha * vector_ref[t].astype(jnp.float32)
        next_ref[t] = (residual / rho).astype(jnp.bfloat16)
    coefficients_ref[0] = alpha[0, 0]
    coefficients_ref[1] = rho[0, 0]


def last(entries, pieces, image, vector):
    def step(*refs):
        last_kernel(entries, *refs)

    return pl.pallas_call(
        step,
        out_shape=(
            jax.ShapeDtypeStruct(vector.shape, jnp.bfloat16),
            jax.ShapeDtypeStruct((2,), jnp.float32),
        ),
        in_specs=[VMEM, VMEM, VMEM],
        out_specs=(VMEM, SMEM),
        compiler_params=SMALL,
    )(pieces, image, vector)


def all_to_all(x, axes):
    return lax.all_to_all(x, axes, 0, 0, tiled=True)


def other_core(x):
    return lax.ppermute(x, C, [(0, 1), (1, 0)])


def body(start_vector, left_env, right_env, left_tensor, right_tensor):
    n_row = lax.axis_size(ROW)
    n_far, n_near = lax.axis_size(FAR), lax.axis_size(NEAR)
    n_z = n_far * n_near
    _, rows, half = start_vector.shape
    entries = float(STATES * rows * half * n_row * n_z * lax.axis_size(C))
    core = lax.axis_index(C).astype(jnp.int32).reshape(1)
    table = coupling(left_tensor, right_tensor)
    vector = jnp.swapaxes(start_vector, 1, 2)
    left = jnp.swapaxes(left_env, 1, 2).reshape(CHANNELS * half, rows)
    left = (left.astype(jnp.float32) * SCALE).astype(jnp.float16)

    own = all_to_all(pack(vector, right_env, n_row), ROW)
    left = lax.all_gather(left, COL, axis=0)
    own, left = lax.optimization_barrier((own, left))
    left = (left.astype(jnp.float32) * (1.0 / SCALE)).astype(jnp.bfloat16)
    order = [n_far * (z % n_near) + z // n_near for z in range(n_z)]
    sent = terms(order, core, table, left, own, other_core(own))

    pieces = lax.all_to_all(sent, COL, 0, 0, axis_index_groups=neighbours(n_far, n_near), tiled=True)
    pieces = all_to_all(near_sum(pieces.reshape(n_near, n_far, *pieces.shape[1:])), FAR)
    image, sums = sums_of(pieces, vector, lax.axis_size((X, Y, C)))
    sums = again(all_to_all(sums, (X, Y, C)), n_z)
    next_vector, coefficients = last(entries, all_to_all(sums, Z), image, vector)
    return jnp.swapaxes(next_vector, 1, 2), coefficients


def solution(mesh):
    finer = Mesh(mesh.devices.reshape(4, 4, 4, 4, 2), (X, Y, FAR, NEAR, C))
    in_specs = (P(None, ROW, COL), P(None, ROW, COL), P(None, COL, ROW), P(), P())
    out_specs = (P(None, ROW, COL), P())
    return jax.shard_map(body, mesh=finer, in_specs=in_specs, out_specs=out_specs, check_vma=False)
```

```python
import jax
import jax.numpy as jnp
from jax import lax
from jax.experimental import pallas as pl
from jax.experimental.pallas import tpu as pltpu
from jax.sharding import Mesh
from jax.sharding import PartitionSpec as P

X, Y, FAR, NEAR, C = "row_0", "row_1", "far", "near", "core"
ROW = (X, Y)
Z = (FAR, NEAR)
COL = (FAR, NEAR, C)
STATES = 4
CHANNELS = 5
PAIRS = STATES * CHANNELS

epsilon = 1e-06
SCALE = 8192.0

VMEM = pl.BlockSpec(memory_space=pltpu.VMEM)
SMEM = pl.BlockSpec(memory_space=pltpu.SMEM)
HBM = pl.BlockSpec(memory_space=pltpu.HBM)
SMALL = pltpu.CompilerParams(vmem_limit_bytes=4 * 1024 * 1024)
LARGE = pltpu.CompilerParams(vmem_limit_bytes=24 * 1024 * 1024)


def in_hbm(x):
    return pltpu.with_memory_space_constraint(x, pltpu.HBM)


def coupling(left_tensor, right_tensor):
    joined = jnp.einsum("wuac,uvbd->vabwcd", left_tensor, right_tensor, precision=lax.Precision.HIGHEST)
    return joined.reshape(PAIRS, PAIRS)


def pack_kernel(vector_hbm, right_hbm, out_hbm, vector_s, right_s, piece_s, in_sems, out_sems):
    states, half, width = vector_s.shape
    rights = right_s.shape[0]
    loads = [
        pltpu.make_async_copy(vector_hbm, vector_s, in_sems.at[0]),
        pltpu.make_async_copy(right_hbm, right_s, in_sems.at[1]),
    ]
    for load in loads:
        load.start()
    loads[0].wait()
    for t in range(states):
        piece_s[t * half : (t + 1) * half, :] = vector_s[t]
    loads[1].wait()
    for v in range(rights):
        turned = right_s[v].astype(jnp.float32).T
        turned = jnp.concatenate([turned[:half], turned[half:]], 1).astype(jnp.bfloat16)
        piece_s[(states + v) * half : (states + v + 1) * half, :] = turned
    stores = [pltpu.make_async_copy(piece_s, out_hbm.at[r], out_sems.at[r]) for r in range(out_hbm.shape[0])]
    for store in stores:
        store.start()
    for store in stores:
        store.wait()


def pack(vector, right, size):
    states, half, width = vector.shape
    rows = (states + right.shape[0]) * half
    return pl.pallas_call(
        pack_kernel,
        out_shape=pltpu.HBM((size, rows, width), jnp.bfloat16),
        in_specs=[HBM, HBM],
        out_specs=HBM,
        scratch_shapes=[
            pltpu.VMEM(vector.shape, jnp.bfloat16),
            pltpu.VMEM(right.shape, jnp.bfloat16),
            pltpu.VMEM((rows, width), jnp.bfloat16),
            pltpu.SemaphoreType.DMA((2,)),
            pltpu.SemaphoreType.DMA((size,)),
        ],
        compiler_params=SMALL,
    )(in_hbm(vector), in_hbm(right))


def contract_and_mix(table_ref, left_ref, source, vec_s, cross_s, store):
    blocks, rows, width = source.shape
    half = rows // STATES
    for r in range(blocks):
        vec_s[:, r * width : (r + 1) * width] = source[r]
    cross_s[...] = jnp.dot(vec_s[...], left_ref[...], preferred_element_type=jnp.float32)
    for v in range(CHANNELS):
        for s in range(STATES):
            total = None
            for w in range(CHANNELS):
                for t in range(STATES):
                    part = (
                        table_ref[v * STATES + s, w * STATES + t]
                        * cross_s[t * half : (t + 1) * half, w * width : (w + 1) * width]
                    )
                    total = part if total is None else total + part
            store(v, s, total.astype(jnp.bfloat16))


def own_kernel(table_ref, left_ref, own_hbm, left_out, mixed_out, right_out, piece_s, vec_s, cross_s, sems):
    _, rows, width = piece_s.shape
    half = rows // STATES
    load = pltpu.make_async_copy(own_hbm.at[:, pl.ds(0, rows)], piece_s, sems.at[0])
    load.start()
    passed = pltpu.make_async_copy(own_hbm.at[:, pl.ds(rows, CHANNELS * half)], right_out, sems.at[1])
    passed.start()
    for k in range(left_ref.shape[0]):
        for w in range(CHANNELS):
            left_out[k * half : (k + 1) * half, w * width : (w + 1) * width] = left_ref[k, w * half : (w + 1) * half, :]
    load.wait()

    def store(v, s, x):
        mixed_out[v * half : (v + 1) * half, s * width : (s + 1) * width] = x

    contract_and_mix(table_ref, left_out, piece_s, vec_s, cross_s, store)
    passed.wait()


def own_part(table, left, own):
    blocks, rows, width = own.shape
    half = rows // (STATES + CHANNELS)
    return pl.pallas_call(
        own_kernel,
        out_shape=(
            jax.ShapeDtypeStruct((left.shape[0] * half, CHANNELS * width), jnp.bfloat16),
            jax.ShapeDtypeStruct((CHANNELS * half, STATES * width), jnp.bfloat16),
            jax.ShapeDtypeStruct((blocks, CHANNELS * half, width), jnp.bfloat16),
        ),
        in_specs=[SMEM, VMEM, HBM],
        out_specs=(VMEM, VMEM, VMEM),
        scratch_shapes=[
            pltpu.VMEM((blocks, STATES * half, width), jnp.bfloat16),
            pltpu.VMEM((STATES * half, blocks * width), jnp.bfloat16),
            pltpu.VMEM((STATES * half, CHANNELS * width), jnp.float32),
            pltpu.SemaphoreType.DMA((2,)),
        ],
        compiler_params=LARGE,
    )(table, left, in_hbm(own))


def terms_kernel(
    order, core_ref, table_ref, left_ref, mixed_ref, right_own, other_hbm, out_ref,
    piece_s, right_other, vec_s, cross_s, right_s, mixed_s, sems,
):
    blocks, half, _ = out_ref.shape
    width = 2 * half
    core = core_ref[0]
    own_at = pl.multiple_of(core * half, half)
    other_at = pl.multiple_of((1 - core) * half, half)
    vectors, rights = pl.ds(0, STATES * half), pl.ds(STATES * half, CHANNELS * half)
    loads = [
        pltpu.make_async_copy(other_hbm.at[:, vectors], piece_s, sems.at[0]),
        pltpu.make_async_copy(other_hbm.at[:, rights], right_other, sems.at[1]),
    ]
    for load in loads:
        load.start()
    for v in range(CHANNELS):
        mixed_s[pl.ds(v * width + own_at, half), :] = mixed_ref[v * half : (v + 1) * half, :]
    loads[0].wait()

    def store(v, s, x):
        mixed_s[pl.ds(v * width + other_at, half), s * width : (s + 1) * width] = x

    contract_and_mix(table_ref, left_ref, piece_s, vec_s, cross_s, store)
    loads[1].wait()
    mine = lax.broadcasted_iota(jnp.int32, (half, width), 1) // half == core
    for r in range(blocks):
        for v in range(CHANNELS):
            own = right_own[r, v * half : (v + 1) * half, :].astype(jnp.float32)
            other = right_other[r, v * half : (v + 1) * half, :].astype(jnp.float32)
            other = jnp.concatenate([other[:, half:], other[:, :half]], 1)
            right_s[r * half : (r + 1) * half, v * width : (v + 1) * width] = jnp.where(mine, own, other).astype(jnp.bfloat16)
    image = jnp.dot(right_s[...], mixed_s[...], preferred_element_type=jnp.float32)
    for r in range(blocks):
        out_ref[order[r]] = image[r * half : (r + 1) * half].astype(jnp.bfloat16)


def terms(order, core, table, left, mixed, right, other):
    def step(*refs):
        terms_kernel(order, *refs)

    blocks, rows, width = other.shape
    half = rows // (STATES + CHANNELS)
    return pl.pallas_call(
        step,
        out_shape=jax.ShapeDtypeStruct((blocks, half, STATES * width), jnp.bfloat16),
        in_specs=[SMEM, SMEM, VMEM, VMEM, VMEM, HBM],
        out_specs=VMEM,
        scratch_shapes=[
            pltpu.VMEM((blocks, STATES * half, width), jnp.bfloat16),
            pltpu.VMEM((blocks, CHANNELS * half, width), jnp.bfloat16),
            pltpu.VMEM((STATES * half, blocks * width), jnp.bfloat16),
            pltpu.VMEM((STATES * half, CHANNELS * width), jnp.float32),
            pltpu.VMEM((blocks * half, CHANNELS * width), jnp.bfloat16),
            pltpu.VMEM((CHANNELS * width, STATES * width), jnp.bfloat16),
            pltpu.SemaphoreType.DMA((2,)),
        ],
        compiler_params=LARGE,
    )(core, table, left, mixed, right, in_hbm(other))


def near_kernel(pieces_ref, out_ref):
    for j in range(out_ref.shape[0]):
        total = pieces_ref[0, j].astype(jnp.float32)
        for k in range(1, pieces_ref.shape[0]):
            total = total + pieces_ref[k, j].astype(jnp.float32)
        out_ref[j] = total.astype(jnp.bfloat16)


def near_sum(pieces):
    return pl.pallas_call(
        near_kernel,
        out_shape=jax.ShapeDtypeStruct(pieces.shape[1:], jnp.bfloat16),
        in_specs=[VMEM],
        out_specs=VMEM,
        compiler_params=SMALL,
    )(pieces)


def neighbours(n_far, n_near):
    n_z = n_far * n_near
    groups = []
    for core in range(2):
        for j in range(n_far):
            first = j * n_near + core * (n_near // 2)
            chips = sorted(((first + i) % n_z for i in range(n_near)), key=lambda z: z % n_near)
            groups.append([2 * z + core for z in chips])
    return groups


def lanes_of(total):
    rows, cols = total.shape
    total = sum(total[:, k : k + 128] for k in range(0, cols, 128))
    return sum(total[k : k + 8] for k in range(0, rows, 8))


def sums_kernel(pieces_ref, vector_ref, image_ref, sums_ref):
    image = pieces_ref[0].astype(jnp.float32)
    for k in range(1, pieces_ref.shape[0]):
        image = image + pieces_ref[k].astype(jnp.float32)
    image_ref[...] = image
    base = jnp.concatenate([vector_ref[t].astype(jnp.float32) for t in range(STATES)], 1)
    found = [lanes_of(base * base), lanes_of(base * image), lanes_of(image * image)]
    lane = lax.broadcasted_iota(jnp.int32, (1, 128), 1)
    row = jnp.zeros((1, 128), jnp.float32)
    for k in range(3):
        row = jnp.where(lane == k, jnp.sum(found[k], keepdims=True), row)
    for r in range(sums_ref.shape[0]):
        sums_ref[r] = row


def sums_of(pieces, vector, size):
    return pl.pallas_call(
        sums_kernel,
        out_shape=(
            jax.ShapeDtypeStruct(pieces.shape[1:], jnp.float32),
            jax.ShapeDtypeStruct((size, 1, 128), jnp.float32),
        ),
        in_specs=[VMEM, VMEM],
        out_specs=(VMEM, VMEM),
        compiler_params=SMALL,
    )(pieces, vector)


def again_kernel(pieces_ref, out_ref):
    total = pieces_ref[0]
    for k in range(1, pieces_ref.shape[0]):
        total = total + pieces_ref[k]
    for r in range(out_ref.shape[0]):
        out_ref[r] = total


def again(pieces, size):
    return pl.pallas_call(
        again_kernel,
        out_shape=jax.ShapeDtypeStruct((size, *pieces.shape[1:]), jnp.float32),
        in_specs=[VMEM],
        out_specs=VMEM,
        compiler_params=SMALL,
    )(pieces)


def last_kernel(entries, pieces_ref, image_ref, vector_ref, next_ref, coefficients_ref):
    total = pieces_ref[0]
    for k in range(1, pieces_ref.shape[0]):
        total = total + pieces_ref[k]
    total = total / entries
    lane = lax.broadcasted_iota(jnp.int32, total.shape, 1)
    base_square, correlation, image_square = (
        jnp.sum(jnp.where(lane == k, total, 0.0), 1, keepdims=True) for k in range(3)
    )
    alpha = correlation / (base_square + epsilon)
    rho = jnp.sqrt(image_square - 2.0 * alpha * correlation + alpha * alpha * base_square + epsilon)
    width = next_ref.shape[2]
    for t in range(STATES):
        residual = image_ref[:, t * width : (t + 1) * width] - alpha * vector_ref[t].astype(jnp.float32)
        next_ref[t] = (residual / rho).astype(jnp.bfloat16)
    coefficients_ref[0] = alpha[0, 0]
    coefficients_ref[1] = rho[0, 0]


def last(entries, pieces, image, vector):
    def step(*refs):
        last_kernel(entries, *refs)

    return pl.pallas_call(
        step,
        out_shape=(
            jax.ShapeDtypeStruct(vector.shape, jnp.bfloat16),
            jax.ShapeDtypeStruct((2,), jnp.float32),
        ),
        in_specs=[VMEM, VMEM, VMEM],
        out_specs=(VMEM, SMEM),
        compiler_params=SMALL,
    )(pieces, image, vector)


def all_to_all(x, axes):
    return lax.all_to_all(x, axes, 0, 0, tiled=True)


def other_core(x):
    return lax.ppermute(x, C, [(0, 1), (1, 0)])


def body(start_vector, left_env, right_env, left_tensor, right_tensor):
    n_row = lax.axis_size(ROW)
    n_far, n_near = lax.axis_size(FAR), lax.axis_size(NEAR)
    n_z = n_far * n_near
    _, rows, half = start_vector.shape
    entries = float(STATES * rows * half * n_row * n_z * lax.axis_size(C))
    core = lax.axis_index(C).astype(jnp.int32).reshape(1)
    table = coupling(left_tensor, right_tensor)
    vector = jnp.swapaxes(start_vector, 1, 2)
    left = jnp.swapaxes(left_env, 1, 2).reshape(CHANNELS * half, rows)
    left = (left.astype(jnp.float32) * SCALE).astype(jnp.float16)

    own = all_to_all(pack(vector, right_env, n_row), ROW)
    left = lax.all_gather(left, COL, axis=0)
    own, left = lax.optimization_barrier((own, left))
    left = (left.astype(jnp.float32) * (1.0 / SCALE)).astype(jnp.bfloat16)
    order = [n_far * (z % n_near) + z // n_near for z in range(n_z)]
    other = other_core(own)
    left, mixed, right = own_part(table, left, own)
    sent = terms(order, core, table, left, mixed, right, other)

    pieces = lax.all_to_all(sent, COL, 0, 0, axis_index_groups=neighbours(n_far, n_near), tiled=True)
    pieces = all_to_all(near_sum(pieces.reshape(n_near, n_far, *pieces.shape[1:])), FAR)
    image, sums = sums_of(pieces, vector, lax.axis_size((X, Y, C)))
    sums = again(all_to_all(sums, (X, Y, C)), n_z)
    next_vector, coefficients = last(entries, all_to_all(sums, Z), image, vector)
    return jnp.swapaxes(next_vector, 1, 2), coefficients


def solution(mesh):
    finer = Mesh(mesh.devices.reshape(4, 4, 4, 4, 2), (X, Y, FAR, NEAR, C))
    in_specs = (P(None, ROW, COL), P(None, ROW, COL), P(None, COL, ROW), P(), P())
    out_specs = (P(None, ROW, COL), P())
    return jax.shard_map(body, mesh=finer, in_specs=in_specs, out_specs=out_specs, check_vma=False)
```

```python
import jax
import jax.numpy as jnp
from jax import lax
from jax.experimental import pallas as pl
from jax.experimental.pallas import tpu as pltpu
from jax.sharding import Mesh
from jax.sharding import PartitionSpec as P

X, Y, FAR, NEAR, C = "row_0", "row_1", "far", "near", "core"
ROW = (X, Y)
Z = (FAR, NEAR)
COL = (FAR, NEAR, C)
STATES = 4
CHANNELS = 5

epsilon = 1e-06
SCALE = 8192.0

VMEM = pl.BlockSpec(memory_space=pltpu.VMEM)
SMEM = pl.BlockSpec(memory_space=pltpu.SMEM)
HBM = pl.BlockSpec(memory_space=pltpu.HBM)
SMALL = pltpu.CompilerParams(vmem_limit_bytes=4 * 1024 * 1024)
LARGE = pltpu.CompilerParams(vmem_limit_bytes=24 * 1024 * 1024)


def in_hbm(x):
    return pltpu.with_memory_space_constraint(x, pltpu.HBM)


def pack_kernel(vector_hbm, right_hbm, out_hbm, vector_s, right_s, piece_s, in_sems, out_sems):
    states, half, width = vector_s.shape
    rights = right_s.shape[0]
    loads = [
        pltpu.make_async_copy(vector_hbm, vector_s, in_sems.at[0]),
        pltpu.make_async_copy(right_hbm, right_s, in_sems.at[1]),
    ]
    for load in loads:
        load.start()
    loads[0].wait()
    for t in range(states):
        piece_s[t * half : (t + 1) * half, :] = vector_s[t]
    loads[1].wait()
    for v in range(rights):
        turned = right_s[v].astype(jnp.float32).T
        turned = jnp.concatenate([turned[:half], turned[half:]], 1).astype(jnp.bfloat16)
        piece_s[(states + v) * half : (states + v + 1) * half, :] = turned
    stores = [pltpu.make_async_copy(piece_s, out_hbm.at[r], out_sems.at[r]) for r in range(out_hbm.shape[0])]
    for store in stores:
        store.start()
    for store in stores:
        store.wait()


def pack(vector, right, size):
    states, half, width = vector.shape
    rows = (states + right.shape[0]) * half
    return pl.pallas_call(
        pack_kernel,
        out_shape=pltpu.HBM((size, rows, width), jnp.bfloat16),
        in_specs=[HBM, HBM],
        out_specs=HBM,
        scratch_shapes=[
            pltpu.VMEM(vector.shape, jnp.bfloat16),
            pltpu.VMEM(right.shape, jnp.bfloat16),
            pltpu.VMEM((rows, width), jnp.bfloat16),
            pltpu.SemaphoreType.DMA((2,)),
            pltpu.SemaphoreType.DMA((size,)),
        ],
        compiler_params=SMALL,
    )(in_hbm(vector), in_hbm(right))


def site_copies(left_site, right_site, left_t, right_t, left_sem, right_sem):
    loads = (
        pltpu.make_async_copy(left_site, left_t, left_sem),
        pltpu.make_async_copy(right_site, right_t, right_sem),
    )
    for load in loads:
        load.start()
    return loads


def combined(terms):
    total = None
    for scale, x in terms:
        total = scale * x if total is None else total + scale * x
    return total


def contract_and_mix(site_loads, left_t, right_t, left_ref, source, vec_s, cross_s, half_s, store):
    blocks, rows, width = source.shape
    half = rows // STATES
    for r in range(blocks):
        vec_s[:, r * width : (r + 1) * width] = source[r]
    cross_s[...] = jnp.dot(vec_s[...], left_ref[...], preferred_element_type=jnp.float32)
    for load in site_loads:
        load.wait()
    for s1 in range(2):
        for u in range(CHANNELS):
            for t2 in range(2):
                half_s[u, t2] = combined(
                    (
                        left_t[w, s1, t1, u],
                        cross_s[(2 * t1 + t2) * half : (2 * t1 + t2 + 1) * half, w * width : (w + 1) * width],
                    )
                    for w in range(CHANNELS)
                    for t1 in range(2)
                )
        for v in range(CHANNELS):
            for s2 in range(2):
                total = combined((right_t[u, s2, t2, v], half_s[u, t2]) for u in range(CHANNELS) for t2 in range(2))
                store(v, 2 * s1 + s2, total.astype(jnp.bfloat16))


def own_kernel(
    left_site, right_site, left_ref, own_hbm, left_out, mixed_out, right_out,
    left_t, right_t, piece_s, vec_s, cross_s, half_s, sems,
):
    _, rows, width = piece_s.shape
    half = rows // STATES
    load = pltpu.make_async_copy(own_hbm.at[:, pl.ds(0, rows)], piece_s, sems.at[0])
    load.start()
    passed = pltpu.make_async_copy(own_hbm.at[:, pl.ds(rows, CHANNELS * half)], right_out, sems.at[1])
    passed.start()
    site_loads = site_copies(left_site, right_site, left_t, right_t, sems.at[2], sems.at[3])
    for k in range(left_ref.shape[0]):
        for w in range(CHANNELS):
            left_out[k * half : (k + 1) * half, w * width : (w + 1) * width] = left_ref[k, w * half : (w + 1) * half, :]
    load.wait()

    def store(v, s, x):
        mixed_out[v * half : (v + 1) * half, s * width : (s + 1) * width] = x

    contract_and_mix(site_loads, left_t, right_t, left_out, piece_s, vec_s, cross_s, half_s, store)
    passed.wait()


def own_part(sites, left, own):
    blocks, rows, width = own.shape
    half = rows // (STATES + CHANNELS)
    return pl.pallas_call(
        own_kernel,
        out_shape=(
            jax.ShapeDtypeStruct((left.shape[0] * half, CHANNELS * width), jnp.bfloat16),
            jax.ShapeDtypeStruct((CHANNELS * half, STATES * width), jnp.bfloat16),
            jax.ShapeDtypeStruct((blocks, CHANNELS * half, width), jnp.bfloat16),
        ),
        in_specs=[HBM, HBM, VMEM, HBM],
        out_specs=(VMEM, VMEM, VMEM),
        scratch_shapes=[
            *(pltpu.SMEM(site.shape, jnp.float32) for site in sites),
            pltpu.VMEM((blocks, STATES * half, width), jnp.bfloat16),
            pltpu.VMEM((STATES * half, blocks * width), jnp.bfloat16),
            pltpu.VMEM((STATES * half, CHANNELS * width), jnp.float32),
            pltpu.VMEM((CHANNELS, 2, half, width), jnp.float32),
            pltpu.SemaphoreType.DMA((4,)),
        ],
        compiler_params=LARGE,
    )(*(in_hbm(site) for site in sites), left, in_hbm(own))


def terms_kernel(
    order, core_ref, left_site, right_site, left_ref, mixed_ref, right_own, other_hbm, out_ref,
    left_t, right_t, piece_s, right_other, vec_s, cross_s, half_s, right_s, mixed_s, sems,
):
    blocks, half, _ = out_ref.shape
    width = 2 * half
    core = core_ref[0]
    own_at = pl.multiple_of(core * half, half)
    other_at = pl.multiple_of((1 - core) * half, half)
    vectors, rights = pl.ds(0, STATES * half), pl.ds(STATES * half, CHANNELS * half)
    loads = [
        pltpu.make_async_copy(other_hbm.at[:, vectors], piece_s, sems.at[0]),
        pltpu.make_async_copy(other_hbm.at[:, rights], right_other, sems.at[1]),
    ]
    for load in loads:
        load.start()
    site_loads = site_copies(left_site, right_site, left_t, right_t, sems.at[2], sems.at[3])
    mine = lax.broadcasted_iota(jnp.int32, (half, width), 1) // half == core
    for v in range(CHANNELS):
        mixed_s[pl.ds(v * width + own_at, half), :] = mixed_ref[v * half : (v + 1) * half, :]
        for r in range(blocks):
            right_s[r * half : (r + 1) * half, v * width : (v + 1) * width] = right_own[r, v * half : (v + 1) * half, :]
    loads[0].wait()

    def store(v, s, x):
        mixed_s[pl.ds(v * width + other_at, half), s * width : (s + 1) * width] = x

    contract_and_mix(site_loads, left_t, right_t, left_ref, piece_s, vec_s, cross_s, half_s, store)
    loads[1].wait()
    for r in range(blocks):
        for v in range(CHANNELS):
            at = (slice(r * half, (r + 1) * half), slice(v * width, (v + 1) * width))
            other = right_other[r, v * half : (v + 1) * half, :].astype(jnp.float32)
            other = jnp.concatenate([other[:, half:], other[:, :half]], 1)
            right_s[at] = jnp.where(mine, right_s[at].astype(jnp.float32), other).astype(jnp.bfloat16)
    image = jnp.dot(right_s[...], mixed_s[...], preferred_element_type=jnp.float32)
    for r in range(blocks):
        out_ref[order[r]] = image[r * half : (r + 1) * half].astype(jnp.bfloat16)


def terms(order, core, sites, left, mixed, right, other):
    def step(*refs):
        terms_kernel(order, *refs)

    blocks, rows, width = other.shape
    half = rows // (STATES + CHANNELS)
    return pl.pallas_call(
        step,
        out_shape=jax.ShapeDtypeStruct((blocks, half, STATES * width), jnp.bfloat16),
        in_specs=[SMEM, HBM, HBM, VMEM, VMEM, VMEM, HBM],
        out_specs=VMEM,
        scratch_shapes=[
            *(pltpu.SMEM(site.shape, jnp.float32) for site in sites),
            pltpu.VMEM((blocks, STATES * half, width), jnp.bfloat16),
            pltpu.VMEM((blocks, CHANNELS * half, width), jnp.bfloat16),
            pltpu.VMEM((STATES * half, blocks * width), jnp.bfloat16),
            pltpu.VMEM((STATES * half, CHANNELS * width), jnp.float32),
            pltpu.VMEM((CHANNELS, 2, half, width), jnp.float32),
            pltpu.VMEM((blocks * half, CHANNELS * width), jnp.bfloat16),
            pltpu.VMEM((CHANNELS * width, STATES * width), jnp.bfloat16),
            pltpu.SemaphoreType.DMA((4,)),
        ],
        compiler_params=LARGE,
    )(core, *(in_hbm(site) for site in sites), left, mixed, right, in_hbm(other))


def near_kernel(pieces_ref, out_ref):
    for j in range(out_ref.shape[0]):
        total = pieces_ref[0, j].astype(jnp.float32)
        for k in range(1, pieces_ref.shape[0]):
            total = total + pieces_ref[k, j].astype(jnp.float32)
        out_ref[j] = total.astype(jnp.bfloat16)


def near_sum(pieces):
    return pl.pallas_call(
        near_kernel,
        out_shape=jax.ShapeDtypeStruct(pieces.shape[1:], jnp.bfloat16),
        in_specs=[VMEM],
        out_specs=VMEM,
        compiler_params=SMALL,
    )(pieces)


def neighbours(n_far, n_near):
    n_z = n_far * n_near
    groups = []
    for core in range(2):
        for j in range(n_far):
            first = j * n_near + core * (n_near // 2)
            chips = sorted(((first + i) % n_z for i in range(n_near)), key=lambda z: z % n_near)
            groups.append([2 * z + core for z in chips])
    return groups


def lanes_of(total):
    rows, cols = total.shape
    total = sum(total[:, k : k + 128] for k in range(0, cols, 128))
    return sum(total[k : k + 8] for k in range(0, rows, 8))


def sums_kernel(pieces_ref, vector_ref, image_ref, sums_ref):
    image = pieces_ref[0].astype(jnp.float32)
    for k in range(1, pieces_ref.shape[0]):
        image = image + pieces_ref[k].astype(jnp.float32)
    image_ref[...] = image
    base = jnp.concatenate([vector_ref[t].astype(jnp.float32) for t in range(STATES)], 1)
    found = [lanes_of(base * base), lanes_of(base * image), lanes_of(image * image)]
    lane = lax.broadcasted_iota(jnp.int32, (1, 128), 1)
    row = jnp.zeros((1, 128), jnp.float32)
    for k in range(3):
        row = jnp.where(lane == k, jnp.sum(found[k], keepdims=True), row)
    for r in range(sums_ref.shape[0]):
        sums_ref[r] = row


def sums_of(pieces, vector, size):
    return pl.pallas_call(
        sums_kernel,
        out_shape=(
            jax.ShapeDtypeStruct(pieces.shape[1:], jnp.float32),
            jax.ShapeDtypeStruct((size, 1, 128), jnp.float32),
        ),
        in_specs=[VMEM, VMEM],
        out_specs=(VMEM, VMEM),
        compiler_params=SMALL,
    )(pieces, vector)


def again_kernel(pieces_ref, out_ref):
    total = pieces_ref[0]
    for k in range(1, pieces_ref.shape[0]):
        total = total + pieces_ref[k]
    for r in range(out_ref.shape[0]):
        out_ref[r] = total


def again(pieces, size):
    return pl.pallas_call(
        again_kernel,
        out_shape=jax.ShapeDtypeStruct((size, *pieces.shape[1:]), jnp.float32),
        in_specs=[VMEM],
        out_specs=VMEM,
        compiler_params=SMALL,
    )(pieces)


def last_kernel(entries, pieces_ref, image_ref, vector_ref, next_ref, coefficients_ref):
    total = pieces_ref[0]
    for k in range(1, pieces_ref.shape[0]):
        total = total + pieces_ref[k]
    total = total / entries
    lane = lax.broadcasted_iota(jnp.int32, total.shape, 1)
    base_square, correlation, image_square = (
        jnp.sum(jnp.where(lane == k, total, 0.0), 1, keepdims=True) for k in range(3)
    )
    alpha = correlation / (base_square + epsilon)
    rho = jnp.sqrt(image_square - 2.0 * alpha * correlation + alpha * alpha * base_square + epsilon)
    width = next_ref.shape[2]
    for t in range(STATES):
        residual = image_ref[:, t * width : (t + 1) * width] - alpha * vector_ref[t].astype(jnp.float32)
        next_ref[t] = (residual / rho).astype(jnp.bfloat16)
    coefficients_ref[0] = alpha[0, 0]
    coefficients_ref[1] = rho[0, 0]


def last(entries, pieces, image, vector):
    def step(*refs):
        last_kernel(entries, *refs)

    return pl.pallas_call(
        step,
        out_shape=(
            jax.ShapeDtypeStruct(vector.shape, jnp.bfloat16),
            jax.ShapeDtypeStruct((2,), jnp.float32),
        ),
        in_specs=[VMEM, VMEM, VMEM],
        out_specs=(VMEM, SMEM),
        compiler_params=SMALL,
    )(pieces, image, vector)


def all_to_all(x, axes):
    return lax.all_to_all(x, axes, 0, 0, tiled=True)


def other_core(x):
    return lax.ppermute(x, C, [(0, 1), (1, 0)])


def body(start_vector, left_env, right_env, left_tensor, right_tensor):
    n_row = lax.axis_size(ROW)
    n_far, n_near = lax.axis_size(FAR), lax.axis_size(NEAR)
    n_z = n_far * n_near
    _, rows, half = start_vector.shape
    entries = float(STATES * rows * half * n_row * n_z * lax.axis_size(C))
    core = lax.axis_index(C).astype(jnp.int32).reshape(1)
    sites = tuple(jnp.transpose(tensor, (0, 2, 3, 1)) for tensor in (left_tensor, right_tensor))
    vector = jnp.swapaxes(start_vector, 1, 2)
    left = jnp.swapaxes(left_env, 1, 2).reshape(CHANNELS * half, rows)
    left = (left.astype(jnp.float32) * SCALE).astype(jnp.float16)

    own = all_to_all(pack(vector, right_env, n_row), ROW)
    left = lax.all_gather(left, COL, axis=0)
    own, left = lax.optimization_barrier((own, left))
    left = (left.astype(jnp.float32) * (1.0 / SCALE)).astype(jnp.bfloat16)
    order = [n_far * (z % n_near) + z // n_near for z in range(n_z)]
    other = other_core(own)
    left, mixed, right = own_part(sites, left, own)
    sent = terms(order, core, sites, left, mixed, right, other)

    pieces = lax.all_to_all(sent, COL, 0, 0, axis_index_groups=neighbours(n_far, n_near), tiled=True)
    pieces = all_to_all(near_sum(pieces.reshape(n_near, n_far, *pieces.shape[1:])), FAR)
    image, sums = sums_of(pieces, vector, n_z)
    sums = again(all_to_all(sums, Z), lax.axis_size((X, Y, C)))
    next_vector, coefficients = last(entries, all_to_all(sums, (X, Y, C)), image, vector)
    return jnp.swapaxes(next_vector, 1, 2), coefficients


def solution(mesh):
    finer = Mesh(mesh.devices.reshape(4, 4, 4, 4, 2), (X, Y, FAR, NEAR, C))
    in_specs = (P(None, ROW, COL), P(None, ROW, COL), P(None, COL, ROW), P(), P())
    out_specs = (P(None, ROW, COL), P())
    return jax.shard_map(body, mesh=finer, in_specs=in_specs, out_specs=out_specs, check_vma=False)
```

```python
import jax
import jax.numpy as jnp
from jax import lax
from jax.experimental import pallas as pl
from jax.experimental.pallas import tpu as pltpu
from jax.sharding import Mesh
from jax.sharding import PartitionSpec as P

X, Y, FAR, NEAR, C = "row_0", "row_1", "far", "near", "core"
ROW = (X, Y)
Z = (FAR, NEAR)
COL = (FAR, NEAR, C)
STATES = 4
CHANNELS = 5

epsilon = 1e-06
SCALE = 8192.0

VMEM = pl.BlockSpec(memory_space=pltpu.VMEM)
SMEM = pl.BlockSpec(memory_space=pltpu.SMEM)
HBM = pl.BlockSpec(memory_space=pltpu.HBM)
SMALL = pltpu.CompilerParams(vmem_limit_bytes=4 * 1024 * 1024)
LARGE = pltpu.CompilerParams(vmem_limit_bytes=24 * 1024 * 1024)


def in_hbm(x):
    return pltpu.with_memory_space_constraint(x, pltpu.HBM)


def pack_kernel(vector_hbm, right_hbm, out_hbm, vector_s, right_s, turned_s, in_sems, out_sems):
    half, _ = right_s.shape[1:]
    rows = vector_s.shape[0]
    loads = [
        pltpu.make_async_copy(vector_hbm, vector_s, in_sems.at[0]),
        pltpu.make_async_copy(right_hbm, right_s, in_sems.at[1]),
    ]
    for load in loads:
        load.start()
    places = range(out_hbm.shape[0])
    stores = [pltpu.make_async_copy(vector_s, out_hbm.at[r, pl.ds(0, rows)], out_sems.at[0, r]) for r in places]
    loads[0].wait()
    for store in stores:
        store.start()
    loads[1].wait()
    for v in range(right_s.shape[0]):
        turned = right_s[v].astype(jnp.float32).T
        turned = jnp.concatenate([turned[:half], turned[half:]], 1).astype(jnp.bfloat16)
        turned_s[v * half : (v + 1) * half, :] = turned
    more = [pltpu.make_async_copy(turned_s, out_hbm.at[r, pl.ds(rows, turned_s.shape[0])], out_sems.at[1, r]) for r in places]
    for store in more:
        store.start()
    for store in stores + more:
        store.wait()


def pack(vector, right, size):
    rows, width = vector.shape
    channels, half, _ = right.shape
    return pl.pallas_call(
        pack_kernel,
        out_shape=pltpu.HBM((size, rows + channels * half, width), jnp.bfloat16),
        in_specs=[HBM, HBM],
        out_specs=HBM,
        scratch_shapes=[
            pltpu.VMEM(vector.shape, jnp.bfloat16),
            pltpu.VMEM(right.shape, jnp.bfloat16),
            pltpu.VMEM((channels * half, width), jnp.bfloat16),
            pltpu.SemaphoreType.DMA((2,)),
            pltpu.SemaphoreType.DMA((2, size)),
        ],
        compiler_params=SMALL,
    )(in_hbm(vector), in_hbm(right))


def site_copies(left_site, right_site, left_t, right_t, sems):
    loads = (
        pltpu.make_async_copy(left_site, left_t, sems.at[0]),
        pltpu.make_async_copy(right_site, right_t, sems.at[1]),
    )
    for load in loads:
        load.start()
    return loads


def combined(terms):
    total = None
    for scale, x in terms:
        total = scale * x if total is None else total + scale * x
    return total


def vector_copies(source, vec_s, sems):
    rows = vec_s.shape[0]
    width = source.shape[2]
    loads = [
        pltpu.make_async_copy(source.at[r, pl.ds(0, rows)], vec_s.at[:, pl.ds(r * width, width)], sems.at[r])
        for r in range(source.shape[0])
    ]
    for load in loads:
        load.start()
    return loads


def contract_and_mix(site_loads, left_t, right_t, left_ref, vec_s, cross_s, half_s, store):
    half = vec_s.shape[0] // STATES
    width = 2 * half
    cross_s[...] = jnp.dot(vec_s[...], left_ref[...], preferred_element_type=jnp.float32)
    for load in site_loads:
        load.wait()
    for s1 in range(2):
        for u in range(CHANNELS):
            for t2 in range(2):
                half_s[u, t2] = combined(
                    (
                        left_t[w, s1, t1, u],
                        cross_s[(2 * t1 + t2) * half : (2 * t1 + t2 + 1) * half, w * width : (w + 1) * width],
                    )
                    for w in range(CHANNELS)
                    for t1 in range(2)
                )
        for v in range(CHANNELS):
            for s2 in range(2):
                total = combined((right_t[u, s2, t2, v], half_s[u, t2]) for u in range(CHANNELS) for t2 in range(2))
                store(v, 2 * s1 + s2, total.astype(jnp.bfloat16))


def own_kernel(
    left_site, right_site, left_ref, own_hbm, left_out, mixed_out, right_out,
    left_t, right_t, vec_s, cross_s, half_s, vec_sems, right_sems, site_sems,
):
    width = own_hbm.shape[2]
    half = width // 2
    loads = vector_copies(own_hbm, vec_s, vec_sems)
    site_loads = site_copies(left_site, right_site, left_t, right_t, site_sems)
    passed = [
        pltpu.make_async_copy(
            own_hbm.at[:, pl.ds((STATES + v) * half, half)], right_out.at[:, :, pl.ds(v * width, width)], right_sems.at[v]
        )
        for v in range(CHANNELS)
    ]
    for copy in passed:
        copy.start()
    for k in range(left_ref.shape[0]):
        for w in range(CHANNELS):
            left_out[k * half : (k + 1) * half, w * width : (w + 1) * width] = left_ref[k, w * half : (w + 1) * half, :]
    for load in loads:
        load.wait()

    def store(v, s, x):
        mixed_out[v * half : (v + 1) * half, s * width : (s + 1) * width] = x

    contract_and_mix(site_loads, left_t, right_t, left_out, vec_s, cross_s, half_s, store)
    for copy in passed:
        copy.wait()


def own_part(sites, left, own):
    blocks, _, width = own.shape
    half = width // 2
    return pl.pallas_call(
        own_kernel,
        out_shape=(
            jax.ShapeDtypeStruct((left.shape[0] * half, CHANNELS * width), jnp.bfloat16),
            jax.ShapeDtypeStruct((CHANNELS * half, STATES * width), jnp.bfloat16),
            jax.ShapeDtypeStruct((blocks, half, CHANNELS * width), jnp.bfloat16),
        ),
        in_specs=[HBM, HBM, VMEM, HBM],
        out_specs=(VMEM, VMEM, VMEM),
        scratch_shapes=[
            *(pltpu.SMEM(site.shape, jnp.float32) for site in sites),
            pltpu.VMEM((STATES * half, blocks * width), jnp.bfloat16),
            pltpu.VMEM((STATES * half, CHANNELS * width), jnp.float32),
            pltpu.VMEM((CHANNELS, 2, half, width), jnp.float32),
            pltpu.SemaphoreType.DMA((blocks,)),
            pltpu.SemaphoreType.DMA((CHANNELS,)),
            pltpu.SemaphoreType.DMA((2,)),
        ],
        compiler_params=LARGE,
    )(*(in_hbm(site) for site in sites), left, in_hbm(own))


def terms_kernel(
    order, core_ref, left_site, right_site, left_ref, mixed_ref, right_own, other_hbm, out_ref,
    left_t, right_t, right_other, vec_s, cross_s, half_s, right_s, mixed_s, vec_sems, right_sem, site_sems,
):
    blocks, half, _ = out_ref.shape
    width = 2 * half
    core = core_ref[0]
    own_at = pl.multiple_of(core * half, half)
    other_at = pl.multiple_of((1 - core) * half, half)
    loads = vector_copies(other_hbm, vec_s, vec_sems)
    site_loads = site_copies(left_site, right_site, left_t, right_t, site_sems)
    right_load = pltpu.make_async_copy(other_hbm.at[:, pl.ds(STATES * half, CHANNELS * half)], right_other, right_sem)
    right_load.start()
    mine = lax.broadcasted_iota(jnp.int32, (half, width), 1) // half == core
    for v in range(CHANNELS):
        mixed_s[pl.ds(v * width + own_at, half), :] = mixed_ref[v * half : (v + 1) * half, :]
    for load in loads:
        load.wait()

    def store(v, s, x):
        mixed_s[pl.ds(v * width + other_at, half), s * width : (s + 1) * width] = x

    contract_and_mix(site_loads, left_t, right_t, left_ref, vec_s, cross_s, half_s, store)
    right_load.wait()
    for r in range(blocks):
        for v in range(CHANNELS):
            own = right_own[r, :, v * width : (v + 1) * width].astype(jnp.float32)
            other = right_other[r, v * half : (v + 1) * half, :].astype(jnp.float32)
            other = jnp.concatenate([other[:, half:], other[:, :half]], 1)
            right_s[r * half : (r + 1) * half, v * width : (v + 1) * width] = jnp.where(mine, own, other).astype(jnp.bfloat16)
    image = jnp.dot(right_s[...], mixed_s[...], preferred_element_type=jnp.float32)
    for r in range(blocks):
        out_ref[order[r]] = image[r * half : (r + 1) * half].astype(jnp.bfloat16)


def terms(order, core, sites, left, mixed, right, other):
    def step(*refs):
        terms_kernel(order, *refs)

    blocks, _, width = other.shape
    half = width // 2
    return pl.pallas_call(
        step,
        out_shape=jax.ShapeDtypeStruct((blocks, half, STATES * width), jnp.bfloat16),
        in_specs=[SMEM, HBM, HBM, VMEM, VMEM, VMEM, HBM],
        out_specs=VMEM,
        scratch_shapes=[
            *(pltpu.SMEM(site.shape, jnp.float32) for site in sites),
            pltpu.VMEM((blocks, CHANNELS * half, width), jnp.bfloat16),
            pltpu.VMEM((STATES * half, blocks * width), jnp.bfloat16),
            pltpu.VMEM((STATES * half, CHANNELS * width), jnp.float32),
            pltpu.VMEM((CHANNELS, 2, half, width), jnp.float32),
            pltpu.VMEM((blocks * half, CHANNELS * width), jnp.bfloat16),
            pltpu.VMEM((CHANNELS * width, STATES * width), jnp.bfloat16),
            pltpu.SemaphoreType.DMA((blocks,)),
            pltpu.SemaphoreType.DMA,
            pltpu.SemaphoreType.DMA((2,)),
        ],
        compiler_params=LARGE,
    )(core, *(in_hbm(site) for site in sites), left, mixed, right, in_hbm(other))


def near_kernel(pieces_ref, out_ref):
    for j in range(out_ref.shape[0]):
        total = pieces_ref[0, j].astype(jnp.float32)
        for k in range(1, pieces_ref.shape[0]):
            total = total + pieces_ref[k, j].astype(jnp.float32)
        out_ref[j] = total.astype(jnp.bfloat16)


def near_sum(pieces):
    return pl.pallas_call(
        near_kernel,
        out_shape=jax.ShapeDtypeStruct(pieces.shape[1:], jnp.bfloat16),
        in_specs=[VMEM],
        out_specs=VMEM,
        compiler_params=SMALL,
    )(pieces)


def neighbours(n_far, n_near):
    n_z = n_far * n_near
    groups = []
    for core in range(2):
        for j in range(n_far):
            first = j * n_near + core * (n_near // 2)
            chips = sorted(((first + i) % n_z for i in range(n_near)), key=lambda z: z % n_near)
            groups.append([2 * z + core for z in chips])
    return groups


def lanes_of(total):
    rows, cols = total.shape
    total = sum(total[:, k : k + 128] for k in range(0, cols, 128))
    return sum(total[k : k + 8] for k in range(0, rows, 8))


def sums_kernel(pieces_ref, vector_ref, image_ref, sums_ref):
    image = pieces_ref[0].astype(jnp.float32)
    for k in range(1, pieces_ref.shape[0]):
        image = image + pieces_ref[k].astype(jnp.float32)
    image_ref[...] = image
    base = jnp.concatenate([vector_ref[t].astype(jnp.float32) for t in range(STATES)], 1)
    found = [lanes_of(base * base), lanes_of(base * image), lanes_of(image * image)]
    lane = lax.broadcasted_iota(jnp.int32, (1, 128), 1)
    row = jnp.zeros((1, 128), jnp.float32)
    for k in range(3):
        row = jnp.where(lane == k, jnp.sum(found[k], keepdims=True), row)
    for r in range(sums_ref.shape[0]):
        sums_ref[r] = row


def sums_of(pieces, vector, size):
    return pl.pallas_call(
        sums_kernel,
        out_shape=(
            jax.ShapeDtypeStruct(pieces.shape[1:], jnp.float32),
            jax.ShapeDtypeStruct((size, 1, 128), jnp.float32),
        ),
        in_specs=[VMEM, VMEM],
        out_specs=(VMEM, VMEM),
        compiler_params=SMALL,
    )(pieces, vector)


def again_kernel(pieces_ref, out_ref):
    total = pieces_ref[0]
    for k in range(1, pieces_ref.shape[0]):
        total = total + pieces_ref[k]
    for r in range(out_ref.shape[0]):
        out_ref[r] = total


def again(pieces, size):
    return pl.pallas_call(
        again_kernel,
        out_shape=jax.ShapeDtypeStruct((size, *pieces.shape[1:]), jnp.float32),
        in_specs=[VMEM],
        out_specs=VMEM,
        compiler_params=SMALL,
    )(pieces)


def last_kernel(entries, pieces_ref, image_ref, vector_ref, next_ref, coefficients_ref):
    total = pieces_ref[0]
    for k in range(1, pieces_ref.shape[0]):
        total = total + pieces_ref[k]
    total = total / entries
    lane = lax.broadcasted_iota(jnp.int32, total.shape, 1)
    base_square, correlation, image_square = (
        jnp.sum(jnp.where(lane == k, total, 0.0), 1, keepdims=True) for k in range(3)
    )
    alpha = correlation / (base_square + epsilon)
    rho = jnp.sqrt(image_square - 2.0 * alpha * correlation + alpha * alpha * base_square + epsilon)
    width = next_ref.shape[2]
    for t in range(STATES):
        residual = image_ref[:, t * width : (t + 1) * width] - alpha * vector_ref[t].astype(jnp.float32)
        next_ref[t] = (residual / rho).astype(jnp.bfloat16)
    coefficients_ref[0] = alpha[0, 0]
    coefficients_ref[1] = rho[0, 0]


def last(entries, pieces, image, vector):
    def step(*refs):
        last_kernel(entries, *refs)

    return pl.pallas_call(
        step,
        out_shape=(
            jax.ShapeDtypeStruct(vector.shape, jnp.bfloat16),
            jax.ShapeDtypeStruct((2,), jnp.float32),
        ),
        in_specs=[VMEM, VMEM, VMEM],
        out_specs=(VMEM, SMEM),
        compiler_params=SMALL,
    )(pieces, image, vector)


def all_to_all(x, axes):
    return lax.all_to_all(x, axes, 0, 0, tiled=True)


def other_core(x):
    return lax.ppermute(x, C, [(0, 1), (1, 0)])


def body(start_vector, left_env, right_env, left_tensor, right_tensor):
    n_row = lax.axis_size(ROW)
    n_far, n_near = lax.axis_size(FAR), lax.axis_size(NEAR)
    n_z = n_far * n_near
    _, rows, half = start_vector.shape
    entries = float(STATES * rows * half * n_row * n_z * lax.axis_size(C))
    core = lax.axis_index(C).astype(jnp.int32).reshape(1)
    sites = tuple(jnp.transpose(tensor, (0, 2, 3, 1)) for tensor in (left_tensor, right_tensor))
    vector = jnp.swapaxes(start_vector, 1, 2)
    left = jnp.swapaxes(left_env, 1, 2).reshape(CHANNELS * half, rows)
    left = (left.astype(jnp.float32) * SCALE).astype(jnp.float16)

    own = all_to_all(pack(vector.reshape(STATES * half, rows), right_env, n_row), ROW)
    left = lax.all_gather(left, COL, axis=0)
    own, left = lax.optimization_barrier((own, left))
    left = (left.astype(jnp.float32) * (1.0 / SCALE)).astype(jnp.bfloat16)
    order = [n_far * (z % n_near) + z // n_near for z in range(n_z)]
    other = other_core(own)
    left, mixed, right = own_part(sites, left, own)
    sent = terms(order, core, sites, left, mixed, right, other)

    pieces = lax.all_to_all(sent, COL, 0, 0, axis_index_groups=neighbours(n_far, n_near), tiled=True)
    pieces = all_to_all(near_sum(pieces.reshape(n_near, n_far, *pieces.shape[1:])), FAR)
    image, sums = sums_of(pieces, vector, lax.axis_size((X, Y, C)))
    sums = again(all_to_all(sums, (X, Y, C)), n_z)
    next_vector, coefficients = last(entries, all_to_all(sums, Z), image, vector)
    return jnp.swapaxes(next_vector, 1, 2), coefficients


def solution(mesh):
    finer = Mesh(mesh.devices.reshape(4, 4, 4, 4, 2), (X, Y, FAR, NEAR, C))
    in_specs = (P(None, ROW, COL), P(None, ROW, COL), P(None, COL, ROW), P(), P())
    out_specs = (P(None, ROW, COL), P())
    return jax.shard_map(body, mesh=finer, in_specs=in_specs, out_specs=out_specs, check_vma=False)
```

```python
import jax
import jax.numpy as jnp
from jax import lax
from jax.experimental import pallas as pl
from jax.experimental.pallas import tpu as pltpu
from jax.sharding import Mesh
from jax.sharding import PartitionSpec as P

X, Y, FAR, NEAR, C = "row_0", "row_1", "far", "near", "core"
ROW = (X, Y)
Z = (FAR, NEAR)
COL = (FAR, NEAR, C)
STATES = 4
CHANNELS = 5

epsilon = 1e-06
SCALE = 8192.0

VMEM = pl.BlockSpec(memory_space=pltpu.VMEM)
SMEM = pl.BlockSpec(memory_space=pltpu.SMEM)
HBM = pl.BlockSpec(memory_space=pltpu.HBM)
SMALL = pltpu.CompilerParams(vmem_limit_bytes=4 * 1024 * 1024)
LARGE = pltpu.CompilerParams(vmem_limit_bytes=24 * 1024 * 1024)


def in_hbm(x):
    return pltpu.with_memory_space_constraint(x, pltpu.HBM)


def pack_kernel(vector_hbm, right_hbm, out_hbm, vector_s, right_s, turned_s, in_sems, out_sems):
    half, _ = right_s.shape[1:]
    rows = vector_s.shape[0]
    loads = [
        pltpu.make_async_copy(vector_hbm, vector_s, in_sems.at[0]),
        pltpu.make_async_copy(right_hbm, right_s, in_sems.at[1]),
    ]
    for load in loads:
        load.start()
    places = range(out_hbm.shape[0])
    stores = [pltpu.make_async_copy(vector_s, out_hbm.at[r, pl.ds(0, rows)], out_sems.at[0, r]) for r in places]
    loads[0].wait()
    for store in stores:
        store.start()
    loads[1].wait()
    for v in range(right_s.shape[0]):
        turned = right_s[v].astype(jnp.float32).T
        turned = jnp.concatenate([turned[:half], turned[half:]], 1).astype(jnp.bfloat16)
        turned_s[v * half : (v + 1) * half, :] = turned
    more = [pltpu.make_async_copy(turned_s, out_hbm.at[r, pl.ds(rows, turned_s.shape[0])], out_sems.at[1, r]) for r in places]
    for store in more:
        store.start()
    for store in stores + more:
        store.wait()


def pack(vector, right, size):
    rows, width = vector.shape
    channels, half, _ = right.shape
    return pl.pallas_call(
        pack_kernel,
        out_shape=pltpu.HBM((size, rows + channels * half, width), jnp.bfloat16),
        in_specs=[HBM, HBM],
        out_specs=HBM,
        scratch_shapes=[
            pltpu.VMEM(vector.shape, jnp.bfloat16),
            pltpu.VMEM(right.shape, jnp.bfloat16),
            pltpu.VMEM((channels * half, width), jnp.bfloat16),
            pltpu.SemaphoreType.DMA((2,)),
            pltpu.SemaphoreType.DMA((2, size)),
        ],
        compiler_params=SMALL,
    )(in_hbm(vector), in_hbm(right))


def site_copies(left_site, right_site, left_t, right_t, sems):
    loads = (
        pltpu.make_async_copy(left_site, left_t, sems.at[0]),
        pltpu.make_async_copy(right_site, right_t, sems.at[1]),
    )
    for load in loads:
        load.start()
    return loads


def combined(terms):
    total = None
    for scale, x in terms:
        total = scale * x if total is None else total + scale * x
    return total


def vector_copies(source, vec_s, sems):
    rows = vec_s.shape[0]
    width = source.shape[2]
    loads = [
        pltpu.make_async_copy(source.at[r, pl.ds(0, rows)], vec_s.at[:, pl.ds(r * width, width)], sems.at[r])
        for r in range(source.shape[0])
    ]
    for load in loads:
        load.start()
    return loads


def contract_and_mix(loads, place_left, site_loads, left_t, right_t, left_ref, vec_s, cross_s, half_s, store):
    half = vec_s.shape[0] // STATES
    width = 2 * half
    parts = 2
    depth = vec_s.shape[1] // parts
    for g in range(parts):
        place_left(g, parts)
        for load in loads[g * len(loads) // parts : (g + 1) * len(loads) // parts]:
            load.wait()
        at = slice(g * depth, (g + 1) * depth)
        part = jnp.dot(vec_s[:, at], left_ref[at, :], preferred_element_type=jnp.float32)
        cross_s[...] = part if g == 0 else cross_s[...] + part
    for load in site_loads:
        load.wait()
    for s1 in range(2):
        for u in range(CHANNELS):
            for t2 in range(2):
                half_s[u, t2] = combined(
                    (
                        left_t[w, s1, t1, u],
                        cross_s[(2 * t1 + t2) * half : (2 * t1 + t2 + 1) * half, w * width : (w + 1) * width],
                    )
                    for w in range(CHANNELS)
                    for t1 in range(2)
                )
        for v in range(CHANNELS):
            for s2 in range(2):
                total = combined((right_t[u, s2, t2, v], half_s[u, t2]) for u in range(CHANNELS) for t2 in range(2))
                store(v, 2 * s1 + s2, total.astype(jnp.bfloat16))


def own_kernel(
    left_site, right_site, left_ref, own_hbm, left_out, mixed_out, right_out,
    left_t, right_t, vec_s, cross_s, half_s, vec_sems, right_sems, site_sems,
):
    width = own_hbm.shape[2]
    half = width // 2
    loads = vector_copies(own_hbm, vec_s, vec_sems)
    site_loads = site_copies(left_site, right_site, left_t, right_t, site_sems)
    passed = [
        pltpu.make_async_copy(
            own_hbm.at[:, pl.ds((STATES + v) * half, half)], right_out.at[:, :, pl.ds(v * width, width)], right_sems.at[v]
        )
        for v in range(CHANNELS)
    ]
    for copy in passed:
        copy.start()

    def place_left(g, parts):
        count = left_ref.shape[0] // parts
        for k in range(g * count, (g + 1) * count):
            for w in range(CHANNELS):
                left_out[k * half : (k + 1) * half, w * width : (w + 1) * width] = left_ref[k, w * half : (w + 1) * half, :]

    def store(v, s, x):
        mixed_out[v * half : (v + 1) * half, s * width : (s + 1) * width] = x

    contract_and_mix(loads, place_left, site_loads, left_t, right_t, left_out, vec_s, cross_s, half_s, store)
    for copy in passed:
        copy.wait()


def own_part(sites, left, own):
    blocks, _, width = own.shape
    half = width // 2
    return pl.pallas_call(
        own_kernel,
        out_shape=(
            jax.ShapeDtypeStruct((left.shape[0] * half, CHANNELS * width), jnp.bfloat16),
            jax.ShapeDtypeStruct((CHANNELS * half, STATES * width), jnp.bfloat16),
            jax.ShapeDtypeStruct((blocks, half, CHANNELS * width), jnp.bfloat16),
        ),
        in_specs=[HBM, HBM, VMEM, HBM],
        out_specs=(VMEM, VMEM, VMEM),
        scratch_shapes=[
            *(pltpu.SMEM(site.shape, jnp.float32) for site in sites),
            pltpu.VMEM((STATES * half, blocks * width), jnp.bfloat16),
            pltpu.VMEM((STATES * half, CHANNELS * width), jnp.float32),
            pltpu.VMEM((CHANNELS, 2, half, width), jnp.float32),
            pltpu.SemaphoreType.DMA((blocks,)),
            pltpu.SemaphoreType.DMA((CHANNELS,)),
            pltpu.SemaphoreType.DMA((2,)),
        ],
        compiler_params=LARGE,
    )(*(in_hbm(site) for site in sites), left, in_hbm(own))


def terms_kernel(
    order, core_ref, left_site, right_site, left_ref, mixed_ref, right_own, other_hbm, out_ref,
    left_t, right_t, right_other, vec_s, cross_s, half_s, right_s, mixed_s, vec_sems, right_sem, site_sems,
):
    blocks, half, _ = out_ref.shape
    width = 2 * half
    core = core_ref[0]
    own_at = pl.multiple_of(core * half, half)
    other_at = pl.multiple_of((1 - core) * half, half)
    loads = vector_copies(other_hbm, vec_s, vec_sems)
    site_loads = site_copies(left_site, right_site, left_t, right_t, site_sems)
    right_load = pltpu.make_async_copy(other_hbm.at[:, pl.ds(STATES * half, CHANNELS * half)], right_other, right_sem)
    right_load.start()
    mine = lax.broadcasted_iota(jnp.int32, (half, width), 1) // half == core
    for v in range(CHANNELS):
        mixed_s[pl.ds(v * width + own_at, half), :] = mixed_ref[v * half : (v + 1) * half, :]

    def store(v, s, x):
        mixed_s[pl.ds(v * width + other_at, half), s * width : (s + 1) * width] = x

    contract_and_mix(loads, lambda g, parts: None, site_loads, left_t, right_t, left_ref, vec_s, cross_s, half_s, store)
    right_load.wait()
    for r in range(blocks):
        for v in range(CHANNELS):
            own = right_own[r, :, v * width : (v + 1) * width].astype(jnp.float32)
            other = right_other[r, v * half : (v + 1) * half, :].astype(jnp.float32)
            other = jnp.concatenate([other[:, half:], other[:, :half]], 1)
            right_s[r * half : (r + 1) * half, v * width : (v + 1) * width] = jnp.where(mine, own, other).astype(jnp.bfloat16)
    image = jnp.dot(right_s[...], mixed_s[...], preferred_element_type=jnp.float32)
    for r in range(blocks):
        out_ref[order[r]] = image[r * half : (r + 1) * half].astype(jnp.bfloat16)


def terms(order, core, sites, left, mixed, right, other):
    def step(*refs):
        terms_kernel(order, *refs)

    blocks, _, width = other.shape
    half = width // 2
    return pl.pallas_call(
        step,
        out_shape=jax.ShapeDtypeStruct((blocks, half, STATES * width), jnp.bfloat16),
        in_specs=[SMEM, HBM, HBM, VMEM, VMEM, VMEM, HBM],
        out_specs=VMEM,
        scratch_shapes=[
            *(pltpu.SMEM(site.shape, jnp.float32) for site in sites),
            pltpu.VMEM((blocks, CHANNELS * half, width), jnp.bfloat16),
            pltpu.VMEM((STATES * half, blocks * width), jnp.bfloat16),
            pltpu.VMEM((STATES * half, CHANNELS * width), jnp.float32),
            pltpu.VMEM((CHANNELS, 2, half, width), jnp.float32),
            pltpu.VMEM((blocks * half, CHANNELS * width), jnp.bfloat16),
            pltpu.VMEM((CHANNELS * width, STATES * width), jnp.bfloat16),
            pltpu.SemaphoreType.DMA((blocks,)),
            pltpu.SemaphoreType.DMA,
            pltpu.SemaphoreType.DMA((2,)),
        ],
        compiler_params=LARGE,
    )(core, *(in_hbm(site) for site in sites), left, mixed, right, in_hbm(other))


def near_kernel(pieces_ref, out_ref):
    for j in range(out_ref.shape[0]):
        total = pieces_ref[0, j].astype(jnp.float32)
        for k in range(1, pieces_ref.shape[0]):
            total = total + pieces_ref[k, j].astype(jnp.float32)
        out_ref[j] = total.astype(jnp.bfloat16)


def near_sum(pieces):
    return pl.pallas_call(
        near_kernel,
        out_shape=jax.ShapeDtypeStruct(pieces.shape[1:], jnp.bfloat16),
        in_specs=[VMEM],
        out_specs=VMEM,
        compiler_params=SMALL,
    )(pieces)


def neighbours(n_far, n_near):
    n_z = n_far * n_near
    groups = []
    for core in range(2):
        for j in range(n_far):
            first = j * n_near + core * (n_near // 2)
            chips = sorted(((first + i) % n_z for i in range(n_near)), key=lambda z: z % n_near)
            groups.append([2 * z + core for z in chips])
    return groups


def lanes_of(total):
    rows, cols = total.shape
    total = sum(total[:, k : k + 128] for k in range(0, cols, 128))
    return sum(total[k : k + 8] for k in range(0, rows, 8))


def sums_kernel(pieces_ref, vector_ref, image_ref, sums_ref):
    image = pieces_ref[0].astype(jnp.float32)
    for k in range(1, pieces_ref.shape[0]):
        image = image + pieces_ref[k].astype(jnp.float32)
    image_ref[...] = image
    base = jnp.concatenate([vector_ref[t].astype(jnp.float32) for t in range(STATES)], 1)
    found = [lanes_of(base * base), lanes_of(base * image), lanes_of(image * image)]
    lane = lax.broadcasted_iota(jnp.int32, (1, 128), 1)
    row = jnp.zeros((1, 128), jnp.float32)
    for k in range(3):
        row = jnp.where(lane == k, jnp.sum(found[k], keepdims=True), row)
    for r in range(sums_ref.shape[0]):
        sums_ref[r] = row


def sums_of(pieces, vector, size):
    return pl.pallas_call(
        sums_kernel,
        out_shape=(
            jax.ShapeDtypeStruct(pieces.shape[1:], jnp.float32),
            jax.ShapeDtypeStruct((size, 1, 128), jnp.float32),
        ),
        in_specs=[VMEM, VMEM],
        out_specs=(VMEM, VMEM),
        compiler_params=SMALL,
    )(pieces, vector)


def again_kernel(pieces_ref, out_ref):
    total = pieces_ref[0]
    for k in range(1, pieces_ref.shape[0]):
        total = total + pieces_ref[k]
    for r in range(out_ref.shape[0]):
        out_ref[r] = total


def again(pieces, size):
    return pl.pallas_call(
        again_kernel,
        out_shape=jax.ShapeDtypeStruct((size, *pieces.shape[1:]), jnp.float32),
        in_specs=[VMEM],
        out_specs=VMEM,
        compiler_params=SMALL,
    )(pieces)


def last_kernel(entries, pieces_ref, image_ref, vector_ref, next_ref, coefficients_ref):
    total = pieces_ref[0]
    for k in range(1, pieces_ref.shape[0]):
        total = total + pieces_ref[k]
    total = total / entries
    lane = lax.broadcasted_iota(jnp.int32, total.shape, 1)
    base_square, correlation, image_square = (
        jnp.sum(jnp.where(lane == k, total, 0.0), 1, keepdims=True) for k in range(3)
    )
    alpha = correlation / (base_square + epsilon)
    rho = jnp.sqrt(image_square - 2.0 * alpha * correlation + alpha * alpha * base_square + epsilon)
    width = next_ref.shape[2]
    for t in range(STATES):
        residual = image_ref[:, t * width : (t + 1) * width] - alpha * vector_ref[t].astype(jnp.float32)
        next_ref[t] = (residual / rho).astype(jnp.bfloat16)
    coefficients_ref[0] = alpha[0, 0]
    coefficients_ref[1] = rho[0, 0]


def last(entries, pieces, image, vector):
    def step(*refs):
        last_kernel(entries, *refs)

    return pl.pallas_call(
        step,
        out_shape=(
            jax.ShapeDtypeStruct(vector.shape, jnp.bfloat16),
            jax.ShapeDtypeStruct((2,), jnp.float32),
        ),
        in_specs=[VMEM, VMEM, VMEM],
        out_specs=(VMEM, SMEM),
        compiler_params=SMALL,
    )(pieces, image, vector)


def all_to_all(x, axes):
    return lax.all_to_all(x, axes, 0, 0, tiled=True)


def other_core(x):
    return lax.ppermute(x, C, [(0, 1), (1, 0)])


def body(start_vector, left_env, right_env, left_tensor, right_tensor):
    n_row = lax.axis_size(ROW)
    n_far, n_near = lax.axis_size(FAR), lax.axis_size(NEAR)
    n_z = n_far * n_near
    _, rows, half = start_vector.shape
    entries = float(STATES * rows * half * n_row * n_z * lax.axis_size(C))
    core = lax.axis_index(C).astype(jnp.int32).reshape(1)
    sites = tuple(jnp.transpose(tensor, (0, 2, 3, 1)) for tensor in (left_tensor, right_tensor))
    vector = jnp.swapaxes(start_vector, 1, 2)
    left = jnp.swapaxes(left_env, 1, 2).reshape(CHANNELS * half, rows)
    left = (left.astype(jnp.float32) * SCALE).astype(jnp.float16)

    own = all_to_all(pack(vector.reshape(STATES * half, rows), right_env, n_row), ROW)
    left = lax.all_gather(left, COL, axis=0)
    own, left = lax.optimization_barrier((own, left))
    left = (left.astype(jnp.float32) * (1.0 / SCALE)).astype(jnp.bfloat16)
    order = [n_far * (z % n_near) + z // n_near for z in range(n_z)]
    other = other_core(own)
    left, mixed, right = own_part(sites, left, own)
    sent = terms(order, core, sites, left, mixed, right, other)

    pieces = lax.all_to_all(sent, COL, 0, 0, axis_index_groups=neighbours(n_far, n_near), tiled=True)
    pieces = all_to_all(near_sum(pieces.reshape(n_near, n_far, *pieces.shape[1:])), FAR)
    image, sums = sums_of(pieces, vector, lax.axis_size((X, Y, C)))
    sums = again(all_to_all(sums, (X, Y, C)), n_z)
    next_vector, coefficients = last(entries, all_to_all(sums, Z), image, vector)
    return jnp.swapaxes(next_vector, 1, 2), coefficients


def solution(mesh):
    finer = Mesh(mesh.devices.reshape(4, 4, 4, 4, 2), (X, Y, FAR, NEAR, C))
    in_specs = (P(None, ROW, COL), P(None, ROW, COL), P(None, COL, ROW), P(), P())
    out_specs = (P(None, ROW, COL), P())
    return jax.shard_map(body, mesh=finer, in_specs=in_specs, out_specs=out_specs, check_vma=False)
```

```python
import jax
import jax.numpy as jnp
from jax import lax
from jax.experimental import pallas as pl
from jax.experimental.pallas import tpu as pltpu
from jax.sharding import Mesh
from jax.sharding import PartitionSpec as P

X, Y, FAR, NEAR, C = "row_0", "row_1", "far", "near", "core"
ROW = (X, Y)
Z = (FAR, NEAR)
COL = (FAR, NEAR, C)
STATES = 4
CHANNELS = 5

epsilon = 1e-06
SCALE = 8192.0

VMEM = pl.BlockSpec(memory_space=pltpu.VMEM)
SMEM = pl.BlockSpec(memory_space=pltpu.SMEM)
HBM = pl.BlockSpec(memory_space=pltpu.HBM)
SMALL = pltpu.CompilerParams(vmem_limit_bytes=4 * 1024 * 1024)
LARGE = pltpu.CompilerParams(vmem_limit_bytes=24 * 1024 * 1024)


def in_hbm(x):
    return pltpu.with_memory_space_constraint(x, pltpu.HBM)


def pack_kernel(vector_hbm, right_hbm, out_hbm, vector_s, right_s, turned_s, in_sems, out_sems):
    half, _ = right_s.shape[1:]
    rows = vector_s.shape[0]
    loads = [
        pltpu.make_async_copy(vector_hbm, vector_s, in_sems.at[0]),
        pltpu.make_async_copy(right_hbm, right_s, in_sems.at[1]),
    ]
    for load in loads:
        load.start()
    places = range(out_hbm.shape[0])
    stores = [pltpu.make_async_copy(vector_s, out_hbm.at[r, pl.ds(0, rows)], out_sems.at[0, r]) for r in places]
    loads[0].wait()
    for store in stores:
        store.start()
    loads[1].wait()
    for v in range(right_s.shape[0]):
        turned = right_s[v].astype(jnp.float32).T
        turned = jnp.concatenate([turned[:half], turned[half:]], 1).astype(jnp.bfloat16)
        turned_s[v * half : (v + 1) * half, :] = turned
    more = [pltpu.make_async_copy(turned_s, out_hbm.at[r, pl.ds(rows, turned_s.shape[0])], out_sems.at[1, r]) for r in places]
    for store in more:
        store.start()
    for store in stores + more:
        store.wait()


def pack(vector, right, size):
    rows, width = vector.shape
    channels, half, _ = right.shape
    return pl.pallas_call(
        pack_kernel,
        out_shape=pltpu.HBM((size, rows + channels * half, width), jnp.bfloat16),
        in_specs=[HBM, HBM],
        out_specs=HBM,
        scratch_shapes=[
            pltpu.VMEM(vector.shape, jnp.bfloat16),
            pltpu.VMEM(right.shape, jnp.bfloat16),
            pltpu.VMEM((channels * half, width), jnp.bfloat16),
            pltpu.SemaphoreType.DMA((2,)),
            pltpu.SemaphoreType.DMA((2, size)),
        ],
        compiler_params=SMALL,
    )(in_hbm(vector), in_hbm(right))


def site_copies(left_site, right_site, left_t, right_t, sems):
    loads = (
        pltpu.make_async_copy(left_site, left_t, sems.at[0]),
        pltpu.make_async_copy(right_site, right_t, sems.at[1]),
    )
    for load in loads:
        load.start()
    return loads


def combined(terms):
    total = None
    for scale, x in terms:
        total = scale * x if total is None else total + scale * x
    return total


def vector_copies(source, vec_s, sems):
    rows = vec_s.shape[0]
    width = source.shape[2]
    loads = [
        pltpu.make_async_copy(source.at[r, pl.ds(0, rows)], vec_s.at[:, pl.ds(r * width, width)], sems.at[r])
        for r in range(source.shape[0])
    ]
    for load in loads:
        load.start()
    return loads


def contract_and_mix(site_loads, left_t, right_t, left_ref, vec_s, cross_s, half_s, store):
    half = vec_s.shape[0] // STATES
    width = 2 * half
    cross_s[...] = jnp.dot(vec_s[...], left_ref[...], preferred_element_type=jnp.float32)
    for load in site_loads:
        load.wait()
    for s1 in range(2):
        for u in range(CHANNELS):
            for t2 in range(2):
                half_s[u, t2] = combined(
                    (
                        left_t[w, s1, t1, u],
                        cross_s[(2 * t1 + t2) * half : (2 * t1 + t2 + 1) * half, w * width : (w + 1) * width],
                    )
                    for w in range(CHANNELS)
                    for t1 in range(2)
                )
        for v in range(CHANNELS):
            for s2 in range(2):
                total = combined((right_t[u, s2, t2, v], half_s[u, t2]) for u in range(CHANNELS) for t2 in range(2))
                store(v, 2 * s1 + s2, total.astype(jnp.bfloat16))


def own_kernel(
    left_site, right_site, left_ref, own_hbm, mixed_out, right_out,
    left_t, right_t, vec_s, cross_s, half_s, vec_sems, right_sems, site_sems,
):
    width = own_hbm.shape[2]
    half = width // 2
    loads = vector_copies(own_hbm, vec_s, vec_sems)
    site_loads = site_copies(left_site, right_site, left_t, right_t, site_sems)
    passed = [
        pltpu.make_async_copy(
            own_hbm.at[:, pl.ds((STATES + v) * half, half)], right_out.at[:, :, pl.ds(v * width, width)], right_sems.at[v]
        )
        for v in range(CHANNELS)
    ]
    for copy in passed:
        copy.start()
    for load in loads:
        load.wait()

    def store(v, s, x):
        mixed_out[v * half : (v + 1) * half, s * width : (s + 1) * width] = x

    contract_and_mix(site_loads, left_t, right_t, left_ref, vec_s, cross_s, half_s, store)
    for copy in passed:
        copy.wait()


def own_part(sites, left, own):
    blocks, _, width = own.shape
    half = width // 2
    return pl.pallas_call(
        own_kernel,
        out_shape=(
            jax.ShapeDtypeStruct((CHANNELS * half, STATES * width), jnp.bfloat16),
            jax.ShapeDtypeStruct((blocks, half, CHANNELS * width), jnp.bfloat16),
        ),
        in_specs=[HBM, HBM, VMEM, HBM],
        out_specs=(VMEM, VMEM),
        scratch_shapes=[
            *(pltpu.SMEM(site.shape, jnp.float32) for site in sites),
            pltpu.VMEM((STATES * half, blocks * width), jnp.bfloat16),
            pltpu.VMEM((STATES * half, CHANNELS * width), jnp.float32),
            pltpu.VMEM((CHANNELS, 2, half, width), jnp.float32),
            pltpu.SemaphoreType.DMA((blocks,)),
            pltpu.SemaphoreType.DMA((CHANNELS,)),
            pltpu.SemaphoreType.DMA((2,)),
        ],
        compiler_params=LARGE,
    )(*(in_hbm(site) for site in sites), left, in_hbm(own))


def terms_kernel(
    order, core_ref, left_site, right_site, left_ref, mixed_ref, right_own, other_hbm, out_ref,
    left_t, right_t, right_other, vec_s, cross_s, half_s, right_s, mixed_s, vec_sems, right_sem, site_sems,
):
    blocks, half, _ = out_ref.shape
    width = 2 * half
    core = core_ref[0]
    own_at = pl.multiple_of(core * half, half)
    other_at = pl.multiple_of((1 - core) * half, half)
    loads = vector_copies(other_hbm, vec_s, vec_sems)
    site_loads = site_copies(left_site, right_site, left_t, right_t, site_sems)
    right_load = pltpu.make_async_copy(other_hbm.at[:, pl.ds(STATES * half, CHANNELS * half)], right_other, right_sem)
    right_load.start()
    mine = lax.broadcasted_iota(jnp.int32, (half, width), 1) // half == core
    for v in range(CHANNELS):
        mixed_s[pl.ds(v * width + own_at, half), :] = mixed_ref[v * half : (v + 1) * half, :]
    for load in loads:
        load.wait()

    def store(v, s, x):
        mixed_s[pl.ds(v * width + other_at, half), s * width : (s + 1) * width] = x

    contract_and_mix(site_loads, left_t, right_t, left_ref, vec_s, cross_s, half_s, store)
    right_load.wait()
    for r in range(blocks):
        for v in range(CHANNELS):
            own = right_own[r, :, v * width : (v + 1) * width].astype(jnp.float32)
            other = right_other[r, v * half : (v + 1) * half, :].astype(jnp.float32)
            other = jnp.concatenate([other[:, half:], other[:, :half]], 1)
            right_s[r * half : (r + 1) * half, v * width : (v + 1) * width] = jnp.where(mine, own, other).astype(jnp.bfloat16)
    image = jnp.dot(right_s[...], mixed_s[...], preferred_element_type=jnp.float32)
    for r in range(blocks):
        out_ref[order[r]] = image[r * half : (r + 1) * half].astype(jnp.bfloat16)


def terms(order, core, sites, left, mixed, right, other):
    def step(*refs):
        terms_kernel(order, *refs)

    blocks, _, width = other.shape
    half = width // 2
    return pl.pallas_call(
        step,
        out_shape=jax.ShapeDtypeStruct((blocks, half, STATES * width), jnp.bfloat16),
        in_specs=[SMEM, HBM, HBM, VMEM, VMEM, VMEM, HBM],
        out_specs=VMEM,
        scratch_shapes=[
            *(pltpu.SMEM(site.shape, jnp.float32) for site in sites),
            pltpu.VMEM((blocks, CHANNELS * half, width), jnp.bfloat16),
            pltpu.VMEM((STATES * half, blocks * width), jnp.bfloat16),
            pltpu.VMEM((STATES * half, CHANNELS * width), jnp.float32),
            pltpu.VMEM((CHANNELS, 2, half, width), jnp.float32),
            pltpu.VMEM((blocks * half, CHANNELS * width), jnp.bfloat16),
            pltpu.VMEM((CHANNELS * width, STATES * width), jnp.bfloat16),
            pltpu.SemaphoreType.DMA((blocks,)),
            pltpu.SemaphoreType.DMA,
            pltpu.SemaphoreType.DMA((2,)),
        ],
        compiler_params=LARGE,
    )(core, *(in_hbm(site) for site in sites), left, mixed, right, in_hbm(other))


def near_kernel(pieces_ref, out_ref):
    for j in range(out_ref.shape[0]):
        total = pieces_ref[0, j].astype(jnp.float32)
        for k in range(1, pieces_ref.shape[0]):
            total = total + pieces_ref[k, j].astype(jnp.float32)
        out_ref[j] = total.astype(jnp.bfloat16)


def near_sum(pieces):
    return pl.pallas_call(
        near_kernel,
        out_shape=jax.ShapeDtypeStruct(pieces.shape[1:], jnp.bfloat16),
        in_specs=[VMEM],
        out_specs=VMEM,
        compiler_params=SMALL,
    )(pieces)


def neighbours(n_far, n_near):
    n_z = n_far * n_near
    groups = []
    for core in range(2):
        for j in range(n_far):
            first = j * n_near + core * (n_near // 2)
            chips = sorted(((first + i) % n_z for i in range(n_near)), key=lambda z: z % n_near)
            groups.append([2 * z + core for z in chips])
    return groups


def lanes_of(total):
    rows, cols = total.shape
    total = sum(total[:, k : k + 128] for k in range(0, cols, 128))
    return sum(total[k : k + 8] for k in range(0, rows, 8))


def sums_kernel(pieces_ref, vector_ref, image_ref, sums_ref):
    image = pieces_ref[0].astype(jnp.float32)
    for k in range(1, pieces_ref.shape[0]):
        image = image + pieces_ref[k].astype(jnp.float32)
    image_ref[...] = image
    base = jnp.concatenate([vector_ref[t].astype(jnp.float32) for t in range(STATES)], 1)
    found = [lanes_of(base * base), lanes_of(base * image), lanes_of(image * image)]
    lane = lax.broadcasted_iota(jnp.int32, (1, 128), 1)
    row = jnp.zeros((1, 128), jnp.float32)
    for k in range(3):
        row = jnp.where(lane == k, jnp.sum(found[k], keepdims=True), row)
    for r in range(sums_ref.shape[0]):
        sums_ref[r] = row


def sums_of(pieces, vector, size):
    return pl.pallas_call(
        sums_kernel,
        out_shape=(
            jax.ShapeDtypeStruct(pieces.shape[1:], jnp.float32),
            jax.ShapeDtypeStruct((size, 1, 128), jnp.float32),
        ),
        in_specs=[VMEM, VMEM],
        out_specs=(VMEM, VMEM),
        compiler_params=SMALL,
    )(pieces, vector)


def again_kernel(pieces_ref, out_ref):
    total = pieces_ref[0]
    for k in range(1, pieces_ref.shape[0]):
        total = total + pieces_ref[k]
    for r in range(out_ref.shape[0]):
        out_ref[r] = total


def again(pieces, size):
    return pl.pallas_call(
        again_kernel,
        out_shape=jax.ShapeDtypeStruct((size, *pieces.shape[1:]), jnp.float32),
        in_specs=[VMEM],
        out_specs=VMEM,
        compiler_params=SMALL,
    )(pieces)


def last_kernel(entries, pieces_ref, image_ref, vector_ref, next_ref, coefficients_ref):
    total = pieces_ref[0]
    for k in range(1, pieces_ref.shape[0]):
        total = total + pieces_ref[k]
    total = total / entries
    lane = lax.broadcasted_iota(jnp.int32, total.shape, 1)
    base_square, correlation, image_square = (
        jnp.sum(jnp.where(lane == k, total, 0.0), 1, keepdims=True) for k in range(3)
    )
    alpha = correlation / (base_square + epsilon)
    rho = jnp.sqrt(image_square - 2.0 * alpha * correlation + alpha * alpha * base_square + epsilon)
    width = next_ref.shape[2]
    for t in range(STATES):
        residual = image_ref[:, t * width : (t + 1) * width] - alpha * vector_ref[t].astype(jnp.float32)
        next_ref[t] = (residual / rho).astype(jnp.bfloat16)
    coefficients_ref[0] = alpha[0, 0]
    coefficients_ref[1] = rho[0, 0]


def last(entries, pieces, image, vector):
    def step(*refs):
        last_kernel(entries, *refs)

    return pl.pallas_call(
        step,
        out_shape=(
            jax.ShapeDtypeStruct(vector.shape, jnp.bfloat16),
            jax.ShapeDtypeStruct((2,), jnp.float32),
        ),
        in_specs=[VMEM, VMEM, VMEM],
        out_specs=(VMEM, SMEM),
        compiler_params=SMALL,
    )(pieces, image, vector)


def all_to_all(x, axes):
    return lax.all_to_all(x, axes, 0, 0, tiled=True)


def other_core(x):
    return lax.ppermute(x, C, [(0, 1), (1, 0)])


def body(start_vector, left_env, right_env, left_tensor, right_tensor):
    n_row = lax.axis_size(ROW)
    n_far, n_near = lax.axis_size(FAR), lax.axis_size(NEAR)
    n_z = n_far * n_near
    _, rows, half = start_vector.shape
    entries = float(STATES * rows * half * n_row * n_z * lax.axis_size(C))
    core = lax.axis_index(C).astype(jnp.int32).reshape(1)
    sites = tuple(jnp.transpose(tensor, (0, 2, 3, 1)) for tensor in (left_tensor, right_tensor))
    vector = jnp.swapaxes(start_vector, 1, 2)
    left = jnp.transpose(left_env, (2, 0, 1)).reshape(half, CHANNELS * rows)
    left = (left.astype(jnp.float32) * SCALE).astype(jnp.float16)

    own = all_to_all(pack(vector.reshape(STATES * half, rows), right_env, n_row), ROW)
    left = lax.all_gather(left, COL, axis=0, tiled=True)
    own, left = lax.optimization_barrier((own, left))
    left = (left.astype(jnp.float32) * (1.0 / SCALE)).astype(jnp.bfloat16)
    order = [n_far * (z % n_near) + z // n_near for z in range(n_z)]
    other = other_core(own)
    mixed, right = own_part(sites, left, own)
    sent = terms(order, core, sites, left, mixed, right, other)

    pieces = lax.all_to_all(sent, COL, 0, 0, axis_index_groups=neighbours(n_far, n_near), tiled=True)
    pieces = all_to_all(near_sum(pieces.reshape(n_near, n_far, *pieces.shape[1:])), FAR)
    image, sums = sums_of(pieces, vector, lax.axis_size((X, Y, C)))
    sums = again(all_to_all(sums, (X, Y, C)), n_z)
    next_vector, coefficients = last(entries, all_to_all(sums, Z), image, vector)
    return jnp.swapaxes(next_vector, 1, 2), coefficients


def solution(mesh):
    finer = Mesh(mesh.devices.reshape(4, 4, 4, 4, 2), (X, Y, FAR, NEAR, C))
    in_specs = (P(None, ROW, COL), P(None, ROW, COL), P(None, COL, ROW), P(), P())
    out_specs = (P(None, ROW, COL), P())
    return jax.shard_map(body, mesh=finer, in_specs=in_specs, out_specs=out_specs, check_vma=False)
```

```python
import jax
import jax.numpy as jnp
from jax import lax
from jax.experimental import pallas as pl
from jax.experimental.pallas import tpu as pltpu
from jax.sharding import Mesh
from jax.sharding import PartitionSpec as P

X, Y, FAR, NEAR, C = "row_0", "row_1", "far", "near", "core"
ROW = (X, Y)
Z = (FAR, NEAR)
COL = (FAR, NEAR, C)
STATES = 4
CHANNELS = 5

epsilon = 1e-06
SCALE = 8192.0

VMEM = pl.BlockSpec(memory_space=pltpu.VMEM)
SMEM = pl.BlockSpec(memory_space=pltpu.SMEM)
HBM = pl.BlockSpec(memory_space=pltpu.HBM)
SMALL = pltpu.CompilerParams(vmem_limit_bytes=4 * 1024 * 1024)
LARGE = pltpu.CompilerParams(vmem_limit_bytes=24 * 1024 * 1024)


def in_hbm(x):
    return pltpu.with_memory_space_constraint(x, pltpu.HBM)


def pack_kernel(vector_hbm, right_hbm, out_hbm, vector_s, right_s, turned_s, in_sems, out_sems):
    half, _ = right_s.shape[1:]
    rows = vector_s.shape[0]
    loads = [
        pltpu.make_async_copy(vector_hbm, vector_s, in_sems.at[0]),
        pltpu.make_async_copy(right_hbm, right_s, in_sems.at[1]),
    ]
    for load in loads:
        load.start()
    places = range(out_hbm.shape[0])
    stores = [pltpu.make_async_copy(vector_s, out_hbm.at[r, pl.ds(0, rows)], out_sems.at[0, r]) for r in places]
    loads[0].wait()
    for store in stores:
        store.start()
    loads[1].wait()
    for v in range(right_s.shape[0]):
        turned = right_s[v].astype(jnp.float32).T
        turned = jnp.concatenate([turned[:half], turned[half:]], 1).astype(jnp.bfloat16)
        turned_s[v * half : (v + 1) * half, :] = turned
    more = [pltpu.make_async_copy(turned_s, out_hbm.at[r, pl.ds(rows, turned_s.shape[0])], out_sems.at[1, r]) for r in places]
    for store in more:
        store.start()
    for store in stores + more:
        store.wait()


def pack(vector, right, size):
    rows, width = vector.shape
    channels, half, _ = right.shape
    return pl.pallas_call(
        pack_kernel,
        out_shape=pltpu.HBM((size, rows + channels * half, width), jnp.bfloat16),
        in_specs=[HBM, HBM],
        out_specs=HBM,
        scratch_shapes=[
            pltpu.VMEM(vector.shape, jnp.bfloat16),
            pltpu.VMEM(right.shape, jnp.bfloat16),
            pltpu.VMEM((channels * half, width), jnp.bfloat16),
            pltpu.SemaphoreType.DMA((2,)),
            pltpu.SemaphoreType.DMA((2, size)),
        ],
        compiler_params=SMALL,
    )(in_hbm(vector), in_hbm(right))


def site_copies(left_site, right_site, left_t, right_t, sems):
    loads = (
        pltpu.make_async_copy(left_site, left_t, sems.at[0]),
        pltpu.make_async_copy(right_site, right_t, sems.at[1]),
    )
    for load in loads:
        load.start()
    return loads


def combined(terms):
    total = None
    for scale, x in terms:
        total = scale * x if total is None else total + scale * x
    return total


def vector_copies(source, vec_s, sems):
    rows = vec_s.shape[0]
    width = source.shape[2]
    loads = [
        pltpu.make_async_copy(source.at[r, pl.ds(0, rows)], vec_s.at[:, pl.ds(r * width, width)], sems.at[r])
        for r in range(source.shape[0])
    ]
    for load in loads:
        load.start()
    return loads


def contract_and_mix(site_loads, left_t, right_t, left_ref, vec_s, cross_s, half_s, store):
    half = vec_s.shape[0] // STATES
    width = 2 * half
    cross_s[...] = jnp.dot(vec_s[...], left_ref[...], preferred_element_type=jnp.float32)
    for load in site_loads:
        load.wait()
    for s1 in range(2):
        for u in range(CHANNELS):
            for t2 in range(2):
                half_s[u, t2] = combined(
                    (
                        left_t[w, s1, t1, u],
                        cross_s[(2 * t1 + t2) * half : (2 * t1 + t2 + 1) * half, w * width : (w + 1) * width],
                    )
                    for w in range(CHANNELS)
                    for t1 in range(2)
                )
        for v in range(CHANNELS):
            for s2 in range(2):
                total = combined((right_t[u, s2, t2, v], half_s[u, t2]) for u in range(CHANNELS) for t2 in range(2))
                store(v, 2 * s1 + s2, total.astype(jnp.bfloat16))


def own_kernel(
    left_site, right_site, left_ref, own_hbm, mixed_out, right_out,
    left_t, right_t, vec_s, cross_s, half_s, vec_sems, right_sems, site_sems,
):
    width = own_hbm.shape[2]
    half = width // 2
    loads = vector_copies(own_hbm, vec_s, vec_sems)
    site_loads = site_copies(left_site, right_site, left_t, right_t, site_sems)
    passed = [
        pltpu.make_async_copy(
            own_hbm.at[:, pl.ds((STATES + v) * half, half)], right_out.at[:, :, pl.ds(v * width, width)], right_sems.at[v]
        )
        for v in range(CHANNELS)
    ]
    for load in loads:
        load.wait()
    for copy in passed:
        copy.start()

    def store(v, s, x):
        mixed_out[v * half : (v + 1) * half, s * width : (s + 1) * width] = x

    contract_and_mix(site_loads, left_t, right_t, left_ref, vec_s, cross_s, half_s, store)
    for copy in passed:
        copy.wait()


def own_part(sites, left, own):
    blocks, _, width = own.shape
    half = width // 2
    return pl.pallas_call(
        own_kernel,
        out_shape=(
            jax.ShapeDtypeStruct((CHANNELS * half, STATES * width), jnp.bfloat16),
            jax.ShapeDtypeStruct((blocks, half, CHANNELS * width), jnp.bfloat16),
        ),
        in_specs=[HBM, HBM, VMEM, HBM],
        out_specs=(VMEM, VMEM),
        scratch_shapes=[
            *(pltpu.SMEM(site.shape, jnp.float32) for site in sites),
            pltpu.VMEM((STATES * half, blocks * width), jnp.bfloat16),
            pltpu.VMEM((STATES * half, CHANNELS * width), jnp.float32),
            pltpu.VMEM((CHANNELS, 2, half, width), jnp.float32),
            pltpu.SemaphoreType.DMA((blocks,)),
            pltpu.SemaphoreType.DMA((CHANNELS,)),
            pltpu.SemaphoreType.DMA((2,)),
        ],
        compiler_params=LARGE,
    )(*(in_hbm(site) for site in sites), left, in_hbm(own))


def terms_kernel(
    order, core_ref, left_site, right_site, left_ref, mixed_ref, right_own, other_hbm, out_ref,
    left_t, right_t, right_other, vec_s, cross_s, half_s, right_s, mixed_s, vec_sems, right_sem, site_sems,
):
    blocks, half, _ = out_ref.shape
    width = 2 * half
    core = core_ref[0]
    own_at = pl.multiple_of(core * half, half)
    other_at = pl.multiple_of((1 - core) * half, half)
    loads = vector_copies(other_hbm, vec_s, vec_sems)
    site_loads = site_copies(left_site, right_site, left_t, right_t, site_sems)
    right_load = pltpu.make_async_copy(other_hbm.at[:, pl.ds(STATES * half, CHANNELS * half)], right_other, right_sem)
    mine = lax.broadcasted_iota(jnp.int32, (half, width), 1) // half == core
    for v in range(CHANNELS):
        mixed_s[pl.ds(v * width + own_at, half), :] = mixed_ref[v * half : (v + 1) * half, :]
    for load in loads:
        load.wait()
    right_load.start()

    def store(v, s, x):
        mixed_s[pl.ds(v * width + other_at, half), s * width : (s + 1) * width] = x

    contract_and_mix(site_loads, left_t, right_t, left_ref, vec_s, cross_s, half_s, store)
    right_load.wait()
    for r in range(blocks):
        for v in range(CHANNELS):
            own = right_own[r, :, v * width : (v + 1) * width].astype(jnp.float32)
            other = right_other[r, v * half : (v + 1) * half, :].astype(jnp.float32)
            other = jnp.concatenate([other[:, half:], other[:, :half]], 1)
            right_s[r * half : (r + 1) * half, v * width : (v + 1) * width] = jnp.where(mine, own, other).astype(jnp.bfloat16)
    image = jnp.dot(right_s[...], mixed_s[...], preferred_element_type=jnp.float32)
    for r in range(blocks):
        out_ref[order[r]] = image[r * half : (r + 1) * half].astype(jnp.bfloat16)


def terms(order, core, sites, left, mixed, right, other):
    def step(*refs):
        terms_kernel(order, *refs)

    blocks, _, width = other.shape
    half = width // 2
    return pl.pallas_call(
        step,
        out_shape=jax.ShapeDtypeStruct((blocks, half, STATES * width), jnp.bfloat16),
        in_specs=[SMEM, HBM, HBM, VMEM, VMEM, VMEM, HBM],
        out_specs=VMEM,
        scratch_shapes=[
            *(pltpu.SMEM(site.shape, jnp.float32) for site in sites),
            pltpu.VMEM((blocks, CHANNELS * half, width), jnp.bfloat16),
            pltpu.VMEM((STATES * half, blocks * width), jnp.bfloat16),
            pltpu.VMEM((STATES * half, CHANNELS * width), jnp.float32),
            pltpu.VMEM((CHANNELS, 2, half, width), jnp.float32),
            pltpu.VMEM((blocks * half, CHANNELS * width), jnp.bfloat16),
            pltpu.VMEM((CHANNELS * width, STATES * width), jnp.bfloat16),
            pltpu.SemaphoreType.DMA((blocks,)),
            pltpu.SemaphoreType.DMA,
            pltpu.SemaphoreType.DMA((2,)),
        ],
        compiler_params=LARGE,
    )(core, *(in_hbm(site) for site in sites), left, mixed, right, in_hbm(other))


def near_kernel(pieces_ref, out_ref):
    for j in range(out_ref.shape[0]):
        total = pieces_ref[0, j].astype(jnp.float32)
        for k in range(1, pieces_ref.shape[0]):
            total = total + pieces_ref[k, j].astype(jnp.float32)
        out_ref[j] = total.astype(jnp.bfloat16)


def near_sum(pieces):
    return pl.pallas_call(
        near_kernel,
        out_shape=jax.ShapeDtypeStruct(pieces.shape[1:], jnp.bfloat16),
        in_specs=[VMEM],
        out_specs=VMEM,
        compiler_params=SMALL,
    )(pieces)


def neighbours(n_far, n_near):
    n_z = n_far * n_near
    groups = []
    for core in range(2):
        for j in range(n_far):
            first = j * n_near + core * (n_near // 2)
            chips = sorted(((first + i) % n_z for i in range(n_near)), key=lambda z: z % n_near)
            groups.append([2 * z + core for z in chips])
    return groups


def lanes_of(total):
    rows, cols = total.shape
    total = sum(total[:, k : k + 128] for k in range(0, cols, 128))
    return sum(total[k : k + 8] for k in range(0, rows, 8))


def sums_kernel(pieces_ref, vector_ref, image_ref, sums_ref):
    image = pieces_ref[0].astype(jnp.float32)
    for k in range(1, pieces_ref.shape[0]):
        image = image + pieces_ref[k].astype(jnp.float32)
    image_ref[...] = image
    base = jnp.concatenate([vector_ref[t].astype(jnp.float32) for t in range(STATES)], 1)
    found = [lanes_of(base * base), lanes_of(base * image), lanes_of(image * image)]
    lane = lax.broadcasted_iota(jnp.int32, (1, 128), 1)
    row = jnp.zeros((1, 128), jnp.float32)
    for k in range(3):
        row = jnp.where(lane == k, jnp.sum(found[k], keepdims=True), row)
    for r in range(sums_ref.shape[0]):
        sums_ref[r] = row


def sums_of(pieces, vector, size):
    return pl.pallas_call(
        sums_kernel,
        out_shape=(
            jax.ShapeDtypeStruct(pieces.shape[1:], jnp.float32),
            jax.ShapeDtypeStruct((size, 1, 128), jnp.float32),
        ),
        in_specs=[VMEM, VMEM],
        out_specs=(VMEM, VMEM),
        compiler_params=SMALL,
    )(pieces, vector)


def again_kernel(pieces_ref, out_ref):
    total = pieces_ref[0]
    for k in range(1, pieces_ref.shape[0]):
        total = total + pieces_ref[k]
    for r in range(out_ref.shape[0]):
        out_ref[r] = total


def again(pieces, size):
    return pl.pallas_call(
        again_kernel,
        out_shape=jax.ShapeDtypeStruct((size, *pieces.shape[1:]), jnp.float32),
        in_specs=[VMEM],
        out_specs=VMEM,
        compiler_params=SMALL,
    )(pieces)


def last_kernel(entries, pieces_ref, image_ref, vector_ref, next_ref, coefficients_ref):
    total = pieces_ref[0]
    for k in range(1, pieces_ref.shape[0]):
        total = total + pieces_ref[k]
    total = total / entries
    lane = lax.broadcasted_iota(jnp.int32, total.shape, 1)
    base_square, correlation, image_square = (
        jnp.sum(jnp.where(lane == k, total, 0.0), 1, keepdims=True) for k in range(3)
    )
    alpha = correlation / (base_square + epsilon)
    rho = jnp.sqrt(image_square - 2.0 * alpha * correlation + alpha * alpha * base_square + epsilon)
    width = next_ref.shape[2]
    for t in range(STATES):
        residual = image_ref[:, t * width : (t + 1) * width] - alpha * vector_ref[t].astype(jnp.float32)
        next_ref[t] = (residual / rho).astype(jnp.bfloat16)
    coefficients_ref[0] = alpha[0, 0]
    coefficients_ref[1] = rho[0, 0]


def last(entries, pieces, image, vector):
    def step(*refs):
        last_kernel(entries, *refs)

    return pl.pallas_call(
        step,
        out_shape=(
            jax.ShapeDtypeStruct(vector.shape, jnp.bfloat16),
            jax.ShapeDtypeStruct((2,), jnp.float32),
        ),
        in_specs=[VMEM, VMEM, VMEM],
        out_specs=(VMEM, SMEM),
        compiler_params=SMALL,
    )(pieces, image, vector)


def all_to_all(x, axes):
    return lax.all_to_all(x, axes, 0, 0, tiled=True)


def other_core(x):
    return lax.ppermute(x, C, [(0, 1), (1, 0)])


def body(start_vector, left_env, right_env, left_tensor, right_tensor):
    n_row = lax.axis_size(ROW)
    n_far, n_near = lax.axis_size(FAR), lax.axis_size(NEAR)
    n_z = n_far * n_near
    _, rows, half = start_vector.shape
    entries = float(STATES * rows * half * n_row * n_z * lax.axis_size(C))
    core = lax.axis_index(C).astype(jnp.int32).reshape(1)
    sites = tuple(jnp.transpose(tensor, (0, 2, 3, 1)) for tensor in (left_tensor, right_tensor))
    vector = jnp.swapaxes(start_vector, 1, 2)
    left = jnp.transpose(left_env, (2, 0, 1)).reshape(half, CHANNELS * rows)
    left = (left.astype(jnp.float32) * SCALE).astype(jnp.float16)

    own = all_to_all(pack(vector.reshape(STATES * half, rows), right_env, n_row), ROW)
    left = lax.all_gather(left, COL, axis=0, tiled=True)
    own, left = lax.optimization_barrier((own, left))
    left = (left.astype(jnp.float32) * (1.0 / SCALE)).astype(jnp.bfloat16)
    order = [n_far * (z % n_near) + z // n_near for z in range(n_z)]
    other = other_core(own)
    mixed, right = own_part(sites, left, own)
    sent = terms(order, core, sites, left, mixed, right, other)

    pieces = lax.all_to_all(sent, COL, 0, 0, axis_index_groups=neighbours(n_far, n_near), tiled=True)
    pieces = all_to_all(near_sum(pieces.reshape(n_near, n_far, *pieces.shape[1:])), FAR)
    image, sums = sums_of(pieces, vector, lax.axis_size((X, Y, C)))
    sums = again(all_to_all(sums, (X, Y, C)), n_z)
    next_vector, coefficients = last(entries, all_to_all(sums, Z), image, vector)
    return jnp.swapaxes(next_vector, 1, 2), coefficients


def solution(mesh):
    finer = Mesh(mesh.devices.reshape(4, 4, 4, 4, 2), (X, Y, FAR, NEAR, C))
    in_specs = (P(None, ROW, COL), P(None, ROW, COL), P(None, COL, ROW), P(), P())
    out_specs = (P(None, ROW, COL), P())
    return jax.shard_map(body, mesh=finer, in_specs=in_specs, out_specs=out_specs, check_vma=False)
```

```python
import jax
import jax.numpy as jnp
from jax import lax
from jax.experimental import pallas as pl
from jax.experimental.pallas import tpu as pltpu
from jax.sharding import Mesh
from jax.sharding import PartitionSpec as P

X, Y, FAR, NEAR, C = "row_0", "row_1", "far", "near", "core"
ROW = (X, Y)
Z = (FAR, NEAR)
COL = (FAR, NEAR, C)
STATES = 4
CHANNELS = 5

epsilon = 1e-06
SCALE = 8192.0

VMEM = pl.BlockSpec(memory_space=pltpu.VMEM)
SMEM = pl.BlockSpec(memory_space=pltpu.SMEM)
HBM = pl.BlockSpec(memory_space=pltpu.HBM)
SMALL = pltpu.CompilerParams(vmem_limit_bytes=4 * 1024 * 1024)
LARGE = pltpu.CompilerParams(vmem_limit_bytes=24 * 1024 * 1024)


def in_hbm(x):
    return pltpu.with_memory_space_constraint(x, pltpu.HBM)


def pack_kernel(vector_hbm, right_hbm, out_hbm, vector_s, right_s, turned_s, in_sems, out_sems):
    half, _ = right_s.shape[1:]
    rows = vector_s.shape[0]
    loads = [
        pltpu.make_async_copy(vector_hbm, vector_s, in_sems.at[0]),
        pltpu.make_async_copy(right_hbm, right_s, in_sems.at[1]),
    ]
    for load in loads:
        load.start()
    places = range(out_hbm.shape[0])
    stores = [pltpu.make_async_copy(vector_s, out_hbm.at[r, pl.ds(0, rows)], out_sems.at[0, r]) for r in places]
    loads[0].wait()
    for store in stores:
        store.start()
    loads[1].wait()
    for v in range(right_s.shape[0]):
        turned = right_s[v].astype(jnp.float32).T
        turned = jnp.concatenate([turned[:half], turned[half:]], 1).astype(jnp.bfloat16)
        turned_s[v * half : (v + 1) * half, :] = turned
    more = [pltpu.make_async_copy(turned_s, out_hbm.at[r, pl.ds(rows, turned_s.shape[0])], out_sems.at[1, r]) for r in places]
    for store in more:
        store.start()
    for store in stores + more:
        store.wait()


def pack(vector, right, size):
    rows, width = vector.shape
    channels, half, _ = right.shape
    return pl.pallas_call(
        pack_kernel,
        out_shape=pltpu.HBM((size, rows + channels * half, width), jnp.bfloat16),
        in_specs=[HBM, HBM],
        out_specs=HBM,
        scratch_shapes=[
            pltpu.VMEM(vector.shape, jnp.bfloat16),
            pltpu.VMEM(right.shape, jnp.bfloat16),
            pltpu.VMEM((channels * half, width), jnp.bfloat16),
            pltpu.SemaphoreType.DMA((2,)),
            pltpu.SemaphoreType.DMA((2, size)),
        ],
        compiler_params=SMALL,
    )(in_hbm(vector), in_hbm(right))


def site_copies(left_site, right_site, left_t, right_t, sems):
    loads = (
        pltpu.make_async_copy(left_site, left_t, sems.at[0]),
        pltpu.make_async_copy(right_site, right_t, sems.at[1]),
    )
    for load in loads:
        load.start()
    return loads


def combined(terms):
    total = None
    for scale, x in terms:
        total = scale * x if total is None else total + scale * x
    return total


def contract_and_mix(site_loads, left_t, right_t, left_ref, piece_s, vec_s, cross_s, half_s, store):
    blocks, rows, width = piece_s.shape
    half = rows // STATES
    for r in range(blocks):
        vec_s[:, r * width : (r + 1) * width] = piece_s[r]
    cross_s[...] = jnp.dot(vec_s[...], left_ref[...], preferred_element_type=jnp.float32)
    for load in site_loads:
        load.wait()
    for s1 in range(2):
        for u in range(CHANNELS):
            for t2 in range(2):
                half_s[u, t2] = combined(
                    (
                        left_t[w, s1, t1, u],
                        cross_s[(2 * t1 + t2) * half : (2 * t1 + t2 + 1) * half, w * width : (w + 1) * width],
                    )
                    for w in range(CHANNELS)
                    for t1 in range(2)
                )
        for v in range(CHANNELS):
            for s2 in range(2):
                total = combined((right_t[u, s2, t2, v], half_s[u, t2]) for u in range(CHANNELS) for t2 in range(2))
                store(v, 2 * s1 + s2, total.astype(jnp.bfloat16))


def own_kernel(
    left_site, right_site, left_ref, own_hbm, mixed_out, right_out,
    left_t, right_t, piece_s, vec_s, cross_s, half_s, sems, site_sems,
):
    _, rows, width = piece_s.shape
    half = rows // STATES
    load = pltpu.make_async_copy(own_hbm.at[:, pl.ds(0, rows)], piece_s, sems.at[0])
    load.start()
    passed = pltpu.make_async_copy(own_hbm.at[:, pl.ds(rows, CHANNELS * half)], right_out, sems.at[1])
    passed.start()
    site_loads = site_copies(left_site, right_site, left_t, right_t, site_sems)
    load.wait()

    def store(v, s, x):
        mixed_out[v * half : (v + 1) * half, s * width : (s + 1) * width] = x

    contract_and_mix(site_loads, left_t, right_t, left_ref, piece_s, vec_s, cross_s, half_s, store)
    passed.wait()


def own_part(sites, left, own):
    blocks, _, width = own.shape
    half = width // 2
    return pl.pallas_call(
        own_kernel,
        out_shape=(
            jax.ShapeDtypeStruct((CHANNELS * half, STATES * width), jnp.bfloat16),
            jax.ShapeDtypeStruct((blocks, CHANNELS * half, width), jnp.bfloat16),
        ),
        in_specs=[HBM, HBM, VMEM, HBM],
        out_specs=(VMEM, VMEM),
        scratch_shapes=[
            *(pltpu.SMEM(site.shape, jnp.float32) for site in sites),
            pltpu.VMEM((blocks, STATES * half, width), jnp.bfloat16),
            pltpu.VMEM((STATES * half, blocks * width), jnp.bfloat16),
            pltpu.VMEM((STATES * half, CHANNELS * width), jnp.float32),
            pltpu.VMEM((CHANNELS, 2, half, width), jnp.float32),
            pltpu.SemaphoreType.DMA((2,)),
            pltpu.SemaphoreType.DMA((2,)),
        ],
        compiler_params=LARGE,
    )(*(in_hbm(site) for site in sites), left, in_hbm(own))


def terms_kernel(
    order, core_ref, left_site, right_site, left_ref, mixed_ref, right_own, other_hbm, out_ref,
    left_t, right_t, piece_s, right_other, vec_s, cross_s, half_s, right_s, mixed_s, sems, site_sems,
):
    blocks, half, _ = out_ref.shape
    width = 2 * half
    core = core_ref[0]
    own_at = pl.multiple_of(core * half, half)
    other_at = pl.multiple_of((1 - core) * half, half)
    load = pltpu.make_async_copy(other_hbm.at[:, pl.ds(0, STATES * half)], piece_s, sems.at[0])
    load.start()
    right_load = pltpu.make_async_copy(other_hbm.at[:, pl.ds(STATES * half, CHANNELS * half)], right_other, sems.at[1])
    right_load.start()
    site_loads = site_copies(left_site, right_site, left_t, right_t, site_sems)
    mine = lax.broadcasted_iota(jnp.int32, (half, width), 1) // half == core
    for v in range(CHANNELS):
        mixed_s[pl.ds(v * width + own_at, half), :] = mixed_ref[v * half : (v + 1) * half, :]
        for r in range(blocks):
            right_s[r * half : (r + 1) * half, v * width : (v + 1) * width] = right_own[r, v * half : (v + 1) * half, :]
    load.wait()

    def store(v, s, x):
        mixed_s[pl.ds(v * width + other_at, half), s * width : (s + 1) * width] = x

    contract_and_mix(site_loads, left_t, right_t, left_ref, piece_s, vec_s, cross_s, half_s, store)
    right_load.wait()
    for r in range(blocks):
        for v in range(CHANNELS):
            at = (slice(r * half, (r + 1) * half), slice(v * width, (v + 1) * width))
            other = right_other[r, v * half : (v + 1) * half, :].astype(jnp.float32)
            other = jnp.concatenate([other[:, half:], other[:, :half]], 1)
            right_s[at] = jnp.where(mine, right_s[at].astype(jnp.float32), other).astype(jnp.bfloat16)
    image = jnp.dot(right_s[...], mixed_s[...], preferred_element_type=jnp.float32)
    for r in range(blocks):
        out_ref[order[r]] = image[r * half : (r + 1) * half].astype(jnp.bfloat16)


def terms(order, core, sites, left, mixed, right, other):
    def step(*refs):
        terms_kernel(order, *refs)

    blocks, _, width = other.shape
    half = width // 2
    return pl.pallas_call(
        step,
        out_shape=jax.ShapeDtypeStruct((blocks, half, STATES * width), jnp.bfloat16),
        in_specs=[SMEM, HBM, HBM, VMEM, VMEM, VMEM, HBM],
        out_specs=VMEM,
        scratch_shapes=[
            *(pltpu.SMEM(site.shape, jnp.float32) for site in sites),
            pltpu.VMEM((blocks, STATES * half, width), jnp.bfloat16),
            pltpu.VMEM((blocks, CHANNELS * half, width), jnp.bfloat16),
            pltpu.VMEM((STATES * half, blocks * width), jnp.bfloat16),
            pltpu.VMEM((STATES * half, CHANNELS * width), jnp.float32),
            pltpu.VMEM((CHANNELS, 2, half, width), jnp.float32),
            pltpu.VMEM((blocks * half, CHANNELS * width), jnp.bfloat16),
            pltpu.VMEM((CHANNELS * width, STATES * width), jnp.bfloat16),
            pltpu.SemaphoreType.DMA((2,)),
            pltpu.SemaphoreType.DMA((2,)),
        ],
        compiler_params=LARGE,
    )(core, *(in_hbm(site) for site in sites), left, mixed, right, in_hbm(other))


def near_kernel(pieces_ref, out_ref):
    for j in range(out_ref.shape[0]):
        total = pieces_ref[0, j].astype(jnp.float32)
        for k in range(1, pieces_ref.shape[0]):
            total = total + pieces_ref[k, j].astype(jnp.float32)
        out_ref[j] = total.astype(jnp.bfloat16)


def near_sum(pieces):
    return pl.pallas_call(
        near_kernel,
        out_shape=jax.ShapeDtypeStruct(pieces.shape[1:], jnp.bfloat16),
        in_specs=[VMEM],
        out_specs=VMEM,
        compiler_params=SMALL,
    )(pieces)


def neighbours(n_far, n_near):
    n_z = n_far * n_near
    groups = []
    for core in range(2):
        for j in range(n_far):
            first = j * n_near + core * (n_near // 2)
            chips = sorted(((first + i) % n_z for i in range(n_near)), key=lambda z: z % n_near)
            groups.append([2 * z + core for z in chips])
    return groups


def lanes_of(total):
    rows, cols = total.shape
    total = sum(total[:, k : k + 128] for k in range(0, cols, 128))
    return sum(total[k : k + 8] for k in range(0, rows, 8))


def sums_kernel(pieces_ref, vector_ref, image_ref, sums_ref):
    image = pieces_ref[0].astype(jnp.float32)
    for k in range(1, pieces_ref.shape[0]):
        image = image + pieces_ref[k].astype(jnp.float32)
    image_ref[...] = image
    base = jnp.concatenate([vector_ref[t].astype(jnp.float32) for t in range(STATES)], 1)
    found = [lanes_of(base * base), lanes_of(base * image), lanes_of(image * image)]
    lane = lax.broadcasted_iota(jnp.int32, (1, 128), 1)
    row = jnp.zeros((1, 128), jnp.float32)
    for k in range(3):
        row = jnp.where(lane == k, jnp.sum(found[k], keepdims=True), row)
    for r in range(sums_ref.shape[0]):
        sums_ref[r] = row


def sums_of(pieces, vector, size):
    return pl.pallas_call(
        sums_kernel,
        out_shape=(
            jax.ShapeDtypeStruct(pieces.shape[1:], jnp.float32),
            jax.ShapeDtypeStruct((size, 1, 128), jnp.float32),
        ),
        in_specs=[VMEM, VMEM],
        out_specs=(VMEM, VMEM),
        compiler_params=SMALL,
    )(pieces, vector)


def again_kernel(pieces_ref, out_ref):
    total = pieces_ref[0]
    for k in range(1, pieces_ref.shape[0]):
        total = total + pieces_ref[k]
    for r in range(out_ref.shape[0]):
        out_ref[r] = total


def again(pieces, size):
    return pl.pallas_call(
        again_kernel,
        out_shape=jax.ShapeDtypeStruct((size, *pieces.shape[1:]), jnp.float32),
        in_specs=[VMEM],
        out_specs=VMEM,
        compiler_params=SMALL,
    )(pieces)


def last_kernel(entries, pieces_ref, image_ref, vector_ref, next_ref, coefficients_ref):
    total = pieces_ref[0]
    for k in range(1, pieces_ref.shape[0]):
        total = total + pieces_ref[k]
    total = total / entries
    lane = lax.broadcasted_iota(jnp.int32, total.shape, 1)
    base_square, correlation, image_square = (
        jnp.sum(jnp.where(lane == k, total, 0.0), 1, keepdims=True) for k in range(3)
    )
    alpha = correlation / (base_square + epsilon)
    rho = jnp.sqrt(image_square - 2.0 * alpha * correlation + alpha * alpha * base_square + epsilon)
    width = next_ref.shape[2]
    for t in range(STATES):
        residual = image_ref[:, t * width : (t + 1) * width] - alpha * vector_ref[t].astype(jnp.float32)
        next_ref[t] = (residual / rho).astype(jnp.bfloat16)
    coefficients_ref[0] = alpha[0, 0]
    coefficients_ref[1] = rho[0, 0]


def last(entries, pieces, image, vector):
    def step(*refs):
        last_kernel(entries, *refs)

    return pl.pallas_call(
        step,
        out_shape=(
            jax.ShapeDtypeStruct(vector.shape, jnp.bfloat16),
            jax.ShapeDtypeStruct((2,), jnp.float32),
        ),
        in_specs=[VMEM, VMEM, VMEM],
        out_specs=(VMEM, SMEM),
        compiler_params=SMALL,
    )(pieces, image, vector)


def all_to_all(x, axes):
    return lax.all_to_all(x, axes, 0, 0, tiled=True)


def other_core(x):
    return lax.ppermute(x, C, [(0, 1), (1, 0)])


def body(start_vector, left_env, right_env, left_tensor, right_tensor):
    n_row = lax.axis_size(ROW)
    n_far, n_near = lax.axis_size(FAR), lax.axis_size(NEAR)
    n_z = n_far * n_near
    _, rows, half = start_vector.shape
    entries = float(STATES * rows * half * n_row * n_z * lax.axis_size(C))
    core = lax.axis_index(C).astype(jnp.int32).reshape(1)
    sites = tuple(jnp.transpose(tensor, (0, 2, 3, 1)) for tensor in (left_tensor, right_tensor))
    vector = jnp.swapaxes(start_vector, 1, 2)
    left = jnp.transpose(left_env, (2, 0, 1)).reshape(half, CHANNELS * rows)
    left = (left.astype(jnp.float32) * SCALE).astype(jnp.float16)

    own = all_to_all(pack(vector.reshape(STATES * half, rows), right_env, n_row), ROW)
    left = lax.all_gather(left, COL, axis=0, tiled=True)
    own, left = lax.optimization_barrier((own, left))
    left = (left.astype(jnp.float32) * (1.0 / SCALE)).astype(jnp.bfloat16)
    order = [n_far * (z % n_near) + z // n_near for z in range(n_z)]
    other = other_core(own)
    mixed, right = own_part(sites, left, own)
    sent = terms(order, core, sites, left, mixed, right, other)

    pieces = lax.all_to_all(sent, COL, 0, 0, axis_index_groups=neighbours(n_far, n_near), tiled=True)
    pieces = all_to_all(near_sum(pieces.reshape(n_near, n_far, *pieces.shape[1:])), FAR)
    image, sums = sums_of(pieces, vector, lax.axis_size((X, Y, C)))
    sums = again(all_to_all(sums, (X, Y, C)), n_z)
    next_vector, coefficients = last(entries, all_to_all(sums, Z), image, vector)
    return jnp.swapaxes(next_vector, 1, 2), coefficients


def solution(mesh):
    finer = Mesh(mesh.devices.reshape(4, 4, 4, 4, 2), (X, Y, FAR, NEAR, C))
    in_specs = (P(None, ROW, COL), P(None, ROW, COL), P(None, COL, ROW), P(), P())
    out_specs = (P(None, ROW, COL), P())
    return jax.shard_map(body, mesh=finer, in_specs=in_specs, out_specs=out_specs, check_vma=False)
```

```python
import jax
import jax.numpy as jnp
from jax import lax
from jax.experimental import pallas as pl
from jax.experimental.pallas import tpu as pltpu
from jax.sharding import Mesh
from jax.sharding import PartitionSpec as P

X, Y, FAR, NEAR, C = "row_0", "row_1", "far", "near", "core"
ROW = (X, Y)
Z = (FAR, NEAR)
COL = (FAR, NEAR, C)
STATES = 4
CHANNELS = 5

epsilon = 1e-06
SCALE = 8192.0

VMEM = pl.BlockSpec(memory_space=pltpu.VMEM)
SMEM = pl.BlockSpec(memory_space=pltpu.SMEM)
HBM = pl.BlockSpec(memory_space=pltpu.HBM)
SMALL = pltpu.CompilerParams(vmem_limit_bytes=4 * 1024 * 1024)
LARGE = pltpu.CompilerParams(vmem_limit_bytes=24 * 1024 * 1024)


def in_hbm(x):
    return pltpu.with_memory_space_constraint(x, pltpu.HBM)


def pack_kernel(vector_hbm, right_hbm, out_hbm, vector_s, right_s, turned_s, in_sems, out_sems):
    half, _ = right_s.shape[1:]
    rows = vector_s.shape[0]
    loads = [
        pltpu.make_async_copy(vector_hbm, vector_s, in_sems.at[0]),
        pltpu.make_async_copy(right_hbm, right_s, in_sems.at[1]),
    ]
    for load in loads:
        load.start()
    places = range(out_hbm.shape[0])
    stores = [pltpu.make_async_copy(vector_s, out_hbm.at[r, pl.ds(0, rows)], out_sems.at[0, r]) for r in places]
    loads[0].wait()
    for store in stores:
        store.start()
    loads[1].wait()
    for v in range(right_s.shape[0]):
        turned = right_s[v].astype(jnp.float32).T
        turned = jnp.concatenate([turned[:half], turned[half:]], 1).astype(jnp.bfloat16)
        turned_s[v * half : (v + 1) * half, :] = turned
    more = [pltpu.make_async_copy(turned_s, out_hbm.at[r, pl.ds(rows, turned_s.shape[0])], out_sems.at[1, r]) for r in places]
    for store in more:
        store.start()
    for store in stores + more:
        store.wait()


def pack(vector, right, size):
    rows, width = vector.shape
    channels, half, _ = right.shape
    return pl.pallas_call(
        pack_kernel,
        out_shape=pltpu.HBM((size, rows + channels * half, width), jnp.bfloat16),
        in_specs=[HBM, HBM],
        out_specs=HBM,
        scratch_shapes=[
            pltpu.VMEM(vector.shape, jnp.bfloat16),
            pltpu.VMEM(right.shape, jnp.bfloat16),
            pltpu.VMEM((channels * half, width), jnp.bfloat16),
            pltpu.SemaphoreType.DMA((2,)),
            pltpu.SemaphoreType.DMA((2, size)),
        ],
        compiler_params=SMALL,
    )(in_hbm(vector), in_hbm(right))


def site_copies(left_site, right_site, left_t, right_t, sems):
    loads = (
        pltpu.make_async_copy(left_site, left_t, sems.at[0]),
        pltpu.make_async_copy(right_site, right_t, sems.at[1]),
    )
    for load in loads:
        load.start()
    return loads


def combined(terms):
    total = None
    for scale, x in terms:
        total = scale * x if total is None else total + scale * x
    return total


def contract_and_mix(site_loads, left_t, right_t, left_ref, piece_s, vec_s, cross_s, half_s, store):
    blocks, rows, width = piece_s.shape
    half = rows // STATES
    for r in range(blocks):
        vec_s[:, r * width : (r + 1) * width] = piece_s[r]
    cross_s[...] = jnp.dot(vec_s[...], left_ref[...], preferred_element_type=jnp.float32)
    for load in site_loads:
        load.wait()
    for s1 in range(2):
        for u in range(CHANNELS):
            for t2 in range(2):
                half_s[u, t2] = combined(
                    (
                        left_t[w, s1, t1, u],
                        cross_s[(2 * t1 + t2) * half : (2 * t1 + t2 + 1) * half, w * width : (w + 1) * width],
                    )
                    for w in range(CHANNELS)
                    for t1 in range(2)
                )
        for v in range(CHANNELS):
            for s2 in range(2):
                total = combined((right_t[u, s2, t2, v], half_s[u, t2]) for u in range(CHANNELS) for t2 in range(2))
                store(v, 2 * s1 + s2, total.astype(jnp.bfloat16))


def own_kernel(
    left_site, right_site, left_ref, own_hbm, mixed_out, right_out,
    left_t, right_t, piece_s, vec_s, cross_s, half_s, sems, site_sems,
):
    _, rows, width = piece_s.shape
    half = rows // STATES
    load = pltpu.make_async_copy(own_hbm.at[:, pl.ds(0, rows)], piece_s, sems.at[0])
    load.start()
    passed = pltpu.make_async_copy(own_hbm.at[:, pl.ds(rows, CHANNELS * half)], right_out, sems.at[1])
    passed.start()
    site_loads = site_copies(left_site, right_site, left_t, right_t, site_sems)
    load.wait()

    def store(v, s, x):
        mixed_out[v * half : (v + 1) * half, s * width : (s + 1) * width] = x

    contract_and_mix(site_loads, left_t, right_t, left_ref, piece_s, vec_s, cross_s, half_s, store)
    passed.wait()


def own_part(sites, left, own):
    blocks, _, width = own.shape
    half = width // 2
    return pl.pallas_call(
        own_kernel,
        out_shape=(
            jax.ShapeDtypeStruct((CHANNELS * half, STATES * width), jnp.bfloat16),
            jax.ShapeDtypeStruct((blocks, CHANNELS * half, width), jnp.bfloat16),
        ),
        in_specs=[HBM, HBM, VMEM, HBM],
        out_specs=(VMEM, VMEM),
        scratch_shapes=[
            *(pltpu.SMEM(site.shape, jnp.float32) for site in sites),
            pltpu.VMEM((blocks, STATES * half, width), jnp.bfloat16),
            pltpu.VMEM((STATES * half, blocks * width), jnp.bfloat16),
            pltpu.VMEM((STATES * half, CHANNELS * width), jnp.float32),
            pltpu.VMEM((CHANNELS, 2, half, width), jnp.float32),
            pltpu.SemaphoreType.DMA((2,)),
            pltpu.SemaphoreType.DMA((2,)),
        ],
        compiler_params=LARGE,
    )(*(in_hbm(site) for site in sites), left, in_hbm(own))


def terms_kernel(
    order, core_ref, left_site, right_site, left_ref, mixed_ref, right_own, other_hbm, out_ref,
    left_t, right_t, piece_s, right_other, vec_s, cross_s, half_s, right_s, mixed_s, sems, site_sems,
):
    blocks, half, _ = out_ref.shape
    width = 2 * half
    core = core_ref[0]
    own_at = pl.multiple_of(core * half, half)
    other_at = pl.multiple_of((1 - core) * half, half)
    load = pltpu.make_async_copy(other_hbm.at[:, pl.ds(0, STATES * half)], piece_s, sems.at[0])
    load.start()
    right_load = pltpu.make_async_copy(other_hbm.at[:, pl.ds(STATES * half, CHANNELS * half)], right_other, sems.at[1])
    right_load.start()
    site_loads = site_copies(left_site, right_site, left_t, right_t, site_sems)
    mine = lax.broadcasted_iota(jnp.int32, (half, width), 1) // half == core
    for v in range(CHANNELS):
        mixed_s[pl.ds(v * width + own_at, half), :] = mixed_ref[v * half : (v + 1) * half, :]
        for r in range(blocks):
            right_s[r * half : (r + 1) * half, v * width : (v + 1) * width] = right_own[r, v * half : (v + 1) * half, :]
    load.wait()

    def store(v, s, x):
        mixed_s[pl.ds(v * width + other_at, half), s * width : (s + 1) * width] = x

    contract_and_mix(site_loads, left_t, right_t, left_ref, piece_s, vec_s, cross_s, half_s, store)
    right_load.wait()
    for r in range(blocks):
        for v in range(CHANNELS):
            at = (slice(r * half, (r + 1) * half), slice(v * width, (v + 1) * width))
            other = right_other[r, v * half : (v + 1) * half, :].astype(jnp.float32)
            other = jnp.concatenate([other[:, half:], other[:, :half]], 1)
            right_s[at] = jnp.where(mine, right_s[at].astype(jnp.float32), other).astype(jnp.bfloat16)
    image = jnp.dot(right_s[...], mixed_s[...], preferred_element_type=jnp.float32)
    for r in range(blocks):
        out_ref[order[r]] = image[r * half : (r + 1) * half].astype(jnp.bfloat16)


def terms(order, core, sites, left, mixed, right, other):
    def step(*refs):
        terms_kernel(order, *refs)

    blocks, _, width = other.shape
    half = width // 2
    return pl.pallas_call(
        step,
        out_shape=jax.ShapeDtypeStruct((blocks, half, STATES * width), jnp.bfloat16),
        in_specs=[SMEM, HBM, HBM, VMEM, VMEM, VMEM, HBM],
        out_specs=VMEM,
        scratch_shapes=[
            *(pltpu.SMEM(site.shape, jnp.float32) for site in sites),
            pltpu.VMEM((blocks, STATES * half, width), jnp.bfloat16),
            pltpu.VMEM((blocks, CHANNELS * half, width), jnp.bfloat16),
            pltpu.VMEM((STATES * half, blocks * width), jnp.bfloat16),
            pltpu.VMEM((STATES * half, CHANNELS * width), jnp.float32),
            pltpu.VMEM((CHANNELS, 2, half, width), jnp.float32),
            pltpu.VMEM((blocks * half, CHANNELS * width), jnp.bfloat16),
            pltpu.VMEM((CHANNELS * width, STATES * width), jnp.bfloat16),
            pltpu.SemaphoreType.DMA((2,)),
            pltpu.SemaphoreType.DMA((2,)),
        ],
        compiler_params=LARGE,
    )(core, *(in_hbm(site) for site in sites), left, mixed, right, in_hbm(other))


def near_kernel(pieces_ref, out_ref):
    for j in range(out_ref.shape[0]):
        total = pieces_ref[0, j].astype(jnp.float32)
        for k in range(1, pieces_ref.shape[0]):
            total = total + pieces_ref[k, j].astype(jnp.float32)
        out_ref[j] = total.astype(jnp.bfloat16)


def near_sum(pieces):
    return pl.pallas_call(
        near_kernel,
        out_shape=jax.ShapeDtypeStruct(pieces.shape[1:], jnp.bfloat16),
        in_specs=[VMEM],
        out_specs=VMEM,
        compiler_params=SMALL,
    )(pieces)


def neighbours(n_far, n_near):
    n_z = n_far * n_near
    groups = []
    for core in range(2):
        for j in range(n_far):
            first = j * n_near + (1 - core) * (n_near // 2)
            chips = sorted(((first + i) % n_z for i in range(n_near)), key=lambda z: z % n_near)
            groups.append([2 * z + core for z in chips])
    return groups


def lanes_of(total):
    rows, cols = total.shape
    total = sum(total[:, k : k + 128] for k in range(0, cols, 128))
    return sum(total[k : k + 8] for k in range(0, rows, 8))


def sums_kernel(pieces_ref, vector_ref, image_ref, sums_ref):
    image = pieces_ref[0].astype(jnp.float32)
    for k in range(1, pieces_ref.shape[0]):
        image = image + pieces_ref[k].astype(jnp.float32)
    image_ref[...] = image
    base = jnp.concatenate([vector_ref[t].astype(jnp.float32) for t in range(STATES)], 1)
    found = [lanes_of(base * base), lanes_of(base * image), lanes_of(image * image)]
    lane = lax.broadcasted_iota(jnp.int32, (1, 128), 1)
    row = jnp.zeros((1, 128), jnp.float32)
    for k in range(3):
        row = jnp.where(lane == k, jnp.sum(found[k], keepdims=True), row)
    for r in range(sums_ref.shape[0]):
        sums_ref[r] = row


def sums_of(pieces, vector, size):
    return pl.pallas_call(
        sums_kernel,
        out_shape=(
            jax.ShapeDtypeStruct(pieces.shape[1:], jnp.float32),
            jax.ShapeDtypeStruct((size, 1, 128), jnp.float32),
        ),
        in_specs=[VMEM, VMEM],
        out_specs=(VMEM, VMEM),
        compiler_params=SMALL,
    )(pieces, vector)


def again_kernel(pieces_ref, out_ref):
    total = pieces_ref[0]
    for k in range(1, pieces_ref.shape[0]):
        total = total + pieces_ref[k]
    for r in range(out_ref.shape[0]):
        out_ref[r] = total


def again(pieces, size):
    return pl.pallas_call(
        again_kernel,
        out_shape=jax.ShapeDtypeStruct((size, *pieces.shape[1:]), jnp.float32),
        in_specs=[VMEM],
        out_specs=VMEM,
        compiler_params=SMALL,
    )(pieces)


def last_kernel(entries, pieces_ref, image_ref, vector_ref, next_ref, coefficients_ref):
    total = pieces_ref[0]
    for k in range(1, pieces_ref.shape[0]):
        total = total + pieces_ref[k]
    total = total / entries
    lane = lax.broadcasted_iota(jnp.int32, total.shape, 1)
    base_square, correlation, image_square = (
        jnp.sum(jnp.where(lane == k, total, 0.0), 1, keepdims=True) for k in range(3)
    )
    alpha = correlation / (base_square + epsilon)
    rho = jnp.sqrt(image_square - 2.0 * alpha * correlation + alpha * alpha * base_square + epsilon)
    width = next_ref.shape[2]
    for t in range(STATES):
        residual = image_ref[:, t * width : (t + 1) * width] - alpha * vector_ref[t].astype(jnp.float32)
        next_ref[t] = (residual / rho).astype(jnp.bfloat16)
    coefficients_ref[0] = alpha[0, 0]
    coefficients_ref[1] = rho[0, 0]


def last(entries, pieces, image, vector):
    def step(*refs):
        last_kernel(entries, *refs)

    return pl.pallas_call(
        step,
        out_shape=(
            jax.ShapeDtypeStruct(vector.shape, jnp.bfloat16),
            jax.ShapeDtypeStruct((2,), jnp.float32),
        ),
        in_specs=[VMEM, VMEM, VMEM],
        out_specs=(VMEM, SMEM),
        compiler_params=SMALL,
    )(pieces, image, vector)


def all_to_all(x, axes):
    return lax.all_to_all(x, axes, 0, 0, tiled=True)


def other_core(x):
    return lax.ppermute(x, C, [(0, 1), (1, 0)])


def body(start_vector, left_env, right_env, left_tensor, right_tensor):
    n_row = lax.axis_size(ROW)
    n_far, n_near = lax.axis_size(FAR), lax.axis_size(NEAR)
    n_z = n_far * n_near
    _, rows, half = start_vector.shape
    entries = float(STATES * rows * half * n_row * n_z * lax.axis_size(C))
    core = lax.axis_index(C).astype(jnp.int32).reshape(1)
    sites = tuple(jnp.transpose(tensor, (0, 2, 3, 1)) for tensor in (left_tensor, right_tensor))
    vector = jnp.swapaxes(start_vector, 1, 2)
    left = jnp.transpose(left_env, (2, 0, 1)).reshape(half, CHANNELS * rows)
    left = (left.astype(jnp.float32) * SCALE).astype(jnp.float16)

    own = all_to_all(pack(vector.reshape(STATES * half, rows), right_env, n_row), ROW)
    left = lax.all_gather(left, COL, axis=0, tiled=True)
    own, left = lax.optimization_barrier((own, left))
    left = (left.astype(jnp.float32) * (1.0 / SCALE)).astype(jnp.bfloat16)
    order = [n_far * (z % n_near) + z // n_near for z in range(n_z)]
    other = other_core(own)
    mixed, right = own_part(sites, left, own)
    sent = terms(order, core, sites, left, mixed, right, other)

    pieces = lax.all_to_all(sent, COL, 0, 0, axis_index_groups=neighbours(n_far, n_near), tiled=True)
    pieces = all_to_all(near_sum(pieces.reshape(n_near, n_far, *pieces.shape[1:])), FAR)
    image, sums = sums_of(pieces, vector, lax.axis_size((X, Y, C)))
    sums = again(all_to_all(sums, (X, Y, C)), n_z)
    next_vector, coefficients = last(entries, all_to_all(sums, Z), image, vector)
    return jnp.swapaxes(next_vector, 1, 2), coefficients


def solution(mesh):
    finer = Mesh(mesh.devices.reshape(4, 4, 4, 4, 2), (X, Y, FAR, NEAR, C))
    in_specs = (P(None, ROW, COL), P(None, ROW, COL), P(None, COL, ROW), P(), P())
    out_specs = (P(None, ROW, COL), P())
    return jax.shard_map(body, mesh=finer, in_specs=in_specs, out_specs=out_specs, check_vma=False)
```

```python
import jax
import jax.numpy as jnp
from jax import lax
from jax.experimental import pallas as pl
from jax.experimental.pallas import tpu as pltpu
from jax.sharding import Mesh
from jax.sharding import PartitionSpec as P

X, Y, FAR, NEAR, C = "row_0", "row_1", "far", "near", "core"
ROW = (X, Y)
Z = (FAR, NEAR)
COL = (FAR, NEAR, C)
STATES = 4
CHANNELS = 5

epsilon = 1e-06
SCALE = 8192.0

VMEM = pl.BlockSpec(memory_space=pltpu.VMEM)
SMEM = pl.BlockSpec(memory_space=pltpu.SMEM)
HBM = pl.BlockSpec(memory_space=pltpu.HBM)
SMALL = pltpu.CompilerParams(vmem_limit_bytes=4 * 1024 * 1024)
LARGE = pltpu.CompilerParams(vmem_limit_bytes=24 * 1024 * 1024)


def in_hbm(x):
    return pltpu.with_memory_space_constraint(x, pltpu.HBM)


def pack_kernel(vector_hbm, right_hbm, out_hbm, vector_s, right_s, turned_s, in_sems, out_sems):
    half, _ = right_s.shape[1:]
    rows = vector_s.shape[0]
    loads = [
        pltpu.make_async_copy(vector_hbm, vector_s, in_sems.at[0]),
        pltpu.make_async_copy(right_hbm, right_s, in_sems.at[1]),
    ]
    for load in loads:
        load.start()
    places = range(out_hbm.shape[0])
    stores = [pltpu.make_async_copy(vector_s, out_hbm.at[r, pl.ds(0, rows)], out_sems.at[0, r]) for r in places]
    loads[0].wait()
    for store in stores:
        store.start()
    loads[1].wait()
    for v in range(right_s.shape[0]):
        turned = right_s[v].astype(jnp.float32).T
        turned = jnp.concatenate([turned[:half], turned[half:]], 1).astype(jnp.bfloat16)
        turned_s[v * half : (v + 1) * half, :] = turned
    more = [pltpu.make_async_copy(turned_s, out_hbm.at[r, pl.ds(rows, turned_s.shape[0])], out_sems.at[1, r]) for r in places]
    for store in more:
        store.start()
    for store in stores + more:
        store.wait()


def pack(vector, right, size):
    rows, width = vector.shape
    channels, half, _ = right.shape
    return pl.pallas_call(
        pack_kernel,
        out_shape=pltpu.HBM((size, rows + channels * half, width), jnp.bfloat16),
        in_specs=[HBM, HBM],
        out_specs=HBM,
        scratch_shapes=[
            pltpu.VMEM(vector.shape, jnp.bfloat16),
            pltpu.VMEM(right.shape, jnp.bfloat16),
            pltpu.VMEM((channels * half, width), jnp.bfloat16),
            pltpu.SemaphoreType.DMA((2,)),
            pltpu.SemaphoreType.DMA((2, size)),
        ],
        compiler_params=SMALL,
    )(in_hbm(vector), in_hbm(right))


def site_copies(left_site, right_site, left_t, right_t, sems):
    loads = (
        pltpu.make_async_copy(left_site, left_t, sems.at[0]),
        pltpu.make_async_copy(right_site, right_t, sems.at[1]),
    )
    for load in loads:
        load.start()
    return loads


def combined(terms):
    total = None
    for scale, x in terms:
        total = scale * x if total is None else total + scale * x
    return total


def contract_and_mix(site_loads, left_t, right_t, left_ref, piece_s, vec_s, cross_s, half_s, store):
    blocks, _, width = piece_s.shape
    half = width // 2
    for r in range(blocks):
        vec_s[:, r * width : (r + 1) * width] = piece_s[r, : STATES * half, :]
    cross_s[...] = jnp.dot(vec_s[...], left_ref[...], preferred_element_type=jnp.float32)
    for load in site_loads:
        load.wait()
    for s1 in range(2):
        for u in range(CHANNELS):
            for t2 in range(2):
                half_s[u, t2] = combined(
                    (
                        left_t[w, s1, t1, u],
                        cross_s[(2 * t1 + t2) * half : (2 * t1 + t2 + 1) * half, w * width : (w + 1) * width],
                    )
                    for w in range(CHANNELS)
                    for t1 in range(2)
                )
        for v in range(CHANNELS):
            for s2 in range(2):
                total = combined((right_t[u, s2, t2, v], half_s[u, t2]) for u in range(CHANNELS) for t2 in range(2))
                store(v, 2 * s1 + s2, total.astype(jnp.bfloat16))


def own_kernel(
    left_site, right_site, left_ref, own_hbm, mixed_out, right_out,
    left_t, right_t, piece_s, vec_s, cross_s, half_s, sems, site_sems,
):
    _, rows, width = piece_s.shape
    half = rows // STATES
    load = pltpu.make_async_copy(own_hbm.at[:, pl.ds(0, rows)], piece_s, sems.at[0])
    load.start()
    passed = pltpu.make_async_copy(own_hbm.at[:, pl.ds(rows, CHANNELS * half)], right_out, sems.at[1])
    passed.start()
    site_loads = site_copies(left_site, right_site, left_t, right_t, site_sems)
    load.wait()

    def store(v, s, x):
        mixed_out[v * half : (v + 1) * half, s * width : (s + 1) * width] = x

    contract_and_mix(site_loads, left_t, right_t, left_ref, piece_s, vec_s, cross_s, half_s, store)
    passed.wait()


def own_part(sites, left, own):
    blocks, _, width = own.shape
    half = width // 2
    return pl.pallas_call(
        own_kernel,
        out_shape=(
            jax.ShapeDtypeStruct((CHANNELS * half, STATES * width), jnp.bfloat16),
            jax.ShapeDtypeStruct((blocks, CHANNELS * half, width), jnp.bfloat16),
        ),
        in_specs=[HBM, HBM, VMEM, HBM],
        out_specs=(VMEM, VMEM),
        scratch_shapes=[
            *(pltpu.SMEM(site.shape, jnp.float32) for site in sites),
            pltpu.VMEM((blocks, STATES * half, width), jnp.bfloat16),
            pltpu.VMEM((STATES * half, blocks * width), jnp.bfloat16),
            pltpu.VMEM((STATES * half, CHANNELS * width), jnp.float32),
            pltpu.VMEM((CHANNELS, 2, half, width), jnp.float32),
            pltpu.SemaphoreType.DMA((2,)),
            pltpu.SemaphoreType.DMA((2,)),
        ],
        compiler_params=LARGE,
    )(*(in_hbm(site) for site in sites), left, in_hbm(own))


def terms_kernel(
    order, left_site, right_site, left_ref, mixed_ref, right_own, other_ref, out_ref,
    left_t, right_t, vec_s, cross_s, half_s, right_s, mixed_s, site_sems,
):
    blocks, half, _ = out_ref.shape
    width = 2 * half
    core = lax.axis_index(C)
    own_at = pl.multiple_of(core * half, half)
    other_at = pl.multiple_of((1 - core) * half, half)
    site_loads = site_copies(left_site, right_site, left_t, right_t, site_sems)
    mine = lax.broadcasted_iota(jnp.int32, (half, width), 1) // half == core
    for v in range(CHANNELS):
        mixed_s[pl.ds(v * width + own_at, half), :] = mixed_ref[v * half : (v + 1) * half, :]
        for r in range(blocks):
            right_s[r * half : (r + 1) * half, v * width : (v + 1) * width] = right_own[r, v * half : (v + 1) * half, :]

    def store(v, s, x):
        mixed_s[pl.ds(v * width + other_at, half), s * width : (s + 1) * width] = x

    contract_and_mix(site_loads, left_t, right_t, left_ref, other_ref, vec_s, cross_s, half_s, store)
    for r in range(blocks):
        for v in range(CHANNELS):
            at = (slice(r * half, (r + 1) * half), slice(v * width, (v + 1) * width))
            other = other_ref[r, (STATES + v) * half : (STATES + v + 1) * half, :].astype(jnp.float32)
            other = jnp.concatenate([other[:, half:], other[:, :half]], 1)
            right_s[at] = jnp.where(mine, right_s[at].astype(jnp.float32), other).astype(jnp.bfloat16)
    image = jnp.dot(right_s[...], mixed_s[...], preferred_element_type=jnp.float32)
    for r in range(blocks):
        out_ref[order[r]] = image[r * half : (r + 1) * half].astype(jnp.bfloat16)


def terms(order, sites, left, mixed, right, other):
    def step(*refs):
        terms_kernel(order, *refs)

    blocks, _, width = other.shape
    half = width // 2
    return pl.pallas_call(
        step,
        out_shape=jax.ShapeDtypeStruct((blocks, half, STATES * width), jnp.bfloat16),
        in_specs=[HBM, HBM, VMEM, VMEM, VMEM, VMEM],
        out_specs=VMEM,
        scratch_shapes=[
            *(pltpu.SMEM(site.shape, jnp.float32) for site in sites),
            pltpu.VMEM((STATES * half, blocks * width), jnp.bfloat16),
            pltpu.VMEM((STATES * half, CHANNELS * width), jnp.float32),
            pltpu.VMEM((CHANNELS, 2, half, width), jnp.float32),
            pltpu.VMEM((blocks * half, CHANNELS * width), jnp.bfloat16),
            pltpu.VMEM((CHANNELS * width, STATES * width), jnp.bfloat16),
            pltpu.SemaphoreType.DMA((2,)),
        ],
        compiler_params=LARGE,
    )(*(in_hbm(site) for site in sites), left, mixed, right, other)


def near_kernel(pieces_ref, out_ref):
    for j in range(out_ref.shape[0]):
        total = pieces_ref[0, j].astype(jnp.float32)
        for k in range(1, pieces_ref.shape[0]):
            total = total + pieces_ref[k, j].astype(jnp.float32)
        out_ref[j] = total.astype(jnp.bfloat16)


def near_sum(pieces):
    return pl.pallas_call(
        near_kernel,
        out_shape=jax.ShapeDtypeStruct(pieces.shape[1:], jnp.bfloat16),
        in_specs=[VMEM],
        out_specs=VMEM,
        compiler_params=SMALL,
    )(pieces)


def neighbours(n_far, n_near):
    n_z = n_far * n_near
    groups = []
    for core in range(2):
        for j in range(n_far):
            first = j * n_near + (1 - core) * (n_near // 2)
            chips = sorted(((first + i) % n_z for i in range(n_near)), key=lambda z: z % n_near)
            groups.append([2 * z + core for z in chips])
    return groups


def lanes_of(total):
    rows, cols = total.shape
    total = sum(total[:, k : k + 128] for k in range(0, cols, 128))
    return sum(total[k : k + 8] for k in range(0, rows, 8))


def sums_kernel(pieces_ref, vector_ref, image_ref, sums_ref):
    image = pieces_ref[0].astype(jnp.float32)
    for k in range(1, pieces_ref.shape[0]):
        image = image + pieces_ref[k].astype(jnp.float32)
    image_ref[...] = image
    base = jnp.concatenate([vector_ref[t].astype(jnp.float32) for t in range(STATES)], 1)
    found = [lanes_of(base * base), lanes_of(base * image), lanes_of(image * image)]
    lane = lax.broadcasted_iota(jnp.int32, (1, 128), 1)
    row = jnp.zeros((1, 128), jnp.float32)
    for k in range(3):
        row = jnp.where(lane == k, jnp.sum(found[k], keepdims=True), row)
    for r in range(sums_ref.shape[0]):
        sums_ref[r] = row


def sums_of(pieces, vector, size):
    return pl.pallas_call(
        sums_kernel,
        out_shape=(
            jax.ShapeDtypeStruct(pieces.shape[1:], jnp.float32),
            jax.ShapeDtypeStruct((size, 1, 128), jnp.float32),
        ),
        in_specs=[VMEM, VMEM],
        out_specs=(VMEM, VMEM),
        compiler_params=SMALL,
    )(pieces, vector)


def again_kernel(pieces_ref, out_ref):
    total = pieces_ref[0]
    for k in range(1, pieces_ref.shape[0]):
        total = total + pieces_ref[k]
    for r in range(out_ref.shape[0]):
        out_ref[r] = total


def again(pieces, size):
    return pl.pallas_call(
        again_kernel,
        out_shape=jax.ShapeDtypeStruct((size, *pieces.shape[1:]), jnp.float32),
        in_specs=[VMEM],
        out_specs=VMEM,
        compiler_params=SMALL,
    )(pieces)


def last_kernel(entries, pieces_ref, image_ref, vector_ref, next_ref, coefficients_ref):
    total = pieces_ref[0]
    for k in range(1, pieces_ref.shape[0]):
        total = total + pieces_ref[k]
    total = total / entries
    lane = lax.broadcasted_iota(jnp.int32, total.shape, 1)
    base_square, correlation, image_square = (
        jnp.sum(jnp.where(lane == k, total, 0.0), 1, keepdims=True) for k in range(3)
    )
    alpha = correlation / (base_square + epsilon)
    rho = jnp.sqrt(image_square - 2.0 * alpha * correlation + alpha * alpha * base_square + epsilon)
    width = next_ref.shape[2]
    for t in range(STATES):
        residual = image_ref[:, t * width : (t + 1) * width] - alpha * vector_ref[t].astype(jnp.float32)
        next_ref[t] = (residual / rho).astype(jnp.bfloat16)
    coefficients_ref[0] = alpha[0, 0]
    coefficients_ref[1] = rho[0, 0]


def last(entries, pieces, image, vector):
    def step(*refs):
        last_kernel(entries, *refs)

    return pl.pallas_call(
        step,
        out_shape=(
            jax.ShapeDtypeStruct(vector.shape, jnp.bfloat16),
            jax.ShapeDtypeStruct((2,), jnp.float32),
        ),
        in_specs=[VMEM, VMEM, VMEM],
        out_specs=(VMEM, SMEM),
        compiler_params=SMALL,
    )(pieces, image, vector)


def all_to_all(x, axes):
    return lax.all_to_all(x, axes, 0, 0, tiled=True)


def other_core(x):
    return lax.ppermute(x, C, [(0, 1), (1, 0)])


def body(start_vector, left_env, right_env, left_tensor, right_tensor):
    n_row = lax.axis_size(ROW)
    n_far, n_near = lax.axis_size(FAR), lax.axis_size(NEAR)
    n_z = n_far * n_near
    _, rows, half = start_vector.shape
    entries = float(STATES * rows * half * n_row * n_z * lax.axis_size(C))
    sites = tuple(jnp.transpose(tensor, (0, 2, 3, 1)) for tensor in (left_tensor, right_tensor))
    vector = jnp.swapaxes(start_vector, 1, 2)
    left = jnp.transpose(left_env, (2, 0, 1)).reshape(half, CHANNELS * rows)
    left = (left.astype(jnp.float32) * SCALE).astype(jnp.float16)

    own = all_to_all(pack(vector.reshape(STATES * half, rows), right_env, n_row), ROW)
    left = lax.all_gather(left, COL, axis=0, tiled=True)
    own, left = lax.optimization_barrier((own, left))
    left = (left.astype(jnp.float32) * (1.0 / SCALE)).astype(jnp.bfloat16)
    order = [n_far * (z % n_near) + z // n_near for z in range(n_z)]
    other = other_core(own)
    mixed, right = own_part(sites, left, own)
    sent = terms(order, sites, left, mixed, right, other)

    pieces = lax.all_to_all(sent, COL, 0, 0, axis_index_groups=neighbours(n_far, n_near), tiled=True)
    pieces = all_to_all(near_sum(pieces.reshape(n_near, n_far, *pieces.shape[1:])), FAR)
    image, sums = sums_of(pieces, vector, lax.axis_size((X, Y, C)))
    sums = again(all_to_all(sums, (X, Y, C)), n_z)
    next_vector, coefficients = last(entries, all_to_all(sums, Z), image, vector)
    return jnp.swapaxes(next_vector, 1, 2), coefficients


def solution(mesh):
    finer = Mesh(mesh.devices.reshape(4, 4, 4, 4, 2), (X, Y, FAR, NEAR, C))
    in_specs = (P(None, ROW, COL), P(None, ROW, COL), P(None, COL, ROW), P(), P())
    out_specs = (P(None, ROW, COL), P())
    return jax.shard_map(body, mesh=finer, in_specs=in_specs, out_specs=out_specs, check_vma=False)
```

```python
import jax
import jax.numpy as jnp
from jax import lax
from jax.experimental import pallas as pl
from jax.experimental.pallas import tpu as pltpu
from jax.sharding import Mesh
from jax.sharding import PartitionSpec as P

X, Y, FAR, NEAR, C = "row_0", "row_1", "far", "near", "core"
ROW = (X, Y)
Z = (FAR, NEAR)
COL = (FAR, NEAR, C)
STATES = 4
CHANNELS = 5

epsilon = 1e-06
SCALE = 8192.0

VMEM = pl.BlockSpec(memory_space=pltpu.VMEM)
SMEM = pl.BlockSpec(memory_space=pltpu.SMEM)
HBM = pl.BlockSpec(memory_space=pltpu.HBM)
SMALL = pltpu.CompilerParams(vmem_limit_bytes=4 * 1024 * 1024)
LARGE = pltpu.CompilerParams(vmem_limit_bytes=24 * 1024 * 1024)


def in_hbm(x):
    return pltpu.with_memory_space_constraint(x, pltpu.HBM)


def pack_kernel(vector_hbm, right_hbm, out_hbm, vector_s, right_s, turned_s, in_sems, out_sems):
    half, _ = right_s.shape[1:]
    rows = vector_s.shape[0]
    loads = [
        pltpu.make_async_copy(vector_hbm, vector_s, in_sems.at[0]),
        pltpu.make_async_copy(right_hbm, right_s, in_sems.at[1]),
    ]
    for load in loads:
        load.start()
    places = range(out_hbm.shape[0])
    stores = [pltpu.make_async_copy(vector_s, out_hbm.at[r, pl.ds(0, rows)], out_sems.at[0, r]) for r in places]
    loads[0].wait()
    for store in stores:
        store.start()
    loads[1].wait()
    for v in range(right_s.shape[0]):
        turned = right_s[v].astype(jnp.float32).T
        turned = jnp.concatenate([turned[:half], turned[half:]], 1).astype(jnp.bfloat16)
        turned_s[v * half : (v + 1) * half, :] = turned
    more = [pltpu.make_async_copy(turned_s, out_hbm.at[r, pl.ds(rows, turned_s.shape[0])], out_sems.at[1, r]) for r in places]
    for store in more:
        store.start()
    for store in stores + more:
        store.wait()


def pack(vector, right, size):
    rows, width = vector.shape
    channels, half, _ = right.shape
    return pl.pallas_call(
        pack_kernel,
        out_shape=pltpu.HBM((size, rows + channels * half, width), jnp.bfloat16),
        in_specs=[HBM, HBM],
        out_specs=HBM,
        scratch_shapes=[
            pltpu.VMEM(vector.shape, jnp.bfloat16),
            pltpu.VMEM(right.shape, jnp.bfloat16),
            pltpu.VMEM((channels * half, width), jnp.bfloat16),
            pltpu.SemaphoreType.DMA((2,)),
            pltpu.SemaphoreType.DMA((2, size)),
        ],
        compiler_params=SMALL,
    )(in_hbm(vector), in_hbm(right))


def site_copies(left_site, right_site, left_t, right_t, sems):
    loads = (
        pltpu.make_async_copy(left_site, left_t, sems.at[0]),
        pltpu.make_async_copy(right_site, right_t, sems.at[1]),
    )
    for load in loads:
        load.start()
    return loads


def combined(terms):
    total = None
    for scale, x in terms:
        total = scale * x if total is None else total + scale * x
    return total


def contract_and_mix(site_loads, left_t, right_t, left_ref, piece_s, vec_s, cross_s, half_s, store):
    blocks, _, width = piece_s.shape
    half = width // 2
    for r in range(blocks):
        vec_s[:, r * width : (r + 1) * width] = piece_s[r, : STATES * half, :]
    cross_s[...] = jnp.dot(vec_s[...], left_ref[...], preferred_element_type=jnp.float32)
    for load in site_loads:
        load.wait()
    for s1 in range(2):
        for u in range(CHANNELS):
            for t2 in range(2):
                half_s[u, t2] = combined(
                    (
                        left_t[w, s1, t1, u],
                        cross_s[(2 * t1 + t2) * half : (2 * t1 + t2 + 1) * half, w * width : (w + 1) * width],
                    )
                    for w in range(CHANNELS)
                    for t1 in range(2)
                )
        for v in range(CHANNELS):
            for s2 in range(2):
                total = combined((right_t[u, s2, t2, v], half_s[u, t2]) for u in range(CHANNELS) for t2 in range(2))
                store(v, 2 * s1 + s2, total.astype(jnp.bfloat16))


def own_kernel(
    left_site, right_site, left_ref, own_hbm, mixed_out, right_out,
    left_t, right_t, piece_s, vec_s, cross_s, half_s, sems, site_sems,
):
    _, rows, width = piece_s.shape
    half = rows // STATES
    load = pltpu.make_async_copy(own_hbm.at[:, pl.ds(0, rows)], piece_s, sems.at[0])
    load.start()
    passed = pltpu.make_async_copy(own_hbm.at[:, pl.ds(rows, CHANNELS * half)], right_out, sems.at[1])
    passed.start()
    site_loads = site_copies(left_site, right_site, left_t, right_t, site_sems)
    load.wait()

    def store(v, s, x):
        mixed_out[v * half : (v + 1) * half, s * width : (s + 1) * width] = x

    contract_and_mix(site_loads, left_t, right_t, left_ref, piece_s, vec_s, cross_s, half_s, store)
    passed.wait()


def own_part(sites, left, own):
    blocks, _, width = own.shape
    half = width // 2
    return pl.pallas_call(
        own_kernel,
        out_shape=(
            jax.ShapeDtypeStruct((CHANNELS * half, STATES * width), jnp.bfloat16),
            jax.ShapeDtypeStruct((blocks, CHANNELS * half, width), jnp.bfloat16),
        ),
        in_specs=[HBM, HBM, VMEM, HBM],
        out_specs=(VMEM, VMEM),
        scratch_shapes=[
            *(pltpu.SMEM(site.shape, jnp.float32) for site in sites),
            pltpu.VMEM((blocks, STATES * half, width), jnp.bfloat16),
            pltpu.VMEM((STATES * half, blocks * width), jnp.bfloat16),
            pltpu.VMEM((STATES * half, CHANNELS * width), jnp.float32),
            pltpu.VMEM((CHANNELS, 2, half, width), jnp.float32),
            pltpu.SemaphoreType.DMA((2,)),
            pltpu.SemaphoreType.DMA((2,)),
        ],
        compiler_params=LARGE,
    )(*(in_hbm(site) for site in sites), left, in_hbm(own))


def terms_kernel(
    order, left_site, right_site, left_ref, mixed_ref, right_own, other_ref, out_ref,
    left_t, right_t, vec_s, cross_s, half_s, right_s, mixed_s, site_sems,
):
    blocks, half, _ = out_ref.shape
    width = 2 * half
    core = lax.axis_index(C)
    own_at = pl.multiple_of(core * half, half)
    other_at = pl.multiple_of((1 - core) * half, half)
    site_loads = site_copies(left_site, right_site, left_t, right_t, site_sems)
    mine = lax.broadcasted_iota(jnp.int32, (half, width), 1) // half == core
    for v in range(CHANNELS):
        mixed_s[pl.ds(v * width + own_at, half), :] = mixed_ref[v * half : (v + 1) * half, :]

    def store(v, s, x):
        mixed_s[pl.ds(v * width + other_at, half), s * width : (s + 1) * width] = x

    contract_and_mix(site_loads, left_t, right_t, left_ref, other_ref, vec_s, cross_s, half_s, store)
    for r in range(blocks):
        for v in range(CHANNELS):
            at = (slice(r * half, (r + 1) * half), slice(v * width, (v + 1) * width))
            other = other_ref[r, (STATES + v) * half : (STATES + v + 1) * half, :].astype(jnp.float32)
            other = jnp.concatenate([other[:, half:], other[:, :half]], 1)
            own = right_own[r, v * half : (v + 1) * half, :].astype(jnp.float32)
            right_s[at] = jnp.where(mine, own, other).astype(jnp.bfloat16)
    image = jnp.dot(right_s[...], mixed_s[...], preferred_element_type=jnp.float32)
    for r in range(blocks):
        out_ref[order[r]] = image[r * half : (r + 1) * half].astype(jnp.bfloat16)


def terms(order, sites, left, mixed, right, other):
    def step(*refs):
        terms_kernel(order, *refs)

    blocks, _, width = other.shape
    half = width // 2
    return pl.pallas_call(
        step,
        out_shape=jax.ShapeDtypeStruct((blocks, half, STATES * width), jnp.bfloat16),
        in_specs=[HBM, HBM, VMEM, VMEM, VMEM, VMEM],
        out_specs=VMEM,
        scratch_shapes=[
            *(pltpu.SMEM(site.shape, jnp.float32) for site in sites),
            pltpu.VMEM((STATES * half, blocks * width), jnp.bfloat16),
            pltpu.VMEM((STATES * half, CHANNELS * width), jnp.float32),
            pltpu.VMEM((CHANNELS, 2, half, width), jnp.float32),
            pltpu.VMEM((blocks * half, CHANNELS * width), jnp.bfloat16),
            pltpu.VMEM((CHANNELS * width, STATES * width), jnp.bfloat16),
            pltpu.SemaphoreType.DMA((2,)),
        ],
        compiler_params=LARGE,
    )(*(in_hbm(site) for site in sites), left, mixed, right, other)


def near_kernel(pieces_ref, out_ref):
    for j in range(out_ref.shape[0]):
        total = pieces_ref[0, j].astype(jnp.float32)
        for k in range(1, pieces_ref.shape[0]):
            total = total + pieces_ref[k, j].astype(jnp.float32)
        out_ref[j] = total.astype(jnp.bfloat16)


def near_sum(pieces):
    return pl.pallas_call(
        near_kernel,
        out_shape=jax.ShapeDtypeStruct(pieces.shape[1:], jnp.bfloat16),
        in_specs=[VMEM],
        out_specs=VMEM,
        compiler_params=SMALL,
    )(pieces)


def neighbours(n_far, n_near):
    n_z = n_far * n_near
    groups = []
    for core in range(2):
        for j in range(n_far):
            first = j * n_near + (1 - core) * (n_near // 2)
            chips = sorted(((first + i) % n_z for i in range(n_near)), key=lambda z: z % n_near)
            groups.append([2 * z + core for z in chips])
    return groups


def lanes_of(total):
    rows, cols = total.shape
    total = sum(total[:, k : k + 128] for k in range(0, cols, 128))
    return sum(total[k : k + 8] for k in range(0, rows, 8))


def sums_kernel(pieces_ref, vector_ref, image_ref, sums_ref):
    image = pieces_ref[0].astype(jnp.float32)
    for k in range(1, pieces_ref.shape[0]):
        image = image + pieces_ref[k].astype(jnp.float32)
    image_ref[...] = image
    base = jnp.concatenate([vector_ref[t].astype(jnp.float32) for t in range(STATES)], 1)
    found = [lanes_of(base * base), lanes_of(base * image), lanes_of(image * image)]
    lane = lax.broadcasted_iota(jnp.int32, (1, 128), 1)
    row = jnp.zeros((1, 128), jnp.float32)
    for k in range(3):
        row = jnp.where(lane == k, jnp.sum(found[k], keepdims=True), row)
    for r in range(sums_ref.shape[0]):
        sums_ref[r] = row


def sums_of(pieces, vector, size):
    return pl.pallas_call(
        sums_kernel,
        out_shape=(
            jax.ShapeDtypeStruct(pieces.shape[1:], jnp.float32),
            jax.ShapeDtypeStruct((size, 1, 128), jnp.float32),
        ),
        in_specs=[VMEM, VMEM],
        out_specs=(VMEM, VMEM),
        compiler_params=SMALL,
    )(pieces, vector)


def again_kernel(pieces_ref, out_ref):
    total = pieces_ref[0]
    for k in range(1, pieces_ref.shape[0]):
        total = total + pieces_ref[k]
    for r in range(out_ref.shape[0]):
        out_ref[r] = total


def again(pieces, size):
    return pl.pallas_call(
        again_kernel,
        out_shape=jax.ShapeDtypeStruct((size, *pieces.shape[1:]), jnp.float32),
        in_specs=[VMEM],
        out_specs=VMEM,
        compiler_params=SMALL,
    )(pieces)


def last_kernel(entries, pieces_ref, image_ref, vector_ref, next_ref, coefficients_ref):
    total = pieces_ref[0]
    for k in range(1, pieces_ref.shape[0]):
        total = total + pieces_ref[k]
    total = total / entries
    lane = lax.broadcasted_iota(jnp.int32, total.shape, 1)
    base_square, correlation, image_square = (
        jnp.sum(jnp.where(lane == k, total, 0.0), 1, keepdims=True) for k in range(3)
    )
    alpha = correlation / (base_square + epsilon)
    rho = jnp.sqrt(image_square - 2.0 * alpha * correlation + alpha * alpha * base_square + epsilon)
    width = next_ref.shape[2]
    for t in range(STATES):
        residual = image_ref[:, t * width : (t + 1) * width] - alpha * vector_ref[t].astype(jnp.float32)
        next_ref[t] = (residual / rho).astype(jnp.bfloat16)
    coefficients_ref[0] = alpha[0, 0]
    coefficients_ref[1] = rho[0, 0]


def last(entries, pieces, image, vector):
    def step(*refs):
        last_kernel(entries, *refs)

    return pl.pallas_call(
        step,
        out_shape=(
            jax.ShapeDtypeStruct(vector.shape, jnp.bfloat16),
            jax.ShapeDtypeStruct((2,), jnp.float32),
        ),
        in_specs=[VMEM, VMEM, VMEM],
        out_specs=(VMEM, SMEM),
        compiler_params=SMALL,
    )(pieces, image, vector)


def all_to_all(x, axes):
    return lax.all_to_all(x, axes, 0, 0, tiled=True)


def other_core(x):
    return lax.ppermute(x, C, [(0, 1), (1, 0)])


def body(start_vector, left_env, right_env, left_tensor, right_tensor):
    n_row = lax.axis_size(ROW)
    n_far, n_near = lax.axis_size(FAR), lax.axis_size(NEAR)
    n_z = n_far * n_near
    _, rows, half = start_vector.shape
    entries = float(STATES * rows * half * n_row * n_z * lax.axis_size(C))
    sites = tuple(jnp.transpose(tensor, (0, 2, 3, 1)) for tensor in (left_tensor, right_tensor))
    vector = jnp.swapaxes(start_vector, 1, 2)
    left = jnp.transpose(left_env, (2, 0, 1)).reshape(half, CHANNELS * rows)
    left = (left.astype(jnp.float32) * SCALE).astype(jnp.float16)

    own = all_to_all(pack(vector.reshape(STATES * half, rows), right_env, n_row), ROW)
    left = lax.all_gather(left, COL, axis=0, tiled=True)
    own, left = lax.optimization_barrier((own, left))
    left = (left.astype(jnp.float32) * (1.0 / SCALE)).astype(jnp.bfloat16)
    order = [n_far * (z % n_near) + z // n_near for z in range(n_z)]
    other = other_core(own)
    mixed, right = own_part(sites, left, own)
    sent = terms(order, sites, left, mixed, right, other)

    pieces = lax.all_to_all(sent, COL, 0, 0, axis_index_groups=neighbours(n_far, n_near), tiled=True)
    pieces = all_to_all(near_sum(pieces.reshape(n_near, n_far, *pieces.shape[1:])), FAR)
    image, sums = sums_of(pieces, vector, lax.axis_size((X, Y, C)))
    sums = again(all_to_all(sums, (X, Y, C)), n_z)
    next_vector, coefficients = last(entries, all_to_all(sums, Z), image, vector)
    return jnp.swapaxes(next_vector, 1, 2), coefficients


def solution(mesh):
    finer = Mesh(mesh.devices.reshape(4, 4, 4, 4, 2), (X, Y, FAR, NEAR, C))
    in_specs = (P(None, ROW, COL), P(None, ROW, COL), P(None, COL, ROW), P(), P())
    out_specs = (P(None, ROW, COL), P())
    return jax.shard_map(body, mesh=finer, in_specs=in_specs, out_specs=out_specs, check_vma=False)
```
